32 devices in a mesh: rep: 1 (over z), data: 4 (over y), stage: 8 (over x, core).
Axes of the slice: x: 4, y: 4, z: 1, core: 2. Of those that a mesh axis runs over, the one named last changes fastest.
The devices are a block of a 4x4x8 slice.
Arguments:
- embeds: bfloat16 [12, 4, 256, 768], P(('rep', 'data'))
- targets: bfloat16 [12, 4, 256, 768], P(('rep', 'data'))
- w_qkv: bfloat16 [8, 3, 12, 64, 768], P(('rep', 'stage'))
- w_out: bfloat16 [8, 12, 64, 768], P(('rep', 'stage'))
- w_up: bfloat16 [8, 768, 3072], P(('rep', 'stage'))
- w_down: bfloat16 [8, 3072, 768], P(('rep', 'stage'))
Outputs:
- output 1: float32 [1], P('rep')
- output 2: float32 [8, 3, 12, 64, 768], P(('rep', 'stage'))
- output 3: float32 [8, 12, 64, 768], P(('rep', 'stage'))
- output 4: float32 [8, 768, 3072], P(('rep', 'stage'))
- output 5: float32 [8, 3072, 768], P(('rep', 'stage'))
- output 6: bfloat16 [12, 4, 256, 768], P(('rep', 'data'))
All inputs are finite; a program needn't handle non-finite values.
Results may differ from the reference program's by a relative error of at most 0.02.
Values are sent between devices in bfloat16 or wider.
A program may use at most 768 MiB of HBM per device.

```python
import jax
import jax.numpy as jnp
from jax import lax

DATA_REPS = 4
N_STAGES = 8
N_MICRO = 3
MICRO_BATCH = 4
SEQ_LEN = 256
D_MODEL = 768
N_HEADS = 12
HEAD_DIM = D_MODEL // N_HEADS
FFN_DIM = 4 * D_MODEL
TOTAL_MICRO = DATA_REPS * N_MICRO
NORM_EPS = 1e-6


def setup_inputs(seed: int = 0, part: int = 0) -> dict:
    part_key = jax.random.fold_in(jax.random.key(seed), part)
    keys = jax.random.split(part_key, 6)
    act_shape = (TOTAL_MICRO, MICRO_BATCH, SEQ_LEN, D_MODEL)
    model_scale = D_MODEL ** -0.5
    ffn_scale = FFN_DIM ** -0.5
    embeds = jax.random.normal(keys[0], act_shape, jnp.float32).astype(jnp.bfloat16)
    targets = jax.random.normal(keys[1], act_shape, jnp.float32).astype(jnp.bfloat16)
    w_qkv = (jax.random.normal(keys[2], (N_STAGES, 3, N_HEADS, HEAD_DIM, D_MODEL), jnp.float32) * model_scale).astype(jnp.bfloat16)
    w_out = (jax.random.normal(keys[3], (N_STAGES, N_HEADS, HEAD_DIM, D_MODEL), jnp.float32) * model_scale).astype(jnp.bfloat16)
    w_up = (jax.random.normal(keys[4], (N_STAGES, D_MODEL, FFN_DIM), jnp.float32) * model_scale).astype(jnp.bfloat16)
    w_down = (jax.random.normal(keys[5], (N_STAGES, FFN_DIM, D_MODEL), jnp.float32) * ffn_scale).astype(jnp.bfloat16)
    return {'embeds': embeds, 'targets': targets, 'w_qkv': w_qkv, 'w_out': w_out, 'w_up': w_up, 'w_down': w_down}


def bf16_cast(vals):
    return vals.astype(jnp.bfloat16).astype(jnp.float32)


def rms_norm(vals):
    return vals * lax.rsqrt(jnp.mean(vals * vals, axis=-1, keepdims=True) + NORM_EPS)


def layer_apply(act_in, w_qkv, w_out, w_up, w_down):
    normed1 = bf16_cast(rms_norm(act_in))
    qkv_proj = bf16_cast(jnp.einsum('bsd,thkd->tbhsk', normed1, w_qkv))
    scale = HEAD_DIM ** -0.5
    scores = jnp.einsum('bhqk,bhsk->bhqs', qkv_proj[0], qkv_proj[1]) * scale
    positions = jnp.arange(SEQ_LEN)
    causal = positions[:, None] >= positions[None, :]
    attn_probs = bf16_cast(jax.nn.softmax(jnp.where(causal, scores, -1e30), axis=-1))
    context = bf16_cast(jnp.einsum('bhqs,bhsk->bhqk', attn_probs, qkv_proj[2]))
    hidden = bf16_cast(act_in + jnp.einsum('bhqk,hkd->bqd', context, w_out))
    pre_act = jnp.einsum('bsd,df->bsf', bf16_cast(rms_norm(hidden)), w_up)
    upper = bf16_cast(jax.nn.gelu(pre_act, approximate=True))
    return bf16_cast(hidden + jnp.einsum('bsf,fd->bsd', upper, w_down))


def reference(embeds, targets, w_qkv, w_out, w_up, w_down):
    weights = tuple(w.astype(jnp.float32) for w in (w_qkv, w_out, w_up, w_down))
    grad_scale = 1.0 / TOTAL_MICRO
    loss_norm = 1.0 / (TOTAL_MICRO * MICRO_BATCH * SEQ_LEN * D_MODEL)

    def forward_layer(act_in, layer_w):
        return layer_apply(act_in, *layer_w), act_in

    def backward_layer(grad_out, layer_pack):
        act_in, layer_w = layer_pack
        vjp_pull = jax.vjp(layer_apply, act_in, *layer_w)[1]
        cotangents = vjp_pull(grad_out)
        return bf16_cast(cotangents[0]), cotangents[1:]

    def micro_step(carry, micro_pair):
        grad_sums, loss_sum = carry
        act_out, stash = lax.scan(forward_layer, micro_pair[0].astype(jnp.float32), weights)
        error_mb = act_out - micro_pair[1].astype(jnp.float32)
        loss_sum = loss_sum + 0.5 * jnp.sum(error_mb * error_mb) * loss_norm
        grad_seed = bf16_cast(error_mb * grad_scale)
        grad_in, layer_grads = lax.scan(backward_layer, grad_seed, (stash, weights), reverse=True)
        grad_sums = tuple(total + piece for total, piece in zip(grad_sums, layer_grads))
        return (grad_sums, loss_sum), grad_in.astype(jnp.bfloat16)

    init_carry = (tuple(jnp.zeros_like(w) for w in weights), jnp.zeros((), jnp.float32))
    (grad_sums, loss_sum), d_embeds = lax.scan(micro_step, init_carry, (embeds, targets))
    return (loss_sum.reshape(1), grad_sums[0], grad_sums[1], grad_sums[2], grad_sums[3], d_embeds)
```

```python
import functools

import jax
import jax.numpy as jnp
from jax import lax
from jax.experimental import pallas as pl
from jax.experimental.pallas import tpu as pltpu
from jax.sharding import PartitionSpec as P

NORM_EPS = 1e-6
LOG2E = 1.4426950408889634
GELU_C = 0.7978845608028654
GELU_A = 0.044715
MESH_ID = pl.DeviceIdType.MESH


def dot_nn(lhs, rhs):
    return lax.dot_general(lhs, rhs, (((1,), (0,)), ((), ())), preferred_element_type=jnp.float32)


def dot_nt(lhs, rhs):
    return lax.dot_general(lhs, rhs, (((1,), (1,)), ((), ())), preferred_element_type=jnp.float32)


def dot_tn(lhs, rhs):
    return lax.dot_general(lhs, rhs, (((0,), (0,)), ((), ())), preferred_element_type=jnp.float32)


def rms_scale(vals):
    return lax.rsqrt(jnp.mean(vals * vals, axis=-1, keepdims=True) + NORM_EPS)


def rms_vjp(vals, cotangent):
    scale = rms_scale(vals)
    inner = jnp.mean(vals * cotangent, axis=-1, keepdims=True)
    return scale * (cotangent - vals * (scale * scale * inner))


def causal_weights(scores_t, col_max, col_inv, scale):
    half = scores_t.shape[0] // 2
    diag = lax.broadcasted_iota(jnp.int32, (half, half), 0) <= lax.broadcasted_iota(jnp.int32, (half, half), 1)
    upper_l = jnp.where(diag, scores_t[:half, :half], -1e30)
    upper_r = scores_t[:half, half:]
    lower_r = jnp.where(diag, scores_t[half:, half:], -1e30)
    fresh = col_max is None
    if fresh:
        max_l = jnp.max(upper_l, axis=0, keepdims=True)
        max_r = jnp.maximum(jnp.max(upper_r, axis=0, keepdims=True), jnp.max(lower_r, axis=0, keepdims=True))
    else:
        max_l, max_r = col_max[:, :half], col_max[:, half:]
    factor = scale * LOG2E
    exp_ul = jnp.exp2((upper_l - max_l) * factor)
    exp_ur = jnp.exp2((upper_r - max_r) * factor)
    exp_lr = jnp.exp2((lower_r - max_r) * factor)
    if fresh:
        inv_l = 1.0 / jnp.sum(exp_ul, axis=0, keepdims=True)
        inv_r = 1.0 / (jnp.sum(exp_ur, axis=0, keepdims=True) + jnp.sum(exp_lr, axis=0, keepdims=True))
        stats = (jnp.concatenate([max_l, max_r], axis=1), jnp.concatenate([inv_l, inv_r], axis=1))
    else:
        inv_l, inv_r = col_inv[:, :half], col_inv[:, half:]
        stats = None
    return (exp_ul * inv_l, exp_ur * inv_r, exp_lr * inv_r), stats


def assemble(blocks, dtype):
    upper_l, upper_r, lower_r = (b.astype(dtype) for b in blocks)
    upper = jnp.concatenate([upper_l, upper_r], axis=1)
    lower = jnp.concatenate([jnp.zeros_like(upper_l), lower_r], axis=1)
    return jnp.concatenate([upper, lower], axis=0)


def forward_layer(dims, act_ref, wqkv, wout, wup, wdown, n1_ref, qkv_ref, stat_ref, ctx_ref, hid_ref, n2_ref, gp_ref, up_ref, out_ref, flush):
    heads, hdim, ffn_tile = dims
    width = heads * hdim
    ffn = wdown.shape[0]
    scale = hdim ** -0.5
    act32 = act_ref[...].astype(jnp.float32)
    normed1 = (act32 * rms_scale(act32)).astype(jnp.bfloat16)
    n1_ref[...] = normed1
    qkv_ref[...] = dot_nt(wqkv[...], normed1).astype(jnp.bfloat16)
    flush(0)

    def head_body(h, carry):
        q_rows = pl.ds(pl.multiple_of(h * hdim, hdim), hdim)
        k_rows = pl.ds(pl.multiple_of(width + h * hdim, hdim), hdim)
        v_rows = pl.ds(pl.multiple_of(2 * width + h * hdim, hdim), hdim)
        scores_t = dot_tn(qkv_ref[k_rows, :], qkv_ref[q_rows, :])
        blocks, stats = causal_weights(scores_t, None, None, scale)
        stat_ref[h, 0:1, :] = stats[0]
        stat_ref[h, 1:2, :] = stats[1]
        ctx_ref[q_rows, :] = dot_nn(qkv_ref[v_rows, :], assemble(blocks, jnp.bfloat16)).astype(jnp.bfloat16)
        return carry

    lax.fori_loop(0, heads, head_body, 0, unroll=True)
    attn = dot_tn(ctx_ref[...], wout[...])
    hid16 = (act_ref[...].astype(jnp.float32) + attn).astype(jnp.bfloat16)
    hid_ref[...] = hid16
    hid32 = hid16.astype(jnp.float32)
    normed2 = (hid32 * rms_scale(hid32)).astype(jnp.bfloat16)
    n2_ref[...] = normed2
    flush(1)
    for tile in range(ffn // ffn_tile):
        cols = pl.ds(tile * ffn_tile, ffn_tile)
        pre = dot_nn(normed2, wup[:, cols])
        gp_ref[:, cols] = pre
        tanh = jnp.tanh(pre * (GELU_C + (GELU_C * GELU_A) * (pre * pre)))
        up_ref[:, cols] = (pre * (0.5 + 0.5 * tanh)).astype(jnp.bfloat16)
    flush(2)
    down = dot_nn(up_ref[...], wdown[...])
    out_ref[...] = (hid_ref[...].astype(jnp.float32) + down).astype(jnp.bfloat16)


def backward_layer(dims, grad_ref, act_ref, wqkv, wout, wup, wdown, qkv_ref, stat_ref, hid_ref, gp_ref, dpre_ref, dhid_ref, dctx_ref, dqkv_ref, dact_ref, flush):
    heads, hdim, ffn_tile = dims
    width = heads * hdim
    ffn = wdown.shape[0]
    scale = hdim ** -0.5
    grad16 = grad_ref[...]
    for tile in range(ffn // ffn_tile):
        cols = pl.ds(tile * ffn_tile, ffn_tile)
        dup = dot_nt(grad16, wdown[cols, :])
        pre = gp_ref[:, cols]
        pre_sq = pre * pre
        tanh = jnp.tanh(pre * (GELU_C + (GELU_C * GELU_A) * pre_sq))
        half = 0.5 + 0.5 * tanh
        bend = (half * (1.0 - half)) * (pre * (2.0 * GELU_C + (6.0 * GELU_C * GELU_A) * pre_sq))
        dpre_ref[:, cols] = (dup * (half + bend)).astype(jnp.bfloat16)
    flush(0)
    dnormed2 = dot_nt(dpre_ref[...], wup[...])
    dhid32 = grad_ref[...].astype(jnp.float32) + rms_vjp(hid_ref[...].astype(jnp.float32), dnormed2)
    dhid16 = dhid32.astype(jnp.bfloat16)
    dhid_ref[...] = dhid16
    flush(1)
    dctx_ref[...] = dot_nt(wout[...], dhid16).astype(jnp.bfloat16)

    def head_body(h, carry):
        q_rows = pl.ds(pl.multiple_of(h * hdim, hdim), hdim)
        k_rows = pl.ds(pl.multiple_of(width + h * hdim, hdim), hdim)
        v_rows = pl.ds(pl.multiple_of(2 * width + h * hdim, hdim), hdim)
        query_t = qkv_ref[q_rows, :]
        keys_t = qkv_ref[k_rows, :]
        dctx_t = dctx_ref[q_rows, :]
        scores_t = dot_tn(keys_t, query_t)
        probs, _ = causal_weights(scores_t, stat_ref[h, 0:1, :], stat_ref[h, 1:2, :], scale)
        dprobs = dot_tn(qkv_ref[v_rows, :], dctx_t)
        half = dprobs.shape[0] // 2
        d_ul, d_ur, d_lr = dprobs[:half, :half], dprobs[:half, half:], dprobs[half:, half:]
        p_ul, p_ur, p_lr = probs
        delta_l = jnp.sum(d_ul * p_ul, axis=0, keepdims=True)
        delta_r = jnp.sum(d_ur * p_ur, axis=0, keepdims=True) + jnp.sum(d_lr * p_lr, axis=0, keepdims=True)
        dscores = assemble((p_ul * (d_ul - delta_l) * scale, p_ur * (d_ur - delta_r) * scale, p_lr * (d_lr - delta_r) * scale), jnp.bfloat16)
        dqkv_ref[v_rows, :] = dot_nt(dctx_t, assemble(probs, jnp.bfloat16)).astype(jnp.bfloat16)
        dqkv_ref[q_rows, :] = dot_nn(keys_t, dscores).astype(jnp.bfloat16)
        dqkv_ref[k_rows, :] = dot_nt(query_t, dscores).astype(jnp.bfloat16)
        return carry

    lax.fori_loop(0, heads, head_body, 0, unroll=True)
    flush(2)
    dnormed1 = dot_tn(dqkv_ref[...], wqkv[...])
    dact = dhid32 + rms_vjp(act_ref[...].astype(jnp.float32), dnormed1)
    dact_ref[...] = dact.astype(jnp.bfloat16)


def pipeline_kernel(
    cfg,
    emb_hbm, tgt_hbm, wqkv_hbm, wout_hbm, wup_hbm, wdown_hbm,
    loss_ref, n1_hbm, n2_hbm, up_hbm, ctx_hbm, dqkv_hbm, dpre_hbm, dhid_hbm, g_hbm, dx_hbm, qkv_hbm, gp_hbm, hid_hbm, stat_hbm,
    wqkv, wout, wup, wdown, act, grad, out_s, dact_s,
    n1_s, n2_s, up_s, ctx_s, qkv_s, gp_s, hid_s, stat_s,
    dpre_s, dhid_s, dctx_s, dqkv_s,
    w_sem, in_sem, act_sem, grad_sem, fout_sem, bin_sem, bout_sem, fsend_sem, bsend_sem, loss_acc, loss_sem,
):
    n_stages, n_seq, tokens, grad_scale, dims = cfg
    stage = lax.axis_index('stage')
    is_first = stage == 0
    is_last = stage == n_stages - 1
    nxt = lax.rem(stage + 1, n_stages)
    prv = lax.rem(stage + n_stages - 1, n_stages)

    weight_pairs = ((wqkv_hbm, wqkv), (wout_hbm, wout), (wup_hbm, wup), (wdown_hbm, wdown))
    for idx, (src, dst) in enumerate(weight_pairs):
        pltpu.make_async_copy(src, dst, w_sem.at[idx]).start()

    def load_embed(m):
        return pltpu.make_async_copy(emb_hbm.at[m], act.at[m], in_sem.at[m])

    def load_target(m):
        return pltpu.make_async_copy(tgt_hbm.at[m], grad.at[m], in_sem.at[m])

    @pl.when(is_first)
    def _():
        def go(m, carry):
            load_embed(m).start()
            return carry
        lax.fori_loop(0, n_seq, go, 0)

    @pl.when(is_last)
    def _():
        def go(m, carry):
            load_target(m).start()
            return carry
        lax.fori_loop(0, n_seq, go, 0)

    barrier = pltpu.get_barrier_semaphore()
    for peer in (prv, nxt):
        pl.semaphore_signal(barrier, inc=1, device_id={'stage': peer}, device_id_type=MESH_ID)
    pl.semaphore_wait(barrier, 2)

    loss_acc[...] = jnp.zeros_like(loss_acc)
    for idx, (src, dst) in enumerate(weight_pairs):
        pltpu.make_async_copy(src, dst, w_sem.at[idx]).wait()

    def send_act(m, slot):
        return pltpu.make_async_remote_copy(
            src_ref=out_s.at[slot], dst_ref=act.at[m], send_sem=fsend_sem.at[slot], recv_sem=act_sem.at[m],
            device_id={'stage': nxt}, device_id_type=MESH_ID)

    def send_grad(m, slot):
        return pltpu.make_async_remote_copy(
            src_ref=dact_s.at[slot], dst_ref=grad.at[m], send_sem=bsend_sem.at[slot], recv_sem=grad_sem.at[m],
            device_id={'stage': prv}, device_id_type=MESH_ID)

    def store_dx(m, slot):
        return pltpu.make_async_copy(dact_s.at[slot], dx_hbm.at[m], bsend_sem.at[slot])

    def token_range(m):
        return pl.ds(pl.multiple_of(m * tokens, tokens), tokens)

    def fout_copies(m, slot):
        rows = token_range(m)
        return (
            (0, pltpu.make_async_copy(n1_s.at[slot], n1_hbm.at[rows, :], fout_sem.at[slot, 0])),
            (0, pltpu.make_async_copy(qkv_s.at[slot], qkv_hbm.at[m], fout_sem.at[slot, 1])),
            (1, pltpu.make_async_copy(ctx_s.at[slot], ctx_hbm.at[:, rows], fout_sem.at[slot, 2])),
            (1, pltpu.make_async_copy(stat_s.at[slot], stat_hbm.at[m], fout_sem.at[slot, 3])),
            (1, pltpu.make_async_copy(hid_s.at[slot], hid_hbm.at[m], fout_sem.at[slot, 4])),
            (1, pltpu.make_async_copy(n2_s.at[slot], n2_hbm.at[rows, :], fout_sem.at[slot, 5])),
            (2, pltpu.make_async_copy(gp_s.at[slot], gp_hbm.at[m], fout_sem.at[slot, 6])),
            (2, pltpu.make_async_copy(up_s.at[slot], up_hbm.at[rows, :], fout_sem.at[slot, 7])),
        )

    def bin_copies(m):
        return (
            pltpu.make_async_copy(qkv_hbm.at[m], qkv_s.at[2], bin_sem.at[0]),
            pltpu.make_async_copy(stat_hbm.at[m], stat_s.at[2], bin_sem.at[1]),
            pltpu.make_async_copy(hid_hbm.at[m], hid_s.at[2], bin_sem.at[2]),
            pltpu.make_async_copy(gp_hbm.at[m], gp_s.at[2], bin_sem.at[3]),
        )

    def bout_copies(m, slot):
        rows = token_range(m)
        return (
            (0, pltpu.make_async_copy(grad.at[m], g_hbm.at[rows, :], bout_sem.at[slot, 0])),
            (0, pltpu.make_async_copy(dpre_s.at[slot], dpre_hbm.at[rows, :], bout_sem.at[slot, 1])),
            (1, pltpu.make_async_copy(dhid_s.at[slot], dhid_hbm.at[rows, :], bout_sem.at[slot, 2])),
            (2, pltpu.make_async_copy(dqkv_s.at[slot], dqkv_hbm.at[:, rows], bout_sem.at[slot, 3])),
        )

    def flusher(copies):
        def flush(group):
            for when, copy in copies:
                if when == group:
                    copy.start()
        return flush

    def in_range(m):
        return (m >= 0) & (m < n_seq)

    def tick(t, carry):
        fwd_m = t - stage
        bwd_m = t + stage - (2 * n_stages - 2)

        @pl.when(in_range(fwd_m))
        def _():
            m = fwd_m
            slot = lax.rem(m, 2)

            @pl.when(is_first)
            def _():
                load_embed(m).wait()

            @pl.when(jnp.logical_not(is_first))
            def _():
                send_act(m, slot).wait_recv()

            forward_layer(
                dims, act.at[m], wqkv, wout, wup, wdown, n1_s.at[slot], qkv_s.at[slot], stat_s.at[slot],
                ctx_s.at[slot], hid_s.at[slot], n2_s.at[slot], gp_s.at[slot], up_s.at[slot], out_s.at[slot],
                flusher(fout_copies(m, slot)))

            @pl.when(jnp.logical_not(is_last))
            def _():
                send_act(m, slot).start()

            @pl.when(is_last)
            def _():
                load_target(m).wait()
                error = out_s[slot].astype(jnp.float32) - grad[m].astype(jnp.float32)
                square = error * error
                total = square[0:8]
                for row in range(8, tokens, 8):
                    total = total + square[row:row + 8]
                loss_acc[...] += total
                grad[m] = (error * grad_scale).astype(jnp.bfloat16)

        @pl.when(in_range(bwd_m))
        def _():
            m = bwd_m
            slot = lax.rem(m, 2)

            @pl.when(jnp.logical_not(is_last))
            def _():
                for copy in bin_copies(m):
                    copy.wait()
                send_grad(m, slot).wait_recv()

            saved = jnp.where(is_last, slot, 2)
            backward_layer(
                dims, grad.at[m], act.at[m], wqkv, wout, wup, wdown, qkv_s.at[saved], stat_s.at[saved], hid_s.at[saved],
                gp_s.at[saved], dpre_s.at[slot], dhid_s.at[slot], dctx_s, dqkv_s.at[slot], dact_s.at[slot],
                flusher(bout_copies(m, slot)))

            @pl.when(jnp.logical_not(is_first))
            def _():
                send_grad(m, slot).start()

            @pl.when(is_first)
            def _():
                store_dx(m, slot).start()

        fwd_old = fwd_m - 1
        bwd_old = bwd_m - 1

        @pl.when(in_range(fwd_old))
        def _():
            slot = lax.rem(fwd_old, 2)
            for _, copy in fout_copies(fwd_old, slot):
                copy.wait()

            @pl.when(jnp.logical_not(is_last))
            def _():
                send_act(fwd_old, slot).wait_send()

        @pl.when(in_range(bwd_old))
        def _():
            slot = lax.rem(bwd_old, 2)
            for _, copy in bout_copies(bwd_old, slot):
                copy.wait()

            @pl.when(jnp.logical_not(is_first))
            def _():
                send_grad(bwd_old, slot).wait_send()

            @pl.when(is_first)
            def _():
                store_dx(bwd_old, slot).wait()

        @pl.when(in_range(bwd_m + 1) & jnp.logical_not(is_last))
        def _():
            for copy in bin_copies(bwd_m + 1):
                copy.start()

        return carry

    lax.fori_loop(0, n_seq + 2 * n_stages - 1, tick, 0)

    def send_loss():
        return pltpu.make_async_remote_copy(
            src_ref=loss_ref, dst_ref=loss_ref, send_sem=loss_sem.at[0], recv_sem=loss_sem.at[1],
            device_id={'stage': prv}, device_id_type=MESH_ID)

    @pl.when(is_last)
    def _():
        lanes = loss_ref.shape[1]
        total = loss_acc[:, 0:lanes]
        for col in range(lanes, loss_acc.shape[1], lanes):
            total = total + loss_acc[:, col:col + lanes]
        loss_ref[...] = total

    @pl.when(jnp.logical_not(is_last))
    def _():
        send_loss().wait_recv()

    @pl.when(jnp.logical_not(is_first))
    def _():
        send_loss().start()
        send_loss().wait_send()


def run_pipeline(n_stages, grad_scale, embeds, targets, wqkv, wout, wup, wdown, heads, hdim):
    n_seq, tokens, width = embeds.shape
    ffn = wdown.shape[0]
    dims = (heads, hdim, 512 if ffn % 512 == 0 else ffn)
    bf16, f32 = jnp.bfloat16, jnp.float32
    total = n_seq * tokens
    out_shapes = [
        ((8, 128), f32),
        ((total, width), bf16),
        ((total, width), bf16),
        ((total, ffn), bf16),
        ((width, total), bf16),
        ((3 * width, total), bf16),
        ((total, ffn), bf16),
        ((total, width), bf16),
        ((total, width), bf16),
        ((n_seq, tokens, width), bf16),
        ((n_seq, 3 * width, tokens), bf16),
        ((n_seq, tokens, ffn), f32),
        ((n_seq, tokens, width), bf16),
        ((n_seq, heads, 8, tokens), f32),
    ]
    any_spec = pl.BlockSpec(memory_space=pl.ANY)
    scratch = [
        pltpu.VMEM(wqkv.shape, bf16), pltpu.VMEM(wout.shape, bf16), pltpu.VMEM(wup.shape, bf16), pltpu.VMEM(wdown.shape, bf16),
        pltpu.VMEM((n_seq, tokens, width), bf16), pltpu.VMEM((n_seq, tokens, width), bf16),
        pltpu.VMEM((2, tokens, width), bf16), pltpu.VMEM((2, tokens, width), bf16),
        pltpu.VMEM((2, tokens, width), bf16), pltpu.VMEM((2, tokens, width), bf16),
        pltpu.VMEM((2, tokens, ffn), bf16), pltpu.VMEM((2, width, tokens), bf16),
        pltpu.VMEM((3, 3 * width, tokens), bf16), pltpu.VMEM((3, tokens, ffn), f32),
        pltpu.VMEM((3, tokens, width), bf16), pltpu.VMEM((3, heads, 8, tokens), f32),
        pltpu.VMEM((2, tokens, ffn), bf16), pltpu.VMEM((2, tokens, width), bf16),
        pltpu.VMEM((width, tokens), bf16), pltpu.VMEM((2, 3 * width, tokens), bf16),
        pltpu.SemaphoreType.DMA((4,)), pltpu.SemaphoreType.DMA((n_seq,)),
        pltpu.SemaphoreType.DMA((n_seq,)), pltpu.SemaphoreType.DMA((n_seq,)),
        pltpu.SemaphoreType.DMA((2, 8)), pltpu.SemaphoreType.DMA((4,)), pltpu.SemaphoreType.DMA((2, 4)),
        pltpu.SemaphoreType.DMA((2,)), pltpu.SemaphoreType.DMA((2,)),
        pltpu.VMEM((8, width), f32), pltpu.SemaphoreType.DMA((2,)),
    ]
    linear = 2 * total * (wqkv.size + wout.size + wup.size + wdown.size)
    return pl.pallas_call(
        functools.partial(pipeline_kernel, (n_stages, n_seq, tokens, grad_scale, dims)),
        out_shape=[jax.ShapeDtypeStruct(s, d) for s, d in out_shapes],
        in_specs=[any_spec] * 6,
        out_specs=[pl.BlockSpec(memory_space=pltpu.VMEM)] + [any_spec] * (len(out_shapes) - 1),
        scratch_shapes=scratch,
        compiler_params=pltpu.CompilerParams(collective_id=0, has_side_effects=True, vmem_limit_bytes=67043328),
        cost_estimate=pl.CostEstimate(flops=3 * linear, bytes_accessed=200 * 2 ** 20, transcendentals=0),
        name='stage_pipeline',
    )(embeds, targets, wqkv, wout, wup, wdown)


def reduce_kernel(
    cfg,
    loss_hbm, ctx_hbm, dhid_hbm, dqkv_hbm, n1_hbm, up_hbm, g_hbm, n2_hbm, dpre_hbm, dx_hbm,
    loss_ref, dout_hbm, dqkvw_hbm, ddown_hbm, dup_hbm, demb_hbm,
    out_res, qkv_res, down_res, up_res, out_in, qkv_in, down_in, up_in, out_sl, qkv_sl, down_sl, up_sl, loss_sl,
    res_sem, in_sem, rs_send, rs_recv, ag_send, ag_recv, store_sem, dx_sem, loss_send, loss_recv, loss_in,
):
    n_data, n_stages = cfg
    rank = lax.axis_index('data')
    stage = lax.axis_index('stage')
    right = lax.rem(rank + 1, n_data)
    left = lax.rem(rank + n_data - 1, n_data)
    toward = (right, left)
    last = n_data - 1

    kinds = (
        ('rows', dhid_hbm, out_res, ctx_hbm, out_in, out_sl, dout_hbm),
        ('rows', n1_hbm, qkv_res, dqkv_hbm, qkv_in, qkv_sl, dqkvw_hbm),
        ('tall', g_hbm, down_res, up_hbm, down_in, down_sl, ddown_hbm),
        ('wide', n2_hbm, up_res, dpre_hbm, up_in, up_sl, dup_hbm),
    )
    order = ((0, 0), (0, 1), (1, 0), (1, 1), (2, 0), (3, 0), (2, 1), (3, 1))

    def owner_of(step, way):
        turn = step + 1
        return lax.rem(rank + (n_data - turn if way == 0 else turn), n_data)

    def piece(kind, way, owner):
        size = kinds[kind][4].shape[1 if kinds[kind][0] == 'rows' else 2]
        return pl.ds(pl.multiple_of((way * n_data + owner) * size, size), size)

    def read_piece(kind, way, step):
        form, _, _, src, buf, _, _ = kinds[kind]
        part = piece(kind, way, owner_of(step, way))
        view = src.at[part, :] if form == 'rows' else src.at[:, part]
        buf_idx = way if buf.shape[0] == 2 else 0
        return pltpu.make_async_copy(view, buf.at[buf_idx], in_sem.at[kind, buf_idx])

    def out_view(kind, way, owner):
        part = piece(kind, way, owner)
        dst = kinds[kind][6]
        return dst.at[:, part] if kinds[kind][0] == 'wide' else dst.at[part, :]

    def pass_sum(kind, way, step):
        slots = kinds[kind][5]
        return pltpu.make_async_remote_copy(
            src_ref=slots.at[step, way], dst_ref=slots.at[step + 1, way], send_sem=rs_send.at[step, kind, way],
            recv_sem=rs_recv.at[step, kind, way], device_id={'data': toward[way]}, device_id_type=MESH_ID)

    def share(kind, way, step):
        owner = lax.rem(rank + (n_data - step if way == 0 else step), n_data)
        view = out_view(kind, way, owner)
        return pltpu.make_async_remote_copy(
            src_ref=kinds[kind][5].at[last, way] if step == 0 else view, dst_ref=view,
            send_sem=ag_send.at[step, kind, way], recv_sem=ag_recv.at[step, kind, way],
            device_id={'data': toward[way]}, device_id_type=MESH_ID)

    def shared_in(kind, way, step):
        owner = lax.rem(rank + (n_data - step - 1 if way == 0 else step + 1), n_data)
        view = out_view(kind, way, owner)
        return pltpu.make_async_remote_copy(
            src_ref=view, dst_ref=view, send_sem=ag_send.at[step, kind, way], recv_sem=ag_recv.at[step, kind, way],
            device_id={'data': toward[way]}, device_id_type=MESH_ID)

    def keep(kind, way):
        return pltpu.make_async_copy(kinds[kind][5].at[last, way], out_view(kind, way, rank), store_sem.at[kind, way])

    def load_resident(kind):
        return pltpu.make_async_copy(kinds[kind][1], kinds[kind][2], res_sem.at[kind])

    my_loss = pltpu.make_async_copy(loss_hbm, loss_sl.at[rank], loss_in)
    my_loss.start()
    for kind in range(len(kinds)):
        load_resident(kind).start()
        for way in range(kinds[kind][4].shape[0]):
            read_piece(kind, way, 0).start()

    spans = []
    span = n_stages // 2
    while span >= 1:
        spans.append(span)
        span //= 2
    barrier = pltpu.get_barrier_semaphore()
    for turn in range(1, n_data):
        pl.semaphore_signal(barrier, inc=1, device_id={'data': lax.rem(rank + turn, n_data)}, device_id_type=MESH_ID)
    for span in spans:
        upper = lax.rem(lax.div(stage, span), 2)
        pl.semaphore_signal(barrier, inc=1, device_id={'stage': stage + span - 2 * span * upper}, device_id_type=MESH_ID)
    pl.semaphore_wait(barrier, n_data - 1 + len(spans))

    def send_loss(turn):
        return pltpu.make_async_remote_copy(
            src_ref=loss_sl.at[rank], dst_ref=loss_sl.at[rank], send_sem=loss_send.at[turn - 1], recv_sem=loss_recv.at[turn - 1],
            device_id={'data': lax.rem(rank + turn, n_data)}, device_id_type=MESH_ID)

    def loss_arrival(turn):
        sender = lax.rem(rank + n_data - turn, n_data)
        return pltpu.make_async_remote_copy(
            src_ref=loss_sl.at[sender], dst_ref=loss_sl.at[sender], send_sem=loss_send.at[turn - 1], recv_sem=loss_recv.at[turn - 1],
            device_id={'data': lax.rem(rank + turn, n_data)}, device_id_type=MESH_ID)

    my_loss.wait()
    for turn in range(1, n_data):
        send_loss(turn).start()

    def spread(idx):
        return pltpu.make_async_remote_copy(
            src_ref=demb_hbm, dst_ref=demb_hbm, send_sem=dx_sem.at[0, idx], recv_sem=dx_sem.at[1, idx],
            device_id={'stage': lax.rem(stage + spans[idx], n_stages)}, device_id_type=MESH_ID)

    def sends_at(idx):
        return lax.rem(stage, 2 * spans[idx]) == 0

    def receives_at(idx):
        return lax.rem(stage, 2 * spans[idx]) == spans[idx]

    def spread_round(idx):
        if idx > 0:
            @pl.when(receives_at(idx - 1))
            def _():
                spread(idx - 1).wait_recv()
        if idx < len(spans):
            @pl.when(sends_at(idx))
            def _():
                spread(idx).start()

    for kind in range(len(kinds)):
        slots = kinds[kind][5]
        for way in range(2):
            slots[0, way] = jnp.zeros(slots.shape[2:], slots.dtype)

    def add_product(kind, way, step):
        form, _, res, _, buf, slots, _ = kinds[kind]
        fed = buf.at[way if buf.shape[0] == 2 else 0]
        tile = min(256, res.shape[1])

        def body(n, carry):
            cols = pl.ds(pl.multiple_of(n * tile, tile), tile)
            if form == 'rows':
                slots[step, way, :, cols] += dot_nn(fed[...], res[:, cols])
            elif form == 'tall':
                slots[step, way, :, cols] += dot_tn(fed[...], res[:, cols])
            else:
                slots[step, way, cols, :] += dot_tn(res[:, cols], fed[...])
            return carry

        lax.fori_loop(0, res.shape[1] // tile, body, 0)

    def ring_step(step, carry):
        for kind, way in order:
            @pl.when(step == 0)
            def _():
                if way == 0:
                    load_resident(kind).wait()

            read_piece(kind, way, step).wait()

            @pl.when(step > 0)
            def _():
                pass_sum(kind, way, step - 1).wait_recv()

            add_product(kind, way, step)
            if kinds[kind][4].shape[0] == 2:
                @pl.when(step < last)
                def _():
                    read_piece(kind, way, step + 1).start()
            elif way == 0:
                read_piece(kind, 1, step).start()
            else:
                @pl.when(step < last)
                def _():
                    read_piece(kind, 0, step + 1).start()

            @pl.when(step < last)
            def _():
                pass_sum(kind, way, step).start()

            @pl.when(step == last)
            def _():
                keep(kind, way).start()
                share(kind, way, 0).start()

        for idx in range(min(last, len(spans))):
            @pl.when(step == idx)
            def _():
                spread_round(idx)
        return carry

    lax.fori_loop(0, n_data, ring_step, 0)

    for idx in range(min(last, len(spans)), len(spans) + 1):
        spread_round(idx)
    for step in range(1, last):
        for kind, way in order:
            shared_in(kind, way, step - 1).wait_recv()
            share(kind, way, step).start()

    for turn in range(1, n_data):
        loss_arrival(turn).wait_recv()
    total = loss_sl[0]
    for idx in range(1, n_data):
        total = total + loss_sl[idx]
    loss_ref[...] = total

    for kind, way in order:
        shared_in(kind, way, last - 1).wait_recv()
    for kind, way in order:
        keep(kind, way).wait()
        for step in range(last):
            pass_sum(kind, way, step).wait_send()
            share(kind, way, step).wait_send()
    for turn in range(1, n_data):
        send_loss(turn).wait_send()
    for idx in range(len(spans)):
        @pl.when(sends_at(idx))
        def _():
            spread(idx).wait_send()


def sum_gradients(n_data, n_stages, loss_part, ctx_t, dhid, dqkv_t, n1, upper, grads, n2, dpre, dx):
    bf16, f32 = jnp.bfloat16, jnp.float32
    total, width = n1.shape
    ffn = upper.shape[1]
    small, mid, big = width // (2 * n_data), 3 * width // (2 * n_data), ffn // (2 * n_data)
    any_spec = pl.BlockSpec(memory_space=pl.ANY)
    vmem_spec = pl.BlockSpec(memory_space=pltpu.VMEM)
    out_shapes = [(loss_part.shape, f32), ((width, width), f32), ((3 * width, width), f32), ((ffn, width), f32), ((width, ffn), f32), (dx.shape, bf16)]
    n_spans = max(1, n_stages.bit_length() - 1)
    scratch = [
        pltpu.VMEM((total, width), bf16), pltpu.VMEM((total, width), bf16), pltpu.VMEM((total, width), bf16), pltpu.VMEM((total, width), bf16),
        pltpu.VMEM((2, small, total), bf16), pltpu.VMEM((2, mid, total), bf16),
        pltpu.VMEM((1, total, big), bf16), pltpu.VMEM((1, total, big), bf16),
        pltpu.VMEM((n_data, 2, small, width), f32), pltpu.VMEM((n_data, 2, mid, width), f32),
        pltpu.VMEM((n_data, 2, big, width), f32), pltpu.VMEM((n_data, 2, width, big), f32),
        pltpu.VMEM((n_data,) + loss_part.shape, f32),
        pltpu.SemaphoreType.DMA((4,)), pltpu.SemaphoreType.DMA((4, 2)),
        pltpu.SemaphoreType.DMA((n_data - 1, 4, 2)), pltpu.SemaphoreType.DMA((n_data - 1, 4, 2)),
        pltpu.SemaphoreType.DMA((n_data - 1, 4, 2)), pltpu.SemaphoreType.DMA((n_data - 1, 4, 2)),
        pltpu.SemaphoreType.DMA((4, 2)), pltpu.SemaphoreType.DMA((2, n_spans)),
        pltpu.SemaphoreType.DMA((n_data - 1,)), pltpu.SemaphoreType.DMA((n_data - 1,)), pltpu.SemaphoreType.DMA(()),
    ]
    flops = 2 * total * width * (4 * width + 2 * ffn)
    return pl.pallas_call(
        functools.partial(reduce_kernel, (n_data, n_stages)),
        out_shape=[jax.ShapeDtypeStruct(s, d) for s, d in out_shapes],
        in_specs=[any_spec] * 10,
        out_specs=[vmem_spec] + [any_spec] * 5,
        scratch_shapes=scratch,
        input_output_aliases={9: 5},
        compiler_params=pltpu.CompilerParams(collective_id=1, has_side_effects=True, vmem_limit_bytes=67043328),
        cost_estimate=pl.CostEstimate(flops=flops, bytes_accessed=150 * 2 ** 20, transcendentals=0),
        name='gradient_sums',
    )(loss_part, ctx_t, dhid, dqkv_t, n1, upper, grads, n2, dpre, dx)


def solution(mesh):
    n_stages = mesh.shape['stage']
    n_data = mesh.shape['data']
    act_spec = P(('rep', 'data'))
    weight_spec = P(('rep', 'stage'))

    def per_device(embeds, targets, w_qkv, w_out, w_up, w_down):
        n_micro, micro_b, seq_len, width = embeds.shape
        heads, hdim = w_qkv.shape[2], w_qkv.shape[3]
        grad_scale = 1.0 / (n_data * n_micro)
        loss_norm = 1.0 / (n_data * n_micro * micro_b * seq_len * width)
        flat = (n_micro * micro_b, seq_len, width)
        outs = run_pipeline(
            n_stages, grad_scale, embeds.reshape(flat), targets.reshape(flat), w_qkv.reshape(3 * width, width),
            w_out.reshape(width, width), w_up[0], w_down[0], heads, hdim)
        loss_part, n1, n2, upper, ctx_t, dqkv_t, dpre, dhid, grads, dx = outs[:10]
        loss_sum, d_out, d_qkv, d_down, d_up, d_embeds = sum_gradients(
            n_data, n_stages, loss_part, ctx_t, dhid, dqkv_t, n1, upper, grads, n2, dpre, dx)
        loss = (0.5 * loss_norm * jnp.sum(loss_sum)).reshape(1)
        return (loss, d_qkv.reshape(w_qkv.shape), d_out.reshape(w_out.shape), d_up[None], d_down[None], d_embeds.reshape(embeds.shape))

    return jax.shard_map(per_device, mesh=mesh, in_specs=(act_spec, act_spec, weight_spec, weight_spec, weight_spec, weight_spec), out_specs=(P('rep'), weight_spec, weight_spec, weight_spec, weight_spec, act_spec), check_vma=False)
```

```python
import functools

import jax
import jax.numpy as jnp
from jax import lax
from jax.experimental import pallas as pl
from jax.experimental.pallas import tpu as pltpu
from jax.sharding import PartitionSpec as P

NORM_EPS = 1e-6
LOG2E = 1.4426950408889634
GELU_C = 0.7978845608028654
GELU_A = 0.044715
MESH_ID = pl.DeviceIdType.MESH


def dot_nn(lhs, rhs):
    return lax.dot_general(lhs, rhs, (((1,), (0,)), ((), ())), preferred_element_type=jnp.float32)


def dot_nt(lhs, rhs):
    return lax.dot_general(lhs, rhs, (((1,), (1,)), ((), ())), preferred_element_type=jnp.float32)


def dot_tn(lhs, rhs):
    return lax.dot_general(lhs, rhs, (((0,), (0,)), ((), ())), preferred_element_type=jnp.float32)


def rms_scale(vals):
    return lax.rsqrt(jnp.mean(vals * vals, axis=-1, keepdims=True) + NORM_EPS)


def rms_vjp(vals, cotangent):
    scale = rms_scale(vals)
    inner = jnp.mean(vals * cotangent, axis=-1, keepdims=True)
    return scale * (cotangent - vals * (scale * scale * inner))


def causal_weights(scores_t, col_max, col_inv, scale):
    half = scores_t.shape[0] // 2
    diag = lax.broadcasted_iota(jnp.int32, (half, half), 0) <= lax.broadcasted_iota(jnp.int32, (half, half), 1)
    upper_l = jnp.where(diag, scores_t[:half, :half], -1e30)
    upper_r = scores_t[:half, half:]
    lower_r = jnp.where(diag, scores_t[half:, half:], -1e30)
    fresh = col_max is None
    if fresh:
        max_l = jnp.max(upper_l, axis=0, keepdims=True)
        max_r = jnp.maximum(jnp.max(upper_r, axis=0, keepdims=True), jnp.max(lower_r, axis=0, keepdims=True))
    else:
        max_l, max_r = col_max[:, :half], col_max[:, half:]
    factor = scale * LOG2E
    exp_ul = jnp.exp2((upper_l - max_l) * factor)
    exp_ur = jnp.exp2((upper_r - max_r) * factor)
    exp_lr = jnp.exp2((lower_r - max_r) * factor)
    if fresh:
        inv_l = 1.0 / jnp.sum(exp_ul, axis=0, keepdims=True)
        inv_r = 1.0 / (jnp.sum(exp_ur, axis=0, keepdims=True) + jnp.sum(exp_lr, axis=0, keepdims=True))
        stats = (jnp.concatenate([max_l, max_r], axis=1), jnp.concatenate([inv_l, inv_r], axis=1))
    else:
        inv_l, inv_r = col_inv[:, :half], col_inv[:, half:]
        stats = None
    return (exp_ul * inv_l, exp_ur * inv_r, exp_lr * inv_r), stats


def assemble(blocks, dtype):
    upper_l, upper_r, lower_r = (b.astype(dtype) for b in blocks)
    upper = jnp.concatenate([upper_l, upper_r], axis=1)
    lower = jnp.concatenate([jnp.zeros_like(upper_l), lower_r], axis=1)
    return jnp.concatenate([upper, lower], axis=0)


def forward_layer(dims, act_ref, wqkv, wout, wup, wdown, n1_ref, qkv_ref, stat_ref, ctx_ref, hid_ref, n2_ref, gp_ref, up_ref, out_ref, flush):
    heads, hdim, ffn_tile = dims
    width = heads * hdim
    ffn = wdown.shape[0]
    scale = hdim ** -0.5
    act32 = act_ref[...].astype(jnp.float32)
    normed1 = (act32 * rms_scale(act32)).astype(jnp.bfloat16)
    n1_ref[...] = normed1
    qkv_ref[...] = dot_nt(wqkv[...], normed1).astype(jnp.bfloat16)
    flush(0)

    def head_body(h, carry):
        q_rows = pl.ds(pl.multiple_of(h * hdim, hdim), hdim)
        k_rows = pl.ds(pl.multiple_of(width + h * hdim, hdim), hdim)
        v_rows = pl.ds(pl.multiple_of(2 * width + h * hdim, hdim), hdim)
        scores_t = dot_tn(qkv_ref[k_rows, :], qkv_ref[q_rows, :])
        blocks, stats = causal_weights(scores_t, None, None, scale)
        stat_ref[h, 0:1, :] = stats[0]
        stat_ref[h, 1:2, :] = stats[1]
        ctx_ref[q_rows, :] = dot_nn(qkv_ref[v_rows, :], assemble(blocks, jnp.bfloat16)).astype(jnp.bfloat16)
        return carry

    lax.fori_loop(0, heads, head_body, 0, unroll=True)
    attn = dot_tn(ctx_ref[...], wout[...])
    hid16 = (act_ref[...].astype(jnp.float32) + attn).astype(jnp.bfloat16)
    hid_ref[...] = hid16
    hid32 = hid16.astype(jnp.float32)
    normed2 = (hid32 * rms_scale(hid32)).astype(jnp.bfloat16)
    n2_ref[...] = normed2
    flush(1)
    for tile in range(ffn // ffn_tile):
        cols = pl.ds(tile * ffn_tile, ffn_tile)
        pre = dot_nn(normed2, wup[:, cols])
        gp_ref[:, cols] = pre
        tanh = jnp.tanh(pre * (GELU_C + (GELU_C * GELU_A) * (pre * pre)))
        up_ref[:, cols] = (pre * (0.5 + 0.5 * tanh)).astype(jnp.bfloat16)
    flush(2)
    down = dot_nn(up_ref[...], wdown[...])
    out_ref[...] = (hid_ref[...].astype(jnp.float32) + down).astype(jnp.bfloat16)


def backward_layer(dims, grad_ref, act_ref, wqkv, wout, wup, wdown, qkv_ref, stat_ref, hid_ref, gp_ref, dpre_ref, dhid_ref, dctx_ref, dqkv_ref, dact_ref, flush):
    heads, hdim, ffn_tile = dims
    width = heads * hdim
    ffn = wdown.shape[0]
    scale = hdim ** -0.5
    grad16 = grad_ref[...]
    for tile in range(ffn // ffn_tile):
        cols = pl.ds(tile * ffn_tile, ffn_tile)
        dup = dot_nt(grad16, wdown[cols, :])
        pre = gp_ref[:, cols]
        pre_sq = pre * pre
        tanh = jnp.tanh(pre * (GELU_C + (GELU_C * GELU_A) * pre_sq))
        half = 0.5 + 0.5 * tanh
        bend = (half * (1.0 - half)) * (pre * (2.0 * GELU_C + (6.0 * GELU_C * GELU_A) * pre_sq))
        dpre_ref[:, cols] = (dup * (half + bend)).astype(jnp.bfloat16)
    flush(0)
    dnormed2 = dot_nt(dpre_ref[...], wup[...])
    dhid32 = grad_ref[...].astype(jnp.float32) + rms_vjp(hid_ref[...].astype(jnp.float32), dnormed2)
    dhid16 = dhid32.astype(jnp.bfloat16)
    dhid_ref[...] = dhid16
    flush(1)
    dctx_ref[...] = dot_nt(wout[...], dhid16).astype(jnp.bfloat16)

    def head_body(h, carry):
        q_rows = pl.ds(pl.multiple_of(h * hdim, hdim), hdim)
        k_rows = pl.ds(pl.multiple_of(width + h * hdim, hdim), hdim)
        v_rows = pl.ds(pl.multiple_of(2 * width + h * hdim, hdim), hdim)
        query_t = qkv_ref[q_rows, :]
        keys_t = qkv_ref[k_rows, :]
        dctx_t = dctx_ref[q_rows, :]
        scores_t = dot_tn(keys_t, query_t)
        probs, _ = causal_weights(scores_t, stat_ref[h, 0:1, :], stat_ref[h, 1:2, :], scale)
        dprobs = dot_tn(qkv_ref[v_rows, :], dctx_t)
        half = dprobs.shape[0] // 2
        d_ul, d_ur, d_lr = dprobs[:half, :half], dprobs[:half, half:], dprobs[half:, half:]
        p_ul, p_ur, p_lr = probs
        delta_l = jnp.sum(d_ul * p_ul, axis=0, keepdims=True)
        delta_r = jnp.sum(d_ur * p_ur, axis=0, keepdims=True) + jnp.sum(d_lr * p_lr, axis=0, keepdims=True)
        dscores = assemble((p_ul * (d_ul - delta_l) * scale, p_ur * (d_ur - delta_r) * scale, p_lr * (d_lr - delta_r) * scale), jnp.bfloat16)
        dqkv_ref[v_rows, :] = dot_nt(dctx_t, assemble(probs, jnp.bfloat16)).astype(jnp.bfloat16)
        dqkv_ref[q_rows, :] = dot_nn(keys_t, dscores).astype(jnp.bfloat16)
        dqkv_ref[k_rows, :] = dot_nt(query_t, dscores).astype(jnp.bfloat16)
        return carry

    lax.fori_loop(0, heads, head_body, 0, unroll=True)
    flush(2)
    dnormed1 = dot_tn(dqkv_ref[...], wqkv[...])
    dact = dhid32 + rms_vjp(act_ref[...].astype(jnp.float32), dnormed1)
    dact_ref[...] = dact.astype(jnp.bfloat16)


class placement:
    def __init__(self, n_stages):
        row = lax.axis_index('data')
        self.row = row
        self.index = lax.axis_index('stage')
        self.column = lax.div(self.index, 2)
        self.core = lax.rem(self.index, 2)
        self.upper = lax.div(row, 2)
        self.half = lax.rem(self.upper + self.column, 2)
        self.layer = 2 * self.column + self.half
        self.home = self.layer
        self.mate = 2 * self.column + 1 - self.core
        across = 3 - row
        along = lax.rem(self.index + jnp.where(self.half == 1, 2, n_stages - 2), n_stages)
        self.mate_id = {'data': row, 'stage': self.mate}
        self.across_id = {'data': across, 'stage': self.index}
        self.along_id = {'data': row, 'stage': along}
        self.next_id = {'data': jnp.where(self.half == 1, row, across), 'stage': jnp.where(self.half == 1, along, self.index)}
        self.prev_id = {'data': jnp.where(self.half == 1, across, row), 'stage': jnp.where(self.half == 1, self.index, along)}


def pipeline_kernel(
    cfg,
    emb_hbm, tgt_hbm, wqkv_hbm, wout_hbm, wup_hbm, wdown_hbm,
    loss_ref, n1_hbm, n2_hbm, up_hbm, ctx_hbm, dqkv_hbm, dpre_hbm, dhid_hbm, g_hbm, dx_hbm, qkv_hbm, gp_hbm, hid_hbm, stat_hbm,
    wqkv, wout, wup, wdown, act, grad, out_s, dact_s,
    n1_s, n2_s, up_s, ctx_s, qkv_s, gp_s, hid_s, stat_s,
    dpre_s, dhid_s, dctx_s, dqkv_s,
    w_sem, in_sem, act_sem, grad_sem, fout_sem, bin_sem, bout_sem, fsend_sem, bsend_sem, loss_acc, loss_sem, dx_sem,
):
    n_stages, n_seq, tokens, grad_scale, dims = cfg
    here = placement(n_stages)
    stage, core, next_id, prev_id = here.layer, here.core, here.next_id, here.prev_id
    is_first = stage == 0
    is_last = stage == n_stages - 1
    own_weights = here.layer == here.index
    own_data = here.upper == core
    feeds_first = (here.column == 0) & (here.half == 1) & (core == 1)
    feeds_last = (here.column == n_stages // 2 - 1) & (here.half == 0) & (core == 1)

    weight_pairs = ((wqkv_hbm, wqkv), (wout_hbm, wout), (wup_hbm, wup), (wdown_hbm, wdown))

    def load_weight(idx):
        return pltpu.make_async_copy(weight_pairs[idx][0], weight_pairs[idx][1], w_sem.at[idx])

    def give_weight(idx):
        return pltpu.make_async_remote_copy(
            src_ref=weight_pairs[idx][0], dst_ref=weight_pairs[idx][1], send_sem=w_sem.at[4 + idx], recv_sem=w_sem.at[8 + idx],
            device_id=here.mate_id, device_id_type=MESH_ID)

    def load_embed(m):
        return pltpu.make_async_copy(emb_hbm.at[m], act.at[m], in_sem.at[m])

    def load_target(m):
        return pltpu.make_async_copy(tgt_hbm.at[m], grad.at[m], in_sem.at[m])

    def give_embed(m):
        return pltpu.make_async_remote_copy(
            src_ref=emb_hbm.at[m], dst_ref=act.at[m], send_sem=in_sem.at[m], recv_sem=act_sem.at[m],
            device_id=here.across_id, device_id_type=MESH_ID)

    def give_target(m):
        return pltpu.make_async_remote_copy(
            src_ref=tgt_hbm.at[m], dst_ref=grad.at[m], send_sem=in_sem.at[m], recv_sem=grad_sem.at[m],
            device_id=here.across_id, device_id_type=MESH_ID)

    def each_seq(when, action):
        @pl.when(when)
        def _():
            def go(m, carry):
                action(m)
                return carry
            lax.fori_loop(0, n_seq, go, 0)

    @pl.when(own_weights)
    def _():
        for idx in range(4):
            load_weight(idx).start()

    each_seq(is_first & own_data, lambda m: load_embed(m).start())
    each_seq(is_last & own_data, lambda m: load_target(m).start())

    barrier = pltpu.get_barrier_semaphore()
    for peer in (here.mate_id, here.across_id, here.along_id):
        pl.semaphore_signal(barrier, inc=1, device_id=peer, device_id_type=MESH_ID)
    pl.semaphore_wait(barrier, 3)

    @pl.when(own_weights)
    def _():
        for idx in range(4):
            give_weight(idx).start()

    each_seq(feeds_first, lambda m: give_embed(m).start())
    each_seq(feeds_last, lambda m: give_target(m).start())
    loss_acc[...] = jnp.zeros_like(loss_acc)

    @pl.when(own_weights)
    def _():
        for idx in range(4):
            load_weight(idx).wait()

    @pl.when(jnp.logical_not(own_weights))
    def _():
        for idx in range(4):
            give_weight(idx).wait_recv()

    def send_act(m, slot):
        return pltpu.make_async_remote_copy(
            src_ref=out_s.at[slot], dst_ref=act.at[m], send_sem=fsend_sem.at[slot], recv_sem=act_sem.at[m],
            device_id=next_id, device_id_type=MESH_ID)

    def send_grad(m, slot):
        return pltpu.make_async_remote_copy(
            src_ref=dact_s.at[slot], dst_ref=grad.at[m], send_sem=bsend_sem.at[slot], recv_sem=grad_sem.at[m],
            device_id=prev_id, device_id_type=MESH_ID)

    def store_dx(m, slot):
        return pltpu.make_async_copy(dact_s.at[slot], dx_hbm.at[m], bsend_sem.at[slot])

    def give_dx(m, slot):
        return pltpu.make_async_remote_copy(
            src_ref=dact_s.at[slot], dst_ref=dx_hbm.at[m], send_sem=bsend_sem.at[slot], recv_sem=dx_sem.at[m],
            device_id=here.across_id, device_id_type=MESH_ID)

    def token_range(m):
        return pl.ds(pl.multiple_of(m * tokens, tokens), tokens)

    def fout_copies(m, slot):
        rows = token_range(m)
        return (
            (0, pltpu.make_async_copy(n1_s.at[slot], n1_hbm.at[rows, :], fout_sem.at[slot, 0])),
            (0, pltpu.make_async_copy(qkv_s.at[slot], qkv_hbm.at[m], fout_sem.at[slot, 1])),
            (1, pltpu.make_async_copy(ctx_s.at[slot], ctx_hbm.at[:, rows], fout_sem.at[slot, 2])),
            (1, pltpu.make_async_copy(stat_s.at[slot], stat_hbm.at[m], fout_sem.at[slot, 3])),
            (1, pltpu.make_async_copy(hid_s.at[slot], hid_hbm.at[m], fout_sem.at[slot, 4])),
            (1, pltpu.make_async_copy(n2_s.at[slot], n2_hbm.at[rows, :], fout_sem.at[slot, 5])),
            (2, pltpu.make_async_copy(gp_s.at[slot], gp_hbm.at[m], fout_sem.at[slot, 6])),
            (2, pltpu.make_async_copy(up_s.at[slot], up_hbm.at[rows, :], fout_sem.at[slot, 7])),
        )

    def bin_copies(m):
        return (
            pltpu.make_async_copy(qkv_hbm.at[m], qkv_s.at[2], bin_sem.at[0]),
            pltpu.make_async_copy(stat_hbm.at[m], stat_s.at[2], bin_sem.at[1]),
            pltpu.make_async_copy(hid_hbm.at[m], hid_s.at[2], bin_sem.at[2]),
            pltpu.make_async_copy(gp_hbm.at[m], gp_s.at[2], bin_sem.at[3]),
        )

    def bout_copies(m, slot):
        rows = token_range(m)
        return (
            (0, pltpu.make_async_copy(grad.at[m], g_hbm.at[rows, :], bout_sem.at[slot, 0])),
            (0, pltpu.make_async_copy(dpre_s.at[slot], dpre_hbm.at[rows, :], bout_sem.at[slot, 1])),
            (1, pltpu.make_async_copy(dhid_s.at[slot], dhid_hbm.at[rows, :], bout_sem.at[slot, 2])),
            (2, pltpu.make_async_copy(dqkv_s.at[slot], dqkv_hbm.at[:, rows], bout_sem.at[slot, 3])),
        )

    def flusher(copies):
        def flush(group):
            for when, copy in copies:
                if when == group:
                    copy.start()
        return flush

    def in_range(m):
        return (m >= 0) & (m < n_seq)

    def tick(t, carry):
        fwd_m = t - stage
        bwd_m = t + stage - (2 * n_stages - 2)

        @pl.when(in_range(fwd_m))
        def _():
            m = fwd_m
            slot = lax.rem(m, 2)

            @pl.when(is_first & own_data)
            def _():
                load_embed(m).wait()

            @pl.when(jnp.logical_not(is_first & own_data))
            def _():
                send_act(m, slot).wait_recv()

            forward_layer(
                dims, act.at[m], wqkv, wout, wup, wdown, n1_s.at[slot], qkv_s.at[slot], stat_s.at[slot],
                ctx_s.at[slot], hid_s.at[slot], n2_s.at[slot], gp_s.at[slot], up_s.at[slot], out_s.at[slot],
                flusher(fout_copies(m, slot)))

            @pl.when(jnp.logical_not(is_last))
            def _():
                send_act(m, slot).start()

            @pl.when(is_last & own_data)
            def _():
                load_target(m).wait()

            @pl.when(is_last & jnp.logical_not(own_data))
            def _():
                send_grad(m, slot).wait_recv()

            @pl.when(is_last)
            def _():
                error = out_s[slot].astype(jnp.float32) - grad[m].astype(jnp.float32)
                square = error * error
                total = square[0:8]
                for row in range(8, tokens, 8):
                    total = total + square[row:row + 8]
                loss_acc[...] += total
                grad[m] = (error * grad_scale).astype(jnp.bfloat16)

        @pl.when(in_range(bwd_m))
        def _():
            m = bwd_m
            slot = lax.rem(m, 2)

            @pl.when(jnp.logical_not(is_last))
            def _():
                for copy in bin_copies(m):
                    copy.wait()
                send_grad(m, slot).wait_recv()

            saved = jnp.where(is_last, slot, 2)
            backward_layer(
                dims, grad.at[m], act.at[m], wqkv, wout, wup, wdown, qkv_s.at[saved], stat_s.at[saved], hid_s.at[saved],
                gp_s.at[saved], dpre_s.at[slot], dhid_s.at[slot], dctx_s, dqkv_s.at[slot], dact_s.at[slot],
                flusher(bout_copies(m, slot)))

            @pl.when(jnp.logical_not(is_first))
            def _():
                send_grad(m, slot).start()

            @pl.when(is_first & own_data)
            def _():
                store_dx(m, slot).start()

            @pl.when(is_first & jnp.logical_not(own_data))
            def _():
                give_dx(m, slot).start()

        fwd_old = fwd_m - 1
        bwd_old = bwd_m - 1

        @pl.when(in_range(fwd_old))
        def _():
            slot = lax.rem(fwd_old, 2)
            for _, copy in fout_copies(fwd_old, slot):
                copy.wait()

            @pl.when(jnp.logical_not(is_last))
            def _():
                send_act(fwd_old, slot).wait_send()

        @pl.when(in_range(bwd_old))
        def _():
            slot = lax.rem(bwd_old, 2)
            for _, copy in bout_copies(bwd_old, slot):
                copy.wait()

            @pl.when(jnp.logical_not(is_first))
            def _():
                send_grad(bwd_old, slot).wait_send()

            @pl.when(is_first & own_data)
            def _():
                store_dx(bwd_old, slot).wait()

            @pl.when(is_first & jnp.logical_not(own_data))
            def _():
                give_dx(bwd_old, slot).wait_send()

        @pl.when(in_range(bwd_m + 1) & jnp.logical_not(is_last))
        def _():
            for copy in bin_copies(bwd_m + 1):
                copy.start()

        return carry

    lax.fori_loop(0, n_seq + 2 * n_stages - 1, tick, 0)

    def send_loss():
        return pltpu.make_async_remote_copy(
            src_ref=loss_ref, dst_ref=loss_ref, send_sem=loss_sem.at[0], recv_sem=loss_sem.at[1],
            device_id=prev_id, device_id_type=MESH_ID)

    @pl.when(is_last)
    def _():
        lanes = loss_ref.shape[1]
        total = loss_acc[:, 0:lanes]
        for col in range(lanes, loss_acc.shape[1], lanes):
            total = total + loss_acc[:, col:col + lanes]
        loss_ref[...] = total

    @pl.when(jnp.logical_not(is_last))
    def _():
        send_loss().wait_recv()

    @pl.when(jnp.logical_not(is_first))
    def _():
        send_loss().start()
        send_loss().wait_send()

    @pl.when(own_weights)
    def _():
        for idx in range(4):
            give_weight(idx).wait_send()

    each_seq(feeds_first, lambda m: give_embed(m).wait_send())
    each_seq(feeds_last, lambda m: give_target(m).wait_send())
    each_seq(feeds_first, lambda m: give_dx(m, 0).wait_recv())


def run_pipeline(n_stages, grad_scale, embeds, targets, wqkv, wout, wup, wdown, heads, hdim):
    n_seq, tokens, width = embeds.shape
    ffn = wdown.shape[0]
    dims = (heads, hdim, 512 if ffn % 512 == 0 else ffn)
    bf16, f32 = jnp.bfloat16, jnp.float32
    total = n_seq * tokens
    out_shapes = [
        ((8, 128), f32),
        ((total, width), bf16),
        ((total, width), bf16),
        ((total, ffn), bf16),
        ((width, total), bf16),
        ((3 * width, total), bf16),
        ((total, ffn), bf16),
        ((total, width), bf16),
        ((total, width), bf16),
        ((n_seq, tokens, width), bf16),
        ((n_seq, 3 * width, tokens), bf16),
        ((n_seq, tokens, ffn), f32),
        ((n_seq, tokens, width), bf16),
        ((n_seq, heads, 8, tokens), f32),
    ]
    any_spec = pl.BlockSpec(memory_space=pl.ANY)
    scratch = [
        pltpu.VMEM(wqkv.shape, bf16), pltpu.VMEM(wout.shape, bf16), pltpu.VMEM(wup.shape, bf16), pltpu.VMEM(wdown.shape, bf16),
        pltpu.VMEM((n_seq, tokens, width), bf16), pltpu.VMEM((n_seq, tokens, width), bf16),
        pltpu.VMEM((2, tokens, width), bf16), pltpu.VMEM((2, tokens, width), bf16),
        pltpu.VMEM((2, tokens, width), bf16), pltpu.VMEM((2, tokens, width), bf16),
        pltpu.VMEM((2, tokens, ffn), bf16), pltpu.VMEM((2, width, tokens), bf16),
        pltpu.VMEM((3, 3 * width, tokens), bf16), pltpu.VMEM((3, tokens, ffn), f32),
        pltpu.VMEM((3, tokens, width), bf16), pltpu.VMEM((3, heads, 8, tokens), f32),
        pltpu.VMEM((2, tokens, ffn), bf16), pltpu.VMEM((2, tokens, width), bf16),
        pltpu.VMEM((width, tokens), bf16), pltpu.VMEM((2, 3 * width, tokens), bf16),
        pltpu.SemaphoreType.DMA((12,)), pltpu.SemaphoreType.DMA((n_seq,)),
        pltpu.SemaphoreType.DMA((n_seq,)), pltpu.SemaphoreType.DMA((n_seq,)),
        pltpu.SemaphoreType.DMA((2, 8)), pltpu.SemaphoreType.DMA((4,)), pltpu.SemaphoreType.DMA((2, 4)),
        pltpu.SemaphoreType.DMA((2,)), pltpu.SemaphoreType.DMA((2,)),
        pltpu.VMEM((8, width), f32), pltpu.SemaphoreType.DMA((2,)), pltpu.SemaphoreType.DMA((n_seq,)),
    ]
    linear = 2 * total * (wqkv.size + wout.size + wup.size + wdown.size)
    return pl.pallas_call(
        functools.partial(pipeline_kernel, (n_stages, n_seq, tokens, grad_scale, dims)),
        out_shape=[jax.ShapeDtypeStruct(s, d) for s, d in out_shapes],
        in_specs=[any_spec] * 6,
        out_specs=[pl.BlockSpec(memory_space=pltpu.VMEM)] + [any_spec] * (len(out_shapes) - 1),
        scratch_shapes=scratch,
        compiler_params=pltpu.CompilerParams(collective_id=0, has_side_effects=True, vmem_limit_bytes=67043328),
        cost_estimate=pl.CostEstimate(flops=3 * linear, bytes_accessed=200 * 2 ** 20, transcendentals=0),
        name='stage_pipeline',
    )(embeds, targets, wqkv, wout, wup, wdown)


def reduce_kernel(
    cfg,
    loss_hbm, ctx_hbm, dhid_hbm, dqkv_hbm, n1_hbm, up_hbm, g_hbm, n2_hbm, dpre_hbm, dx_hbm,
    loss_ref, dout_hbm, dqkvw_hbm, ddown_hbm, dup_hbm, demb_hbm,
    out_res, qkv_res, down_res, up_res, out_in, qkv_in, down_in, up_in,
    out_give, qkv_give, down_give, up_give, out_core, qkv_core, down_core, up_core, out_row, qkv_row, down_row, up_row, loss_sl,
    res_sem, in_sem, give_sem, core_sem, row_send, row_recv, put_send, put_recv, pass_send, store_sem, dx_sem,
    loss_send, loss_recv, loss_in,
):
    (n_stages,) = cfg
    here = placement(n_stages)
    row, core, stage = here.row, here.core, here.index
    pair = lax.rem(row, 2)
    pair_row = row + 1 - 2 * pair
    across = 3 - row
    is_home = here.home == stage
    home_id = {'data': row, 'stage': here.home}
    pair_id = {'data': pair_row, 'stage': stage}
    pair_home_id = {'data': pair_row, 'stage': here.home}
    across_home_id = {'data': across, 'stage': here.home}

    kinds = (
        ('rows', dhid_hbm, out_res, ctx_hbm, out_in, out_give, out_core, out_row, dout_hbm),
        ('rows', n1_hbm, qkv_res, dqkv_hbm, qkv_in, qkv_give, qkv_core, qkv_row, dqkvw_hbm),
        ('tall', g_hbm, down_res, up_hbm, down_in, down_give, down_core, down_row, ddown_hbm),
        ('wide', n2_hbm, up_res, dpre_hbm, up_in, up_give, up_core, up_row, dup_hbm),
    )
    n_kinds = len(kinds)
    turns = ((1, 1), (0, 1), (1, 0), (0, 0))

    def piece(kind, member, unit, num):
        size = kinds[kind][4].shape[1 if kinds[kind][0] == 'rows' else 2]
        return pl.ds(pl.multiple_of(((member * 2 + unit) * 2 + num) * size, size), size)

    def flip(val, by):
        return 1 - val if by else val

    def read_piece(kind, turn, num):
        form, _, _, src, buf = kinds[kind][:5]
        part = piece(kind, flip(pair, turns[turn][0]), flip(core, turns[turn][1]), num)
        view = src.at[part, :] if form == 'rows' else src.at[:, part]
        return pltpu.make_async_copy(view, buf.at[turn % 2], in_sem.at[kind, turn % 2])

    def out_view(kind, member, unit, num):
        part = piece(kind, member, unit, num)
        dst = kinds[kind][8]
        return dst.at[:, part] if kinds[kind][0] == 'wide' else dst.at[part, :]

    def give(kind, other, num):
        return pltpu.make_async_remote_copy(
            src_ref=kinds[kind][5].at[other], dst_ref=kinds[kind][6].at[num, other], send_sem=give_sem.at[kind, other],
            recv_sem=core_sem.at[kind, num, other], device_id=here.mate_id, device_id_type=MESH_ID)

    def send_row(kind, num):
        return pltpu.make_async_remote_copy(
            src_ref=kinds[kind][6].at[num, 1], dst_ref=kinds[kind][7].at[num], send_sem=row_send.at[kind, num],
            recv_sem=row_recv.at[kind, num], device_id=pair_id, device_id_type=MESH_ID)

    def put(kind, num, target, device_id):
        return pltpu.make_async_remote_copy(
            src_ref=kinds[kind][7].at[num], dst_ref=out_view(kind, pair, core, num), send_sem=put_send.at[target, kind, num],
            recv_sem=put_recv.at[pair, core, kind, num], device_id=device_id, device_id_type=MESH_ID)

    def keep(kind, num):
        return pltpu.make_async_copy(kinds[kind][7].at[num], out_view(kind, pair, core, num), store_sem.at[kind, num])

    def arrival(kind, num, member, unit):
        view = out_view(kind, member, unit, num)
        return pltpu.make_async_remote_copy(
            src_ref=view, dst_ref=view, send_sem=pass_send.at[unit, kind, num], recv_sem=put_recv.at[member, unit, kind, num],
            device_id=across_home_id, device_id_type=MESH_ID)

    def load_resident(kind):
        return pltpu.make_async_copy(kinds[kind][1], kinds[kind][2], res_sem.at[kind])

    def pipeline_id(row_idx, unit):
        return 2 * jnp.minimum(row_idx, 3 - row_idx) + unit

    my_loss = pltpu.make_async_copy(loss_hbm, loss_sl.at[pipeline_id(row, core)], loss_in)
    my_loss.start()
    for kind in range(n_kinds):
        load_resident(kind).start()
        read_piece(kind, 0, 0).start()

    source = here.upper
    rank = stage + source - 2 * source * core
    spans = []
    span = n_stages // 2
    while span >= 1:
        spans.append(span)
        span //= 2

    def swapped(span):
        return stage + span - 2 * span * lax.rem(lax.div(stage, span), 2)

    loss_ids = (
        ({'data': row, 'stage': here.mate}, row, 1 - core),
        ({'data': pair_row, 'stage': stage}, pair_row, core),
        ({'data': pair_row, 'stage': here.mate}, pair_row, 1 - core),
    )
    peers = [ident for ident, _, _ in loss_ids]
    peers += [{'data': across, 'stage': stage}, {'data': across, 'stage': here.mate}]
    peers += [{'data': row, 'stage': swapped(span)} for span in spans if span > 1]
    barrier = pltpu.get_barrier_semaphore()
    for ident in peers:
        pl.semaphore_signal(barrier, inc=1, device_id=ident, device_id_type=MESH_ID)
    pl.semaphore_wait(barrier, len(peers))

    def send_loss(idx):
        slot = loss_sl.at[pipeline_id(row, core)]
        return pltpu.make_async_remote_copy(
            src_ref=slot, dst_ref=slot, send_sem=loss_send.at[idx], recv_sem=loss_recv.at[idx],
            device_id=loss_ids[idx][0], device_id_type=MESH_ID)

    def loss_arrival(idx):
        slot = loss_sl.at[pipeline_id(loss_ids[idx][1], loss_ids[idx][2])]
        return pltpu.make_async_remote_copy(
            src_ref=slot, dst_ref=slot, send_sem=loss_send.at[idx], recv_sem=loss_recv.at[idx],
            device_id=loss_ids[idx][0], device_id_type=MESH_ID)

    my_loss.wait()
    for idx in range(3):
        send_loss(idx).start()

    def spread(idx):
        return pltpu.make_async_remote_copy(
            src_ref=demb_hbm, dst_ref=demb_hbm, send_sem=dx_sem.at[0, idx], recv_sem=dx_sem.at[1, idx],
            device_id={'data': row, 'stage': swapped(spans[idx])}, device_id_type=MESH_ID)

    def sends_at(idx):
        return lax.rem(rank, 2 * spans[idx]) == 0

    def receives_at(idx):
        return lax.rem(rank, 2 * spans[idx]) == spans[idx]

    def spread_round(idx):
        if idx > 0:
            @pl.when(receives_at(idx - 1))
            def _():
                spread(idx - 1).wait_recv()
        if idx < len(spans):
            @pl.when(sends_at(idx))
            def _():
                spread(idx).start()

    def product(kind, turn, num, sink, base):
        form, _, res, _, buf = kinds[kind][:5]
        read_piece(kind, turn, num).wait()
        if turn < 3:
            read_piece(kind, turn + 1, num).start()
        else:
            @pl.when(num == 0)
            def _():
                read_piece(kind, 0, 1).start()
        fed = buf.at[turn % 2]
        tile = min(256, res.shape[1])

        def body(n, carry):
            span = pl.ds(pl.multiple_of(n * tile, tile), tile)
            if form == 'rows':
                part, at = dot_nn(fed[...], res[:, span]), (slice(None), span)
            elif form == 'tall':
                part, at = dot_tn(fed[...], res[:, span]), (slice(None), span)
            else:
                part, at = dot_tn(res[:, span], fed[...]), (span, slice(None))
            for ref in base:
                part = part + ref[at]
            sink[at] = part
            return carry

        lax.fori_loop(0, res.shape[1] // tile, body, 0)

    def first_half(kind, num):
        give_buf, core_buf = kinds[kind][5:7]

        @pl.when(num == 0)
        def _():
            load_resident(kind).wait()

        for turn, other in ((0, 1), (1, 0)):
            @pl.when(num > 0)
            def _():
                give(kind, other, num - 1).wait_send()

            product(kind, turn, num, give_buf.at[other], ())
            give(kind, other, num).start()
        give(kind, 1, num).wait_recv()
        product(kind, 2, num, core_buf.at[num, 1], (core_buf.at[num, 1],))
        send_row(kind, num).start()

    def second_half(kind, num):
        core_buf, row_buf = kinds[kind][6:8]
        give(kind, 0, num).wait_recv()
        send_row(kind, num).wait_recv()
        product(kind, 3, num, row_buf.at[num], (core_buf.at[num, 0], row_buf.at[num]))
        put(kind, num, 1, pair_home_id).start()
        put(kind, num, 2, across_home_id).start()

        @pl.when(is_home)
        def _():
            keep(kind, num).start()

        @pl.when(jnp.logical_not(is_home))
        def _():
            put(kind, num, 0, home_id).start()

    def pass_on(kind, num):
        @pl.when(is_home)
        def _():
            for unit in range(2):
                arrival(kind, num, 1 - pair, unit).wait_recv()
                arrival(kind, num, 1 - pair, unit).start()

    def round_body(num, carry):
        for kind in range(n_kinds):
            first_half(kind, num)
            if kind >= 1:
                second_half(kind - 1, num)
            else:
                @pl.when(num > 0)
                def _():
                    second_half(n_kinds - 1, num - 1)
            if kind >= 2:
                pass_on(kind - 2, num)
            else:
                @pl.when(num > 0)
                def _():
                    pass_on(kind + 2, num - 1)
        for idx in range(2):
            if idx < len(spans):
                @pl.when(num == idx)
                def _():
                    spread_round(idx)
        return carry

    lax.fori_loop(0, 2, round_body, 0)
    second_half(n_kinds - 1, 1)
    for idx in range(min(2, len(spans)), len(spans) + 1):
        spread_round(idx)
    pass_on(n_kinds - 2, 1)
    pass_on(n_kinds - 1, 1)

    for idx in range(3):
        loss_arrival(idx).wait_recv()
    total = loss_sl[0]
    for idx in range(1, 4):
        total = total + loss_sl[idx]
    loss_ref[...] = total

    for kind in range(n_kinds):
        for num in range(2):
            @pl.when(is_home)
            def _():
                arrival(kind, num, pair, 1 - core).wait_recv()
                keep(kind, num).wait()
                for unit in range(2):
                    arrival(kind, num, 1 - pair, unit).wait_send()

            @pl.when(jnp.logical_not(is_home))
            def _():
                for member in range(2):
                    for unit in range(2):
                        arrival(kind, num, member, unit).wait_recv()
                put(kind, num, 0, home_id).wait_send()

            send_row(kind, num).wait_send()
            put(kind, num, 1, pair_home_id).wait_send()
            put(kind, num, 2, across_home_id).wait_send()
        for other in range(2):
            give(kind, other, 1).wait_send()
    for idx in range(3):
        send_loss(idx).wait_send()
    for idx in range(len(spans)):
        @pl.when(sends_at(idx))
        def _():
            spread(idx).wait_send()


def sum_gradients(n_stages, loss_part, ctx_t, dhid, dqkv_t, n1, upper, grads, n2, dpre, dx):
    bf16, f32 = jnp.bfloat16, jnp.float32
    total, width = n1.shape
    ffn = upper.shape[1]
    small, mid, big = width // 8, 3 * width // 8, ffn // 8
    any_spec = pl.BlockSpec(memory_space=pl.ANY)
    vmem_spec = pl.BlockSpec(memory_space=pltpu.VMEM)
    out_shapes = [(loss_part.shape, f32), ((width, width), f32), ((3 * width, width), f32), ((ffn, width), f32), ((width, ffn), f32), (dx.shape, bf16)]
    n_spans = n_stages.bit_length() - 1
    pieces = ((small, width), (mid, width), (big, width), (width, big))
    dma = pltpu.SemaphoreType.DMA
    scratch = [pltpu.VMEM((total, width), bf16)] * 4 + [
        pltpu.VMEM((2, small, total), bf16), pltpu.VMEM((2, mid, total), bf16),
        pltpu.VMEM((2, total, big), bf16), pltpu.VMEM((2, total, big), bf16),
    ]
    scratch += [pltpu.VMEM((2,) + p, f32) for p in pieces]
    scratch += [pltpu.VMEM((2, 2) + p, f32) for p in pieces]
    scratch += [pltpu.VMEM((2,) + p, f32) for p in pieces]
    scratch += [
        pltpu.VMEM((4,) + loss_part.shape, f32),
        dma((4,)), dma((4, 2)), dma((4, 2)), dma((4, 2, 2)), dma((4, 2)), dma((4, 2)), dma((3, 4, 2)), dma((2, 2, 4, 2)),
        dma((2, 4, 2)), dma((4, 2)), dma((2, n_spans)), dma((3,)), dma((3,)), dma(()),
    ]
    flops = 2 * total * width * (4 * width + 2 * ffn)
    return pl.pallas_call(
        functools.partial(reduce_kernel, (n_stages,)),
        out_shape=[jax.ShapeDtypeStruct(s, d) for s, d in out_shapes],
        in_specs=[any_spec] * 10,
        out_specs=[vmem_spec] + [any_spec] * 5,
        scratch_shapes=scratch,
        input_output_aliases={9: 5},
        compiler_params=pltpu.CompilerParams(collective_id=1, has_side_effects=True, vmem_limit_bytes=67043328),
        cost_estimate=pl.CostEstimate(flops=flops, bytes_accessed=150 * 2 ** 20, transcendentals=0),
        name='gradient_sums',
    )(loss_part, ctx_t, dhid, dqkv_t, n1, upper, grads, n2, dpre, dx)


def solution(mesh):
    n_stages = mesh.shape['stage']
    n_data = mesh.shape['data']
    act_spec = P(('rep', 'data'))
    weight_spec = P(('rep', 'stage'))

    def per_device(embeds, targets, w_qkv, w_out, w_up, w_down):
        n_micro, micro_b, seq_len, width = embeds.shape
        heads, hdim = w_qkv.shape[2], w_qkv.shape[3]
        grad_scale = 1.0 / (n_data * n_micro)
        loss_norm = 1.0 / (n_data * n_micro * micro_b * seq_len * width)
        flat = (n_micro * micro_b, seq_len, width)
        outs = run_pipeline(
            n_stages, grad_scale, embeds.reshape(flat), targets.reshape(flat), w_qkv.reshape(3 * width, width),
            w_out.reshape(width, width), w_up[0], w_down[0], heads, hdim)
        loss_part, n1, n2, upper, ctx_t, dqkv_t, dpre, dhid, grads, dx = outs[:10]
        loss_sum, d_out, d_qkv, d_down, d_up, d_embeds = sum_gradients(
            n_stages, loss_part, ctx_t, dhid, dqkv_t, n1, upper, grads, n2, dpre, dx)
        loss = (0.5 * loss_norm * jnp.sum(loss_sum)).reshape(1)
        return (loss, d_qkv.reshape(w_qkv.shape), d_out.reshape(w_out.shape), d_up[None], d_down[None], d_embeds.reshape(embeds.shape))

    return jax.shard_map(per_device, mesh=mesh, in_specs=(act_spec, act_spec, weight_spec, weight_spec, weight_spec, weight_spec), out_specs=(P('rep'), weight_spec, weight_spec, weight_spec, weight_spec, act_spec), check_vma=False)
```

```python
import functools

import jax
import jax.numpy as jnp
from jax import lax
from jax.experimental import pallas as pl
from jax.experimental.pallas import tpu as pltpu
from jax.sharding import PartitionSpec as P

NORM_EPS = 1e-6
LOG2E = 1.4426950408889634
GELU_C = 0.7978845608028654
GELU_A = 0.044715
MESH_ID = pl.DeviceIdType.MESH
LAG_MLP = 1
GROUP = 4
ROW_BLOCK = 32


def dot_nn(lhs, rhs):
    return lax.dot_general(lhs, rhs, (((1,), (0,)), ((), ())), preferred_element_type=jnp.float32)


def dot_nt(lhs, rhs):
    return lax.dot_general(lhs, rhs, (((1,), (1,)), ((), ())), preferred_element_type=jnp.float32)


def dot_tn(lhs, rhs):
    return lax.dot_general(lhs, rhs, (((0,), (0,)), ((), ())), preferred_element_type=jnp.float32)


def rms_scale(vals):
    return lax.rsqrt(jnp.mean(vals * vals, axis=-1, keepdims=True) + NORM_EPS)


def rms_vjp(vals, cotangent):
    scale = rms_scale(vals)
    inner = jnp.mean(vals * cotangent, axis=-1, keepdims=True)
    return scale * (cotangent - vals * (scale * scale * inner))


def row_blocks(count):
    return [pl.ds(start, ROW_BLOCK) for start in range(0, count, ROW_BLOCK)]


def causal_weights(scores_t, col_max, col_inv, scale):
    half = scores_t.shape[0] // 2
    diag = lax.broadcasted_iota(jnp.int32, (half, half), 0) <= lax.broadcasted_iota(jnp.int32, (half, half), 1)
    upper_l = jnp.where(diag, scores_t[:half, :half], -1e30)
    upper_r = scores_t[:half, half:]
    lower_r = jnp.where(diag, scores_t[half:, half:], -1e30)
    fresh = col_max is None
    if fresh:
        max_l = jnp.max(upper_l, axis=0, keepdims=True)
        max_r = jnp.maximum(jnp.max(upper_r, axis=0, keepdims=True), jnp.max(lower_r, axis=0, keepdims=True))
    else:
        max_l, max_r = col_max[:, :half], col_max[:, half:]
    factor = scale * LOG2E
    exp_ul = jnp.exp2((upper_l - max_l) * factor)
    exp_ur = jnp.exp2((upper_r - max_r) * factor)
    exp_lr = jnp.exp2((lower_r - max_r) * factor)
    if fresh:
        inv_l = 1.0 / jnp.sum(exp_ul, axis=0, keepdims=True)
        inv_r = 1.0 / (jnp.sum(exp_ur, axis=0, keepdims=True) + jnp.sum(exp_lr, axis=0, keepdims=True))
        stats = (jnp.concatenate([max_l, max_r], axis=1), jnp.concatenate([inv_l, inv_r], axis=1))
    else:
        inv_l, inv_r = col_inv[:, :half], col_inv[:, half:]
        stats = None
    return (exp_ul * inv_l, exp_ur * inv_r, exp_lr * inv_r), stats


def assemble(blocks, dtype):
    upper_l, upper_r, lower_r = (b.astype(dtype) for b in blocks)
    upper = jnp.concatenate([upper_l, upper_r], axis=1)
    lower = jnp.concatenate([jnp.zeros_like(upper_l), lower_r], axis=1)
    return jnp.concatenate([upper, lower], axis=0)


def forward_layer(dims, act_ref, wqkv, wout, wup, wdown, n1_ref, qkv_ref, stat_ref, ctx_ref, hid_ref, n2_ref, gp_ref, up_ref, out_ref, flush, n1t_s, score_s, prob_s, acc_s, ready):
    heads, hdim, ffn_tile = dims
    width = heads * hdim
    ffn = wdown.shape[0]
    scale = hdim ** -0.5
    for rows in row_blocks(act_ref.shape[0]):
        act32 = act_ref[rows, :].astype(jnp.float32)
        n1_ref[rows, :] = (act32 * rms_scale(act32)).astype(jnp.bfloat16)
    n1t_s[...] = n1_ref[...].T
    ready(0)

    def rows_of(h):
        return tuple(pl.ds(part * width + h * hdim, hdim) for part in range(3))

    def project(h):
        rows = rows_of(h)
        stacked = jnp.concatenate([wqkv[r, :] for r in rows], axis=0)
        proj = dot_nn(stacked, n1t_s[...]).astype(jnp.bfloat16)
        for part, r in enumerate(rows):
            qkv_ref[r, :] = proj[part * hdim:(part + 1) * hdim]

    def score(h):
        rows = rows_of(h)
        score_s[h % 3] = dot_tn(qkv_ref[rows[1], :], qkv_ref[rows[0], :])

    def soften(h):
        blocks, stats = causal_weights(score_s.at[h % 3], None, None, scale)
        stat_ref[h, 0:1, :] = stats[0]
        stat_ref[h, 1:2, :] = stats[1]
        prob_s[h % 2] = assemble(blocks, jnp.bfloat16)

    def mix(h):
        rows = rows_of(h)
        ctx_ref[rows[0], :] = dot_nn(qkv_ref[rows[2], :], prob_s[h % 2]).astype(jnp.bfloat16)

    for step in range(heads + 5):
        for lag, action in ((0, project), (2, score), (4, soften), (5, mix)):
            h = step - lag
            if 0 <= h < heads:
                action(h)
    flush(0)
    ready(1)
    acc_s[...] = dot_tn(ctx_ref[...], wout[...])
    for rows in row_blocks(act_ref.shape[0]):
        hid16 = (act_ref[rows, :].astype(jnp.float32) + acc_s[rows, :]).astype(jnp.bfloat16)
        hid_ref[rows, :] = hid16
        hid32 = hid16.astype(jnp.float32)
        n2_ref[rows, :] = (hid32 * rms_scale(hid32)).astype(jnp.bfloat16)
    normed2 = n2_ref[...]
    flush(1)
    ready(2)
    for tile in range(ffn // ffn_tile):
        cols = pl.ds(tile * ffn_tile, ffn_tile)
        pre = dot_nn(normed2, wup[:, cols])
        gp_ref[:, cols] = pre
        tanh = jnp.tanh(pre * (GELU_C + (GELU_C * GELU_A) * (pre * pre)))
        up_ref[:, cols] = (pre * (0.5 + 0.5 * tanh)).astype(jnp.bfloat16)
    flush(2)
    ready(3)
    acc_s[...] = dot_nn(up_ref[...], wdown[...])
    for rows in row_blocks(act_ref.shape[0]):
        out_ref[rows, :] = (hid_ref[rows, :].astype(jnp.float32) + acc_s[rows, :]).astype(jnp.bfloat16)


def backward_layer(dims, grad_ref, act_ref, wqkv, wout, wup, wdown, qkv_ref, stat_ref, hid_ref, gp_ref, dpre_ref, dhid_ref, dctx_ref, dqkv_ref, dact_ref, flush, acc_s, dhid_s32, dhidt_s, score_s, dprob_s, prob_s, dscore_s):
    heads, hdim, ffn_tile = dims
    width = heads * hdim
    ffn = wdown.shape[0]
    scale = hdim ** -0.5
    grad16 = grad_ref[...]

    def slope(tile):
        cols = pl.ds(tile * ffn_tile, ffn_tile)
        dup = dot_nt(grad16, wdown[cols, :])
        pre = gp_ref[:, cols]
        pre_sq = pre * pre
        tanh = jnp.tanh(pre * (GELU_C + (GELU_C * GELU_A) * pre_sq))
        half = 0.5 + 0.5 * tanh
        bend = (half * (1.0 - half)) * (pre * (2.0 * GELU_C + (6.0 * GELU_C * GELU_A) * pre_sq))
        dpre_ref[:, cols] = (dup * (half + bend)).astype(jnp.bfloat16)

    def gather(tile):
        cols = pl.ds(tile * ffn_tile, ffn_tile)
        part = dot_nt(dpre_ref[:, cols], wup[:, cols])
        if tile == 0:
            acc_s[...] = part
        else:
            acc_s[...] += part

    tiles = ffn // ffn_tile
    for step in range(tiles + LAG_MLP):
        if step < tiles:
            slope(step)
        if step >= LAG_MLP:
            gather(step - LAG_MLP)
    flush(0)
    for rows in row_blocks(act_ref.shape[0]):
        dhid32 = grad_ref[rows, :].astype(jnp.float32) + rms_vjp(hid_ref[rows, :].astype(jnp.float32), acc_s[rows, :])
        dhid_s32[rows, :] = dhid32
        dhid_ref[rows, :] = dhid32.astype(jnp.bfloat16)
    dhidt_s[...] = dhid_ref[...].T
    flush(1)

    def rows_of(h):
        return tuple(pl.ds(part * width + h * hdim, hdim) for part in range(3))

    def project(h):
        rows = rows_of(h)[0]
        dctx_ref[rows, :] = dot_nn(wout[rows, :], dhidt_s[...]).astype(jnp.bfloat16)

    def score(h):
        rows = rows_of(h)
        score_s[h % 3] = dot_tn(qkv_ref[rows[1], :], qkv_ref[rows[0], :])
        dprob_s[h % 3] = dot_tn(qkv_ref[rows[2], :], dctx_ref[rows[0], :])

    def soften(h):
        probs, _ = causal_weights(score_s.at[h % 3], stat_ref[h, 0:1, :], stat_ref[h, 1:2, :], scale)
        dprobs = dprob_s.at[h % 3]
        half = dprobs.shape[0] // 2
        d_ul, d_ur, d_lr = dprobs[:half, :half], dprobs[:half, half:], dprobs[half:, half:]
        p_ul, p_ur, p_lr = probs
        delta_l = jnp.sum(d_ul * p_ul, axis=0, keepdims=True)
        delta_r = jnp.sum(d_ur * p_ur, axis=0, keepdims=True) + jnp.sum(d_lr * p_lr, axis=0, keepdims=True)
        prob_s[h % 2] = assemble(probs, jnp.bfloat16)
        dscore_s[h % 2] = assemble((p_ul * (d_ul - delta_l) * scale, p_ur * (d_ur - delta_r) * scale, p_lr * (d_lr - delta_r) * scale), jnp.bfloat16)

    def mix(h):
        rows = rows_of(h)
        dqkv_ref[rows[2], :] = dot_nt(dctx_ref[rows[0], :], prob_s[h % 2]).astype(jnp.bfloat16)
        dqkv_ref[rows[0], :] = dot_nn(qkv_ref[rows[1], :], dscore_s[h % 2]).astype(jnp.bfloat16)
        dqkv_ref[rows[1], :] = dot_nt(qkv_ref[rows[0], :], dscore_s[h % 2]).astype(jnp.bfloat16)

    def collect(first, count):
        spans = [pl.ds(part * width + first * hdim, count * hdim) for part in range(3)]
        part = dot_tn(jnp.concatenate([dqkv_ref[r, :] for r in spans], axis=0), jnp.concatenate([wqkv[r, :] for r in spans], axis=0))
        if first == 0:
            acc_s[...] = part
        else:
            acc_s[...] += part

    group = min(GROUP, heads)
    for step in range(heads + 5):
        for lag, action in ((0, project), (2, score), (4, soften), (5, mix)):
            h = step - lag
            if 0 <= h < heads:
                action(h)
        done = step - 6
        if done >= 0 and done % group == group - 1 and done < heads - group:
            collect(done - group + 1, group)
    flush(2)
    collect(heads - group, group)
    for rows in row_blocks(act_ref.shape[0]):
        dact = dhid_s32[rows, :] + rms_vjp(act_ref[rows, :].astype(jnp.float32), acc_s[rows, :])
        dact_ref[rows, :] = dact.astype(jnp.bfloat16)


class placement:
    def __init__(self, n_stages):
        row = lax.axis_index('data')
        self.row = row
        self.index = lax.axis_index('stage')
        self.column = lax.div(self.index, 2)
        self.core = lax.rem(self.index, 2)
        self.upper = lax.div(row, 2)
        self.half = lax.rem(self.upper + self.column, 2)
        self.layer = 2 * self.column + self.half
        self.home = self.layer
        self.mate = 2 * self.column + 1 - self.core
        across = 3 - row
        along = lax.rem(self.index + jnp.where(self.half == 1, 2, n_stages - 2), n_stages)
        self.mate_id = {'data': row, 'stage': self.mate}
        self.across_id = {'data': across, 'stage': self.index}
        self.along_id = {'data': row, 'stage': along}
        self.next_id = {'data': jnp.where(self.half == 1, row, across), 'stage': jnp.where(self.half == 1, along, self.index)}
        self.prev_id = {'data': jnp.where(self.half == 1, across, row), 'stage': jnp.where(self.half == 1, self.index, along)}


def pipeline_kernel(
    cfg,
    emb_hbm, tgt_hbm, wqkv_hbm, wout_hbm, wup_hbm, wdown_hbm,
    loss_ref, n1_hbm, n2_hbm, up_hbm, ctx_hbm, dqkv_hbm, dpre_hbm, dhid_hbm, g_hbm, dx_hbm, qkv_hbm, gp_hbm, hid_hbm, stat_hbm,
    wqkv, wout, wup, wdown, act, grad, out_s, dact_s,
    n1_s, n2_s, up_s, ctx_s, qkv_s, gp_s, hid_s, stat_s,
    dpre_s, dhid_s, dctx_s, dqkv_s,
    w_sem, in_sem, act_sem, grad_sem, fout_sem, bin_sem, bout_sem, fsend_sem, bsend_sem, loss_acc, loss_sem, dx_sem, n1t_s, score_s, prob_s, dprob_s, dscore_s, acc_s, dhid_s32,
):
    n_stages, n_seq, tokens, grad_scale, dims = cfg
    here = placement(n_stages)
    stage, core, next_id, prev_id = here.layer, here.core, here.next_id, here.prev_id
    is_first = stage == 0
    is_last = stage == n_stages - 1
    own_weights = here.layer == here.index
    own_data = here.upper == core
    feeds_first = (here.column == 0) & (here.half == 1) & (core == 1)
    feeds_last = (here.column == n_stages // 2 - 1) & (here.half == 0) & (core == 1)

    weight_pairs = ((wqkv_hbm, wqkv), (wout_hbm, wout), (wup_hbm, wup), (wdown_hbm, wdown))

    def load_weight(idx):
        return pltpu.make_async_copy(weight_pairs[idx][0], weight_pairs[idx][1], w_sem.at[idx])

    def give_weight(idx):
        return pltpu.make_async_remote_copy(
            src_ref=weight_pairs[idx][0], dst_ref=weight_pairs[idx][1], send_sem=w_sem.at[4 + idx], recv_sem=w_sem.at[8 + idx],
            device_id=here.mate_id, device_id_type=MESH_ID)

    def load_embed(m):
        return pltpu.make_async_copy(emb_hbm.at[m], act.at[m], in_sem.at[m])

    def load_target(m):
        return pltpu.make_async_copy(tgt_hbm.at[m], grad.at[m], in_sem.at[m])

    def give_embed(m):
        return pltpu.make_async_remote_copy(
            src_ref=emb_hbm.at[m], dst_ref=act.at[m], send_sem=in_sem.at[m], recv_sem=act_sem.at[m],
            device_id=here.across_id, device_id_type=MESH_ID)

    def give_target(m):
        return pltpu.make_async_remote_copy(
            src_ref=tgt_hbm.at[m], dst_ref=grad.at[m], send_sem=in_sem.at[m], recv_sem=grad_sem.at[m],
            device_id=here.across_id, device_id_type=MESH_ID)

    def each_seq(when, action):
        @pl.when(when)
        def _():
            def go(m, carry):
                action(m)
                return carry
            lax.fori_loop(0, n_seq, go, 0)

    @pl.when(own_weights)
    def _():
        for idx in range(4):
            load_weight(idx).start()

    each_seq(is_first & own_data, lambda m: load_embed(m).start())
    each_seq(is_last & own_data, lambda m: load_target(m).start())

    barrier = pltpu.get_barrier_semaphore()
    for peer in (here.mate_id, here.across_id, here.along_id):
        pl.semaphore_signal(barrier, inc=1, device_id=peer, device_id_type=MESH_ID)
    pl.semaphore_wait(barrier, 3)

    @pl.when(own_weights)
    def _():
        for idx in range(4):
            give_weight(idx).start()

    each_seq(feeds_first, lambda m: give_embed(m).start())
    each_seq(feeds_last, lambda m: give_target(m).start())
    loss_acc[...] = jnp.zeros_like(loss_acc)

    def await_weight(idx):
        @pl.when(own_weights)
        def _():
            load_weight(idx).wait()

        @pl.when(jnp.logical_not(own_weights))
        def _():
            give_weight(idx).wait_recv()

    def send_act(m, slot):
        return pltpu.make_async_remote_copy(
            src_ref=out_s.at[slot], dst_ref=act.at[m], send_sem=fsend_sem.at[slot], recv_sem=act_sem.at[m],
            device_id=next_id, device_id_type=MESH_ID)

    def send_grad(m, slot):
        return pltpu.make_async_remote_copy(
            src_ref=dact_s.at[slot], dst_ref=grad.at[m], send_sem=bsend_sem.at[slot], recv_sem=grad_sem.at[m],
            device_id=prev_id, device_id_type=MESH_ID)

    def store_dx(m, slot):
        return pltpu.make_async_copy(dact_s.at[slot], dx_hbm.at[m], bsend_sem.at[slot])

    def give_dx(m, slot):
        return pltpu.make_async_remote_copy(
            src_ref=dact_s.at[slot], dst_ref=dx_hbm.at[m], send_sem=bsend_sem.at[slot], recv_sem=dx_sem.at[m],
            device_id=here.across_id, device_id_type=MESH_ID)

    def token_range(m):
        return pl.ds(pl.multiple_of(m * tokens, tokens), tokens)

    def fout_copies(m, slot):
        rows = token_range(m)
        return (
            (0, pltpu.make_async_copy(n1_s.at[slot], n1_hbm.at[rows, :], fout_sem.at[slot, 0])),
            (0, pltpu.make_async_copy(qkv_s.at[slot], qkv_hbm.at[m], fout_sem.at[slot, 1])),
            (1, pltpu.make_async_copy(ctx_s.at[slot], ctx_hbm.at[:, rows], fout_sem.at[slot, 2])),
            (1, pltpu.make_async_copy(stat_s.at[slot], stat_hbm.at[m], fout_sem.at[slot, 3])),
            (1, pltpu.make_async_copy(hid_s.at[slot], hid_hbm.at[m], fout_sem.at[slot, 4])),
            (1, pltpu.make_async_copy(n2_s.at[slot], n2_hbm.at[rows, :], fout_sem.at[slot, 5])),
            (2, pltpu.make_async_copy(gp_s.at[slot], gp_hbm.at[m], fout_sem.at[slot, 6])),
            (2, pltpu.make_async_copy(up_s.at[slot], up_hbm.at[rows, :], fout_sem.at[slot, 7])),
        )

    def bin_copies(m):
        return (
            pltpu.make_async_copy(qkv_hbm.at[m], qkv_s.at[2], bin_sem.at[0]),
            pltpu.make_async_copy(stat_hbm.at[m], stat_s.at[2], bin_sem.at[1]),
            pltpu.make_async_copy(hid_hbm.at[m], hid_s.at[2], bin_sem.at[2]),
            pltpu.make_async_copy(gp_hbm.at[m], gp_s.at[2], bin_sem.at[3]),
        )

    def bout_copies(m, slot):
        rows = token_range(m)
        return (
            (0, pltpu.make_async_copy(grad.at[m], g_hbm.at[rows, :], bout_sem.at[slot, 0])),
            (0, pltpu.make_async_copy(dpre_s.at[slot], dpre_hbm.at[rows, :], bout_sem.at[slot, 1])),
            (1, pltpu.make_async_copy(dhid_s.at[slot], dhid_hbm.at[rows, :], bout_sem.at[slot, 2])),
            (2, pltpu.make_async_copy(dqkv_s.at[slot], dqkv_hbm.at[:, rows], bout_sem.at[slot, 3])),
        )

    def flusher(copies):
        def flush(group):
            for when, copy in copies:
                if when == group:
                    copy.start()
        return flush

    def in_range(m):
        return (m >= 0) & (m < n_seq)

    def tick(t, carry):
        fwd_m = t - stage
        bwd_m = t + stage - (2 * n_stages - 2)

        @pl.when(in_range(fwd_m))
        def _():
            m = fwd_m
            slot = lax.rem(m, 2)

            @pl.when(is_first & own_data)
            def _():
                load_embed(m).wait()

            @pl.when(jnp.logical_not(is_first & own_data))
            def _():
                send_act(m, slot).wait_recv()

            def run_forward(ready):
                forward_layer(
                    dims, act.at[m], wqkv, wout, wup, wdown, n1_s.at[slot], qkv_s.at[slot], stat_s.at[slot],
                    ctx_s.at[slot], hid_s.at[slot], n2_s.at[slot], gp_s.at[slot], up_s.at[slot], out_s.at[slot],
                    flusher(fout_copies(m, slot)), n1t_s, score_s, prob_s, acc_s, ready)

            @pl.when(m == 0)
            def _():
                run_forward(await_weight)

            @pl.when(m > 0)
            def _():
                run_forward(lambda idx: None)

            @pl.when(jnp.logical_not(is_last))
            def _():
                send_act(m, slot).start()

            @pl.when(is_last & own_data)
            def _():
                load_target(m).wait()

            @pl.when(is_last & jnp.logical_not(own_data))
            def _():
                send_grad(m, slot).wait_recv()

            @pl.when(is_last)
            def _():
                for start in range(0, tokens, 32):
                    rows = pl.ds(start, 32)
                    error = out_s[slot, rows, :].astype(jnp.float32) - grad[m, rows, :].astype(jnp.float32)
                    square = error * error
                    loss_acc[...] += (square[0:8] + square[8:16]) + (square[16:24] + square[24:32])
                    grad[m, rows, :] = (error * grad_scale).astype(jnp.bfloat16)

        @pl.when(in_range(bwd_m))
        def _():
            m = bwd_m
            slot = lax.rem(m, 2)

            @pl.when(jnp.logical_not(is_last))
            def _():
                for copy in bin_copies(m):
                    copy.wait()
                send_grad(m, slot).wait_recv()

            saved = jnp.where(is_last, slot, 2)
            backward_layer(
                dims, grad.at[m], act.at[m], wqkv, wout, wup, wdown, qkv_s.at[saved], stat_s.at[saved], hid_s.at[saved],
                gp_s.at[saved], dpre_s.at[slot], dhid_s.at[slot], dctx_s, dqkv_s.at[slot], dact_s.at[slot],
                flusher(bout_copies(m, slot)), acc_s, dhid_s32, n1t_s, score_s, dprob_s, prob_s, dscore_s)

            @pl.when(jnp.logical_not(is_first))
            def _():
                send_grad(m, slot).start()

            @pl.when(is_first & own_data)
            def _():
                store_dx(m, slot).start()

            @pl.when(is_first & jnp.logical_not(own_data))
            def _():
                give_dx(m, slot).start()

        fwd_old = fwd_m - 1
        bwd_old = bwd_m - 1

        @pl.when(in_range(fwd_old))
        def _():
            slot = lax.rem(fwd_old, 2)
            for _, copy in fout_copies(fwd_old, slot):
                copy.wait()

            @pl.when(jnp.logical_not(is_last))
            def _():
                send_act(fwd_old, slot).wait_send()

        @pl.when(in_range(bwd_old))
        def _():
            slot = lax.rem(bwd_old, 2)
            for _, copy in bout_copies(bwd_old, slot):
                copy.wait()

            @pl.when(jnp.logical_not(is_first))
            def _():
                send_grad(bwd_old, slot).wait_send()

            @pl.when(is_first & own_data)
            def _():
                store_dx(bwd_old, slot).wait()

            @pl.when(is_first & jnp.logical_not(own_data))
            def _():
                give_dx(bwd_old, slot).wait_send()

        @pl.when(in_range(bwd_m + 1) & jnp.logical_not(is_last))
        def _():
            for copy in bin_copies(bwd_m + 1):
                copy.start()

        return carry

    lax.fori_loop(0, n_seq + 2 * n_stages - 1, tick, 0)

    def send_loss():
        return pltpu.make_async_remote_copy(
            src_ref=loss_ref, dst_ref=loss_ref, send_sem=loss_sem.at[0], recv_sem=loss_sem.at[1],
            device_id=prev_id, device_id_type=MESH_ID)

    @pl.when(is_last)
    def _():
        lanes = loss_ref.shape[1]
        total = loss_acc[:, 0:lanes]
        for col in range(lanes, loss_acc.shape[1], lanes):
            total = total + loss_acc[:, col:col + lanes]
        loss_ref[...] = total

    @pl.when(jnp.logical_not(is_last))
    def _():
        send_loss().wait_recv()

    @pl.when(jnp.logical_not(is_first))
    def _():
        send_loss().start()
        send_loss().wait_send()

    @pl.when(own_weights)
    def _():
        for idx in range(4):
            give_weight(idx).wait_send()

    each_seq(feeds_first, lambda m: give_embed(m).wait_send())
    each_seq(feeds_last, lambda m: give_target(m).wait_send())
    each_seq(feeds_first, lambda m: give_dx(m, 0).wait_recv())


def run_pipeline(n_stages, grad_scale, embeds, targets, wqkv, wout, wup, wdown, heads, hdim):
    n_seq, tokens, width = embeds.shape
    ffn = wdown.shape[0]
    dims = (heads, hdim, 512 if ffn % 512 == 0 else ffn)
    bf16, f32 = jnp.bfloat16, jnp.float32
    total = n_seq * tokens
    out_shapes = [
        ((8, 128), f32),
        ((total, width), bf16),
        ((total, width), bf16),
        ((total, ffn), bf16),
        ((width, total), bf16),
        ((3 * width, total), bf16),
        ((total, ffn), bf16),
        ((total, width), bf16),
        ((total, width), bf16),
        ((n_seq, tokens, width), bf16),
        ((n_seq, 3 * width, tokens), bf16),
        ((n_seq, tokens, ffn), f32),
        ((n_seq, tokens, width), bf16),
        ((n_seq, heads, 8, tokens), f32),
    ]
    any_spec = pl.BlockSpec(memory_space=pl.ANY)
    scratch = [
        pltpu.VMEM(wqkv.shape, bf16), pltpu.VMEM(wout.shape, bf16), pltpu.VMEM(wup.shape, bf16), pltpu.VMEM(wdown.shape, bf16),
        pltpu.VMEM((n_seq, tokens, width), bf16), pltpu.VMEM((n_seq, tokens, width), bf16),
        pltpu.VMEM((2, tokens, width), bf16), pltpu.VMEM((2, tokens, width), bf16),
        pltpu.VMEM((2, tokens, width), bf16), pltpu.VMEM((2, tokens, width), bf16),
        pltpu.VMEM((2, tokens, ffn), bf16), pltpu.VMEM((2, width, tokens), bf16),
        pltpu.VMEM((3, 3 * width, tokens), bf16), pltpu.VMEM((3, tokens, ffn), f32),
        pltpu.VMEM((3, tokens, width), bf16), pltpu.VMEM((3, heads, 8, tokens), f32),
        pltpu.VMEM((2, tokens, ffn), bf16), pltpu.VMEM((2, tokens, width), bf16),
        pltpu.VMEM((width, tokens), bf16), pltpu.VMEM((2, 3 * width, tokens), bf16),
        pltpu.SemaphoreType.DMA((12,)), pltpu.SemaphoreType.DMA((n_seq,)),
        pltpu.SemaphoreType.DMA((n_seq,)), pltpu.SemaphoreType.DMA((n_seq,)),
        pltpu.SemaphoreType.DMA((2, 8)), pltpu.SemaphoreType.DMA((4,)), pltpu.SemaphoreType.DMA((2, 4)),
        pltpu.SemaphoreType.DMA((2,)), pltpu.SemaphoreType.DMA((2,)),
        pltpu.VMEM((8, width), f32), pltpu.SemaphoreType.DMA((2,)), pltpu.SemaphoreType.DMA((n_seq,)),
        pltpu.VMEM((width, tokens), bf16), pltpu.VMEM((3, tokens, tokens), f32), pltpu.VMEM((2, tokens, tokens), bf16),
        pltpu.VMEM((3, tokens, tokens), f32), pltpu.VMEM((2, tokens, tokens), bf16), pltpu.VMEM((tokens, width), f32), pltpu.VMEM((tokens, width), f32),
    ]
    linear = 2 * total * (wqkv.size + wout.size + wup.size + wdown.size)
    return pl.pallas_call(
        functools.partial(pipeline_kernel, (n_stages, n_seq, tokens, grad_scale, dims)),
        out_shape=[jax.ShapeDtypeStruct(s, d) for s, d in out_shapes],
        in_specs=[any_spec] * 6,
        out_specs=[pl.BlockSpec(memory_space=pltpu.VMEM)] + [any_spec] * (len(out_shapes) - 1),
        scratch_shapes=scratch,
        compiler_params=pltpu.CompilerParams(collective_id=0, has_side_effects=True, vmem_limit_bytes=67043328),
        cost_estimate=pl.CostEstimate(flops=3 * linear, bytes_accessed=200 * 2 ** 20, transcendentals=0),
        name='stage_pipeline',
    )(embeds, targets, wqkv, wout, wup, wdown)


def reduce_kernel(
    cfg,
    loss_hbm, ctx_hbm, dhid_hbm, dqkv_hbm, n1_hbm, up_hbm, g_hbm, n2_hbm, dpre_hbm, dx_hbm,
    loss_ref, dout_hbm, dqkvw_hbm, ddown_hbm, dup_hbm, demb_hbm,
    out_res, qkv_res, down_res, up_res, out_in, qkv_in, down_in, up_in,
    out_give, qkv_give, down_give, up_give, out_core, qkv_core, down_core, up_core, out_row, qkv_row, down_row, up_row, loss_sl,
    res_sem, in_sem, give_sem, core_sem, row_send, row_recv, put_send, put_recv, pass_send, store_sem, dx_sem,
    loss_send, loss_recv, loss_in,
):
    (n_stages,) = cfg
    here = placement(n_stages)
    row, core, stage = here.row, here.core, here.index
    pair = lax.rem(row, 2)
    pair_row = row + 1 - 2 * pair
    across = 3 - row
    is_home = here.home == stage
    home_id = {'data': row, 'stage': here.home}
    pair_id = {'data': pair_row, 'stage': stage}
    pair_home_id = {'data': pair_row, 'stage': here.home}
    across_home_id = {'data': across, 'stage': here.home}

    kinds = (
        ('rows', dhid_hbm, out_res, ctx_hbm, out_in, out_give, out_core, out_row, dout_hbm),
        ('rows', n1_hbm, qkv_res, dqkv_hbm, qkv_in, qkv_give, qkv_core, qkv_row, dqkvw_hbm),
        ('tall', g_hbm, down_res, up_hbm, down_in, down_give, down_core, down_row, ddown_hbm),
        ('wide', n2_hbm, up_res, dpre_hbm, up_in, up_give, up_core, up_row, dup_hbm),
    )
    n_kinds = len(kinds)
    turns = ((1, 1), (0, 1), (1, 0), (0, 0))

    def piece(kind, member, unit, num):
        size = kinds[kind][4].shape[1 if kinds[kind][0] == 'rows' else 2]
        return pl.ds(pl.multiple_of(((member * 2 + unit) * 2 + num) * size, size), size)

    def flip(val, by):
        return 1 - val if by else val

    def read_piece(kind, turn, num):
        form, _, _, src, buf = kinds[kind][:5]
        part = piece(kind, flip(pair, turns[turn][0]), flip(core, turns[turn][1]), num)
        view = src.at[part, :] if form == 'rows' else src.at[:, part]
        return pltpu.make_async_copy(view, buf.at[turn % 2], in_sem.at[kind, turn % 2])

    def out_view(kind, member, unit, num):
        part = piece(kind, member, unit, num)
        dst = kinds[kind][8]
        return dst.at[:, part] if kinds[kind][0] == 'wide' else dst.at[part, :]

    def give(kind, other, num):
        return pltpu.make_async_remote_copy(
            src_ref=kinds[kind][5].at[other], dst_ref=kinds[kind][6].at[num, other], send_sem=give_sem.at[kind, other],
            recv_sem=core_sem.at[kind, num, other], device_id=here.mate_id, device_id_type=MESH_ID)

    def send_row(kind, num):
        return pltpu.make_async_remote_copy(
            src_ref=kinds[kind][6].at[num, 1], dst_ref=kinds[kind][7].at[num], send_sem=row_send.at[kind, num],
            recv_sem=row_recv.at[kind, num], device_id=pair_id, device_id_type=MESH_ID)

    def put(kind, num, target, device_id):
        return pltpu.make_async_remote_copy(
            src_ref=kinds[kind][7].at[num], dst_ref=out_view(kind, pair, core, num), send_sem=put_send.at[target, kind, num],
            recv_sem=put_recv.at[pair, core, kind, num], device_id=device_id, device_id_type=MESH_ID)

    def keep(kind, num):
        return pltpu.make_async_copy(kinds[kind][7].at[num], out_view(kind, pair, core, num), store_sem.at[kind, num])

    def arrival(kind, num, member, unit):
        view = out_view(kind, member, unit, num)
        return pltpu.make_async_remote_copy(
            src_ref=view, dst_ref=view, send_sem=pass_send.at[unit, kind, num], recv_sem=put_recv.at[member, unit, kind, num],
            device_id=across_home_id, device_id_type=MESH_ID)

    def load_resident(kind):
        return pltpu.make_async_copy(kinds[kind][1], kinds[kind][2], res_sem.at[kind])

    def pipeline_id(row_idx, unit):
        return 2 * jnp.minimum(row_idx, 3 - row_idx) + unit

    my_loss = pltpu.make_async_copy(loss_hbm, loss_sl.at[pipeline_id(row, core)], loss_in)
    my_loss.start()
    for kind in range(n_kinds):
        load_resident(kind).start()
        read_piece(kind, 0, 0).start()

    source = here.upper
    rank = stage + source - 2 * source * core
    spans = []
    span = n_stages // 2
    while span >= 1:
        spans.append(span)
        span //= 2

    def swapped(span):
        return stage + span - 2 * span * lax.rem(lax.div(stage, span), 2)

    loss_ids = (
        ({'data': row, 'stage': here.mate}, row, 1 - core),
        ({'data': pair_row, 'stage': stage}, pair_row, core),
        ({'data': pair_row, 'stage': here.mate}, pair_row, 1 - core),
    )
    peers = [ident for ident, _, _ in loss_ids]
    peers += [{'data': across, 'stage': stage}, {'data': across, 'stage': here.mate}]
    peers += [{'data': row, 'stage': swapped(span)} for span in spans if span > 1]
    barrier = pltpu.get_barrier_semaphore()
    for ident in peers:
        pl.semaphore_signal(barrier, inc=1, device_id=ident, device_id_type=MESH_ID)
    pl.semaphore_wait(barrier, len(peers))

    def send_loss(idx):
        slot = loss_sl.at[pipeline_id(row, core)]
        return pltpu.make_async_remote_copy(
            src_ref=slot, dst_ref=slot, send_sem=loss_send.at[idx], recv_sem=loss_recv.at[idx],
            device_id=loss_ids[idx][0], device_id_type=MESH_ID)

    def loss_arrival(idx):
        slot = loss_sl.at[pipeline_id(loss_ids[idx][1], loss_ids[idx][2])]
        return pltpu.make_async_remote_copy(
            src_ref=slot, dst_ref=slot, send_sem=loss_send.at[idx], recv_sem=loss_recv.at[idx],
            device_id=loss_ids[idx][0], device_id_type=MESH_ID)

    my_loss.wait()
    for idx in range(3):
        send_loss(idx).start()

    def spread(idx):
        return pltpu.make_async_remote_copy(
            src_ref=demb_hbm, dst_ref=demb_hbm, send_sem=dx_sem.at[0, idx], recv_sem=dx_sem.at[1, idx],
            device_id={'data': row, 'stage': swapped(spans[idx])}, device_id_type=MESH_ID)

    def sends_at(idx):
        return lax.rem(rank, 2 * spans[idx]) == 0

    def receives_at(idx):
        return lax.rem(rank, 2 * spans[idx]) == spans[idx]

    def spread_round(idx):
        if idx > 0:
            @pl.when(receives_at(idx - 1))
            def _():
                spread(idx - 1).wait_recv()
        if idx < len(spans):
            @pl.when(sends_at(idx))
            def _():
                spread(idx).start()

    def product(kind, turn, num, sink, base):
        form, _, res, _, buf = kinds[kind][:5]
        read_piece(kind, turn, num).wait()
        if turn < 3:
            read_piece(kind, turn + 1, num).start()
        else:
            @pl.when(num == 0)
            def _():
                read_piece(kind, 0, 1).start()
        fed = buf.at[turn % 2]
        tile = min(256, res.shape[1])

        def body(n, carry):
            span = pl.ds(pl.multiple_of(n * tile, tile), tile)
            if form == 'rows':
                part, at = dot_nn(fed[...], res[:, span]), (slice(None), span)
            elif form == 'tall':
                part, at = dot_tn(fed[...], res[:, span]), (slice(None), span)
            else:
                part, at = dot_tn(res[:, span], fed[...]), (span, slice(None))
            for ref in base:
                part = part + ref[at]
            sink[at] = part
            return carry

        lax.fori_loop(0, res.shape[1] // tile, body, 0)

    def first_half(kind, num):
        give_buf, core_buf = kinds[kind][5:7]

        @pl.when(num == 0)
        def _():
            load_resident(kind).wait()

        for turn, other in ((0, 1), (1, 0)):
            @pl.when(num > 0)
            def _():
                give(kind, other, num - 1).wait_send()

            product(kind, turn, num, give_buf.at[other], ())
            give(kind, other, num).start()
        give(kind, 1, num).wait_recv()
        product(kind, 2, num, core_buf.at[num, 1], (core_buf.at[num, 1],))
        send_row(kind, num).start()

    def second_half(kind, num):
        core_buf, row_buf = kinds[kind][6:8]
        give(kind, 0, num).wait_recv()
        send_row(kind, num).wait_recv()
        product(kind, 3, num, row_buf.at[num], (core_buf.at[num, 0], row_buf.at[num]))
        put(kind, num, 1, pair_home_id).start()
        put(kind, num, 2, across_home_id).start()

        @pl.when(is_home)
        def _():
            keep(kind, num).start()

        @pl.when(jnp.logical_not(is_home))
        def _():
            put(kind, num, 0, home_id).start()

    def pass_on(kind, num):
        @pl.when(is_home)
        def _():
            for unit in range(2):
                arrival(kind, num, 1 - pair, unit).wait_recv()
                arrival(kind, num, 1 - pair, unit).start()

    def kind_at(pos):
        late = jnp.where(pos == 4, 2, jnp.where(pos == 5, 3, jnp.where(pos == 6, 1, 0)))
        return jnp.where(pos < 4, pos, late)

    def num_at(pos):
        return jnp.where(pos < 4, 0, 1)

    n_steps = 2 * n_kinds

    def step_body(pos, carry):
        for kind in range(n_kinds):
            @pl.when((pos < n_steps) & (kind_at(pos) == kind))
            def _():
                first_half(kind, num_at(pos))

        for kind in range(n_kinds):
            @pl.when((pos >= 1) & (pos < n_steps + 1) & (kind_at(pos - 1) == kind))
            def _():
                second_half(kind, num_at(pos - 1))

        for kind in range(n_kinds):
            @pl.when((pos >= 2) & (kind_at(pos - 2) == kind))
            def _():
                pass_on(kind, num_at(pos - 2))

        for idx in range(len(spans) + 1):
            @pl.when(pos == 3 * idx)
            def _():
                spread_round(idx)
        return carry

    lax.fori_loop(0, n_steps + 2, step_body, 0)

    for idx in range(3):
        loss_arrival(idx).wait_recv()
    total = loss_sl[0]
    for idx in range(1, 4):
        total = total + loss_sl[idx]
    loss_ref[...] = total

    for kind in range(n_kinds):
        for num in range(2):
            @pl.when(is_home)
            def _():
                arrival(kind, num, pair, 1 - core).wait_recv()
                keep(kind, num).wait()
                for unit in range(2):
                    arrival(kind, num, 1 - pair, unit).wait_send()

            @pl.when(jnp.logical_not(is_home))
            def _():
                for member in range(2):
                    for unit in range(2):
                        arrival(kind, num, member, unit).wait_recv()
                put(kind, num, 0, home_id).wait_send()

            send_row(kind, num).wait_send()
            put(kind, num, 1, pair_home_id).wait_send()
            put(kind, num, 2, across_home_id).wait_send()
        for other in range(2):
            give(kind, other, 1).wait_send()
    for idx in range(3):
        send_loss(idx).wait_send()
    for idx in range(len(spans)):
        @pl.when(sends_at(idx))
        def _():
            spread(idx).wait_send()


def sum_gradients(n_stages, loss_part, ctx_t, dhid, dqkv_t, n1, upper, grads, n2, dpre, dx):
    bf16, f32 = jnp.bfloat16, jnp.float32
    total, width = n1.shape
    ffn = upper.shape[1]
    small, mid, big = width // 8, 3 * width // 8, ffn // 8
    any_spec = pl.BlockSpec(memory_space=pl.ANY)
    vmem_spec = pl.BlockSpec(memory_space=pltpu.VMEM)
    out_shapes = [(loss_part.shape, f32), ((width, width), f32), ((3 * width, width), f32), ((ffn, width), f32), ((width, ffn), f32), (dx.shape, bf16)]
    n_spans = n_stages.bit_length() - 1
    pieces = ((small, width), (mid, width), (big, width), (width, big))
    dma = pltpu.SemaphoreType.DMA
    scratch = [pltpu.VMEM((total, width), bf16)] * 4 + [
        pltpu.VMEM((2, small, total), bf16), pltpu.VMEM((2, mid, total), bf16),
        pltpu.VMEM((2, total, big), bf16), pltpu.VMEM((2, total, big), bf16),
    ]
    scratch += [pltpu.VMEM((2,) + p, f32) for p in pieces]
    scratch += [pltpu.VMEM((2, 2) + p, f32) for p in pieces]
    scratch += [pltpu.VMEM((2,) + p, f32) for p in pieces]
    scratch += [
        pltpu.VMEM((4,) + loss_part.shape, f32),
        dma((4,)), dma((4, 2)), dma((4, 2)), dma((4, 2, 2)), dma((4, 2)), dma((4, 2)), dma((3, 4, 2)), dma((2, 2, 4, 2)),
        dma((2, 4, 2)), dma((4, 2)), dma((2, n_spans)), dma((3,)), dma((3,)), dma(()),
    ]
    flops = 2 * total * width * (4 * width + 2 * ffn)
    return pl.pallas_call(
        functools.partial(reduce_kernel, (n_stages,)),
        out_shape=[jax.ShapeDtypeStruct(s, d) for s, d in out_shapes],
        in_specs=[any_spec] * 10,
        out_specs=[vmem_spec] + [any_spec] * 5,
        scratch_shapes=scratch,
        input_output_aliases={9: 5},
        compiler_params=pltpu.CompilerParams(collective_id=1, has_side_effects=True, vmem_limit_bytes=67043328),
        cost_estimate=pl.CostEstimate(flops=flops, bytes_accessed=150 * 2 ** 20, transcendentals=0),
        name='gradient_sums',
    )(loss_part, ctx_t, dhid, dqkv_t, n1, upper, grads, n2, dpre, dx)


def solution(mesh):
    n_stages = mesh.shape['stage']
    n_data = mesh.shape['data']
    act_spec = P(('rep', 'data'))
    weight_spec = P(('rep', 'stage'))

    def per_device(embeds, targets, w_qkv, w_out, w_up, w_down):
        n_micro, micro_b, seq_len, width = embeds.shape
        heads, hdim = w_qkv.shape[2], w_qkv.shape[3]
        grad_scale = 1.0 / (n_data * n_micro)
        loss_norm = 1.0 / (n_data * n_micro * micro_b * seq_len * width)
        flat = (n_micro * micro_b, seq_len, width)
        outs = run_pipeline(
            n_stages, grad_scale, embeds.reshape(flat), targets.reshape(flat), w_qkv.reshape(3 * width, width),
            w_out.reshape(width, width), w_up[0], w_down[0], heads, hdim)
        loss_part, n1, n2, upper, ctx_t, dqkv_t, dpre, dhid, grads, dx = outs[:10]
        loss_sum, d_out, d_qkv, d_down, d_up, d_embeds = sum_gradients(
            n_stages, loss_part, ctx_t, dhid, dqkv_t, n1, upper, grads, n2, dpre, dx)
        loss = (0.5 * loss_norm * jnp.sum(loss_sum)).reshape(1)
        return (loss, d_qkv.reshape(w_qkv.shape), d_out.reshape(w_out.shape), d_up[None], d_down[None], d_embeds.reshape(embeds.shape))

    return jax.shard_map(per_device, mesh=mesh, in_specs=(act_spec, act_spec, weight_spec, weight_spec, weight_spec, weight_spec), out_specs=(P('rep'), weight_spec, weight_spec, weight_spec, weight_spec, act_spec), check_vma=False)
```

```python
import functools

import jax
import jax.numpy as jnp
from jax import lax
from jax.experimental import pallas as pl
from jax.experimental.pallas import tpu as pltpu
from jax.sharding import PartitionSpec as P

NORM_EPS = 1e-6
LOG2E = 1.4426950408889634
GELU_C = 0.7978845608028654
GELU_A = 0.044715
MESH_ID = pl.DeviceIdType.MESH
LAG_MLP = 1
GROUP = 4
ROW_BLOCK = 32


def dot_nn(lhs, rhs):
    return lax.dot_general(lhs, rhs, (((1,), (0,)), ((), ())), preferred_element_type=jnp.float32)


def dot_nt(lhs, rhs):
    return lax.dot_general(lhs, rhs, (((1,), (1,)), ((), ())), preferred_element_type=jnp.float32)


def dot_tn(lhs, rhs):
    return lax.dot_general(lhs, rhs, (((0,), (0,)), ((), ())), preferred_element_type=jnp.float32)


def rms_scale(vals):
    return lax.rsqrt(jnp.mean(vals * vals, axis=-1, keepdims=True) + NORM_EPS)


def rms_vjp(vals, cotangent):
    scale = rms_scale(vals)
    inner = jnp.mean(vals * cotangent, axis=-1, keepdims=True)
    return scale * (cotangent - vals * (scale * scale * inner))


def row_blocks(count):
    return [pl.ds(start, ROW_BLOCK) for start in range(0, count, ROW_BLOCK)]


def causal_weights(scores_t, col_max, col_inv, scale):
    half = scores_t.shape[0] // 2
    diag = lax.broadcasted_iota(jnp.int32, (half, half), 0) <= lax.broadcasted_iota(jnp.int32, (half, half), 1)
    upper_l = jnp.where(diag, scores_t[:half, :half], -1e30)
    upper_r = scores_t[:half, half:]
    lower_r = jnp.where(diag, scores_t[half:, half:], -1e30)
    fresh = col_max is None
    if fresh:
        max_l = jnp.max(upper_l, axis=0, keepdims=True)
        max_r = jnp.maximum(jnp.max(upper_r, axis=0, keepdims=True), jnp.max(lower_r, axis=0, keepdims=True))
    else:
        max_l, max_r = col_max[:, :half], col_max[:, half:]
    factor = scale * LOG2E
    exp_ul = jnp.exp2((upper_l - max_l) * factor)
    exp_ur = jnp.exp2((upper_r - max_r) * factor)
    exp_lr = jnp.exp2((lower_r - max_r) * factor)
    if fresh:
        inv_l = 1.0 / jnp.sum(exp_ul, axis=0, keepdims=True)
        inv_r = 1.0 / (jnp.sum(exp_ur, axis=0, keepdims=True) + jnp.sum(exp_lr, axis=0, keepdims=True))
        stats = (jnp.concatenate([max_l, max_r], axis=1), jnp.concatenate([inv_l, inv_r], axis=1))
    else:
        inv_l, inv_r = col_inv[:, :half], col_inv[:, half:]
        stats = None
    return (exp_ul * inv_l, exp_ur * inv_r, exp_lr * inv_r), stats


def assemble(blocks, dtype):
    upper_l, upper_r, lower_r = (b.astype(dtype) for b in blocks)
    upper = jnp.concatenate([upper_l, upper_r], axis=1)
    lower = jnp.concatenate([jnp.zeros_like(upper_l), lower_r], axis=1)
    return jnp.concatenate([upper, lower], axis=0)


def forward_layer(dims, act_ref, wqkv, wout, wup, wdown, n1_ref, qkv_ref, stat_ref, ctx_ref, hid_ref, n2_ref, gp_ref, up_ref, out_ref, flush, n1t_s, score_s, prob_s, acc_s, ready):
    heads, hdim, ffn_tile = dims
    width = heads * hdim
    ffn = wdown.shape[0]
    scale = hdim ** -0.5
    for rows in row_blocks(act_ref.shape[0]):
        act32 = act_ref[rows, :].astype(jnp.float32)
        n1_ref[rows, :] = (act32 * rms_scale(act32)).astype(jnp.bfloat16)
    n1t_s[...] = n1_ref[...].T
    ready(0)

    def rows_of(h):
        return tuple(pl.ds(part * width + h * hdim, hdim) for part in range(3))

    def project(h):
        rows = rows_of(h)
        stacked = jnp.concatenate([wqkv[r, :] for r in rows], axis=0)
        proj = dot_nn(stacked, n1t_s[...]).astype(jnp.bfloat16)
        for part, r in enumerate(rows):
            qkv_ref[r, :] = proj[part * hdim:(part + 1) * hdim]

    def score(h):
        rows = rows_of(h)
        score_s[h % 3] = dot_tn(qkv_ref[rows[1], :], qkv_ref[rows[0], :])

    def soften(h):
        blocks, stats = causal_weights(score_s.at[h % 3], None, None, scale)
        stat_ref[h, 0:1, :] = stats[0]
        stat_ref[h, 1:2, :] = stats[1]
        prob_s[h % 2] = assemble(blocks, jnp.bfloat16)

    def mix(h):
        rows = rows_of(h)
        ctx_ref[rows[0], :] = dot_nn(qkv_ref[rows[2], :], prob_s[h % 2]).astype(jnp.bfloat16)

    for step in range(heads + 5):
        for lag, action in ((0, project), (2, score), (4, soften), (5, mix)):
            h = step - lag
            if 0 <= h < heads:
                action(h)
    flush(0)
    ready(1)
    acc_s[...] = dot_tn(ctx_ref[...], wout[...])
    for rows in row_blocks(act_ref.shape[0]):
        hid16 = (act_ref[rows, :].astype(jnp.float32) + acc_s[rows, :]).astype(jnp.bfloat16)
        hid_ref[rows, :] = hid16
        hid32 = hid16.astype(jnp.float32)
        n2_ref[rows, :] = (hid32 * rms_scale(hid32)).astype(jnp.bfloat16)
    normed2 = n2_ref[...]
    flush(1)
    ready(2)
    for tile in range(ffn // ffn_tile):
        cols = pl.ds(tile * ffn_tile, ffn_tile)
        pre = dot_nn(normed2, wup[:, cols])
        gp_ref[:, cols] = pre
        tanh = jnp.tanh(pre * (GELU_C + (GELU_C * GELU_A) * (pre * pre)))
        up_ref[:, cols] = (pre * (0.5 + 0.5 * tanh)).astype(jnp.bfloat16)
    flush(2)
    ready(3)
    acc_s[...] = dot_nn(up_ref[...], wdown[...])
    for rows in row_blocks(act_ref.shape[0]):
        out_ref[rows, :] = (hid_ref[rows, :].astype(jnp.float32) + acc_s[rows, :]).astype(jnp.bfloat16)


def backward_layer(dims, grad_ref, act_ref, wqkv, wout, wup, wdown, qkv_ref, stat_ref, hid_ref, gp_ref, dpre_ref, dhid_ref, dctx_ref, dqkv_ref, dact_ref, flush, acc_s, dhid_s32, dhidt_s, score_s, dprob_s, prob_s, dscore_s):
    heads, hdim, ffn_tile = dims
    width = heads * hdim
    ffn = wdown.shape[0]
    scale = hdim ** -0.5
    grad16 = grad_ref[...]

    def slope(tile):
        cols = pl.ds(tile * ffn_tile, ffn_tile)
        dup = dot_nt(grad16, wdown[cols, :])
        pre = gp_ref[:, cols]
        pre_sq = pre * pre
        tanh = jnp.tanh(pre * (GELU_C + (GELU_C * GELU_A) * pre_sq))
        half = 0.5 + 0.5 * tanh
        bend = (half * (1.0 - half)) * (pre * (2.0 * GELU_C + (6.0 * GELU_C * GELU_A) * pre_sq))
        dpre_ref[:, cols] = (dup * (half + bend)).astype(jnp.bfloat16)

    def gather(tile):
        cols = pl.ds(tile * ffn_tile, ffn_tile)
        part = dot_nt(dpre_ref[:, cols], wup[:, cols])
        if tile == 0:
            acc_s[...] = part
        else:
            acc_s[...] += part

    tiles = ffn // ffn_tile
    for step in range(tiles + LAG_MLP):
        if step < tiles:
            slope(step)
        if step >= LAG_MLP:
            gather(step - LAG_MLP)
    flush(0)
    for rows in row_blocks(act_ref.shape[0]):
        dhid32 = grad_ref[rows, :].astype(jnp.float32) + rms_vjp(hid_ref[rows, :].astype(jnp.float32), acc_s[rows, :])
        dhid_s32[rows, :] = dhid32
        dhid_ref[rows, :] = dhid32.astype(jnp.bfloat16)
    dhidt_s[...] = dhid_ref[...].T
    flush(1)

    def rows_of(h):
        return tuple(pl.ds(part * width + h * hdim, hdim) for part in range(3))

    def project(h):
        rows = rows_of(h)[0]
        dctx_ref[rows, :] = dot_nn(wout[rows, :], dhidt_s[...]).astype(jnp.bfloat16)

    def score(h):
        rows = rows_of(h)
        score_s[h % 3] = dot_tn(qkv_ref[rows[1], :], qkv_ref[rows[0], :])
        dprob_s[h % 3] = dot_tn(qkv_ref[rows[2], :], dctx_ref[rows[0], :])

    def soften(h):
        probs, _ = causal_weights(score_s.at[h % 3], stat_ref[h, 0:1, :], stat_ref[h, 1:2, :], scale)
        dprobs = dprob_s.at[h % 3]
        half = dprobs.shape[0] // 2
        d_ul, d_ur, d_lr = dprobs[:half, :half], dprobs[:half, half:], dprobs[half:, half:]
        p_ul, p_ur, p_lr = probs
        delta_l = jnp.sum(d_ul * p_ul, axis=0, keepdims=True)
        delta_r = jnp.sum(d_ur * p_ur, axis=0, keepdims=True) + jnp.sum(d_lr * p_lr, axis=0, keepdims=True)
        prob_s[h % 2] = assemble(probs, jnp.bfloat16)
        dscore_s[h % 2] = assemble((p_ul * (d_ul - delta_l) * scale, p_ur * (d_ur - delta_r) * scale, p_lr * (d_lr - delta_r) * scale), jnp.bfloat16)

    def mix(h):
        rows = rows_of(h)
        dqkv_ref[rows[2], :] = dot_nt(dctx_ref[rows[0], :], prob_s[h % 2]).astype(jnp.bfloat16)
        dqkv_ref[rows[0], :] = dot_nn(qkv_ref[rows[1], :], dscore_s[h % 2]).astype(jnp.bfloat16)
        dqkv_ref[rows[1], :] = dot_nt(qkv_ref[rows[0], :], dscore_s[h % 2]).astype(jnp.bfloat16)

    def collect(first, count):
        spans = [pl.ds(part * width + first * hdim, count * hdim) for part in range(3)]
        part = dot_tn(jnp.concatenate([dqkv_ref[r, :] for r in spans], axis=0), jnp.concatenate([wqkv[r, :] for r in spans], axis=0))
        if first == 0:
            acc_s[...] = part
        else:
            acc_s[...] += part

    group = min(GROUP, heads)
    for step in range(heads + 5):
        for lag, action in ((0, project), (2, score), (4, soften), (5, mix)):
            h = step - lag
            if 0 <= h < heads:
                action(h)
        done = step - 6
        if done >= 0 and done % group == group - 1 and done < heads - group:
            collect(done - group + 1, group)
    flush(2)
    collect(heads - group, group)
    for rows in row_blocks(act_ref.shape[0]):
        dact = dhid_s32[rows, :] + rms_vjp(act_ref[rows, :].astype(jnp.float32), acc_s[rows, :])
        dact_ref[rows, :] = dact.astype(jnp.bfloat16)


class placement:
    def __init__(self, n_stages):
        row = lax.axis_index('data')
        self.row = row
        self.index = lax.axis_index('stage')
        self.column = lax.div(self.index, 2)
        self.core = lax.rem(self.index, 2)
        self.upper = lax.div(row, 2)
        self.half = lax.rem(self.upper + self.column, 2)
        self.layer = 2 * self.column + self.half
        self.home = self.layer
        self.mate = 2 * self.column + 1 - self.core
        across = 3 - row
        along = lax.rem(self.index + jnp.where(self.half == 1, 2, n_stages - 2), n_stages)
        self.mate_id = {'data': row, 'stage': self.mate}
        self.across_id = {'data': across, 'stage': self.index}
        self.along_id = {'data': row, 'stage': along}
        self.next_id = {'data': jnp.where(self.half == 1, row, across), 'stage': jnp.where(self.half == 1, along, self.index)}
        self.prev_id = {'data': jnp.where(self.half == 1, across, row), 'stage': jnp.where(self.half == 1, self.index, along)}


def pipeline_kernel(
    cfg,
    emb_hbm, tgt_hbm, wqkv_hbm, wout_hbm, wup_hbm, wdown_hbm,
    loss_ref, n1_hbm, n2_hbm, up_hbm, ctx_hbm, dqkv_hbm, dpre_hbm, dhid_hbm, g_hbm, dx_hbm, qkv_hbm, gp_hbm, hid_hbm, stat_hbm,
    wqkv, wout, wup, wdown, act, grad, out_s, dact_s,
    n1_s, n2_s, up_s, ctx_s, qkv_s, gp_s, hid_s, stat_s,
    dpre_s, dhid_s, dctx_s, dqkv_s,
    w_sem, in_sem, act_sem, grad_sem, fout_sem, bin_sem, bout_sem, fsend_sem, bsend_sem, loss_acc, loss_sem, dx_sem, n1t_s, score_s, prob_s, dprob_s, dscore_s, acc_s, dhid_s32,
):
    n_stages, n_seq, tokens, grad_scale, dims = cfg
    here = placement(n_stages)
    stage, core, next_id, prev_id = here.layer, here.core, here.next_id, here.prev_id
    is_first = stage == 0
    is_last = stage == n_stages - 1
    own_weights = here.layer == here.index
    own_data = here.upper == core
    feeds_first = (here.column == 0) & (here.half == 1) & (core == 1)
    feeds_last = (here.column == n_stages // 2 - 1) & (here.half == 0) & (core == 1)

    weight_pairs = ((wqkv_hbm, wqkv), (wout_hbm, wout), (wup_hbm, wup), (wdown_hbm, wdown))

    def load_weight(idx):
        return pltpu.make_async_copy(weight_pairs[idx][0], weight_pairs[idx][1], w_sem.at[idx])

    def give_weight(idx):
        return pltpu.make_async_remote_copy(
            src_ref=weight_pairs[idx][0], dst_ref=weight_pairs[idx][1], send_sem=w_sem.at[4 + idx], recv_sem=w_sem.at[8 + idx],
            device_id=here.mate_id, device_id_type=MESH_ID)

    def load_embed(m):
        return pltpu.make_async_copy(emb_hbm.at[m], act.at[m], in_sem.at[m])

    def load_target(m):
        return pltpu.make_async_copy(tgt_hbm.at[m], grad.at[m], in_sem.at[m])

    def give_embed(m):
        return pltpu.make_async_remote_copy(
            src_ref=emb_hbm.at[m], dst_ref=act.at[m], send_sem=in_sem.at[m], recv_sem=act_sem.at[m],
            device_id=here.across_id, device_id_type=MESH_ID)

    def give_target(m):
        return pltpu.make_async_remote_copy(
            src_ref=tgt_hbm.at[m], dst_ref=grad.at[m], send_sem=in_sem.at[m], recv_sem=grad_sem.at[m],
            device_id=here.across_id, device_id_type=MESH_ID)

    def each_seq(when, action):
        @pl.when(when)
        def _():
            def go(m, carry):
                action(m)
                return carry
            lax.fori_loop(0, n_seq, go, 0)

    @pl.when(own_weights)
    def _():
        for idx in range(4):
            load_weight(idx).start()

    each_seq(is_first & own_data, lambda m: load_embed(m).start())
    each_seq(is_last & own_data, lambda m: load_target(m).start())

    barrier = pltpu.get_barrier_semaphore()
    for peer in (here.mate_id, here.across_id, here.along_id):
        pl.semaphore_signal(barrier, inc=1, device_id=peer, device_id_type=MESH_ID)
    pl.semaphore_wait(barrier, 3)

    @pl.when(own_weights)
    def _():
        for idx in range(4):
            give_weight(idx).start()

    each_seq(feeds_first, lambda m: give_embed(m).start())
    each_seq(feeds_last, lambda m: give_target(m).start())
    loss_acc[...] = jnp.zeros_like(loss_acc)

    def await_weight(idx):
        @pl.when(own_weights)
        def _():
            load_weight(idx).wait()

        @pl.when(jnp.logical_not(own_weights))
        def _():
            give_weight(idx).wait_recv()

    def send_act(m, slot):
        return pltpu.make_async_remote_copy(
            src_ref=out_s.at[slot], dst_ref=act.at[m], send_sem=fsend_sem.at[slot], recv_sem=act_sem.at[m],
            device_id=next_id, device_id_type=MESH_ID)

    def send_grad(m, slot):
        return pltpu.make_async_remote_copy(
            src_ref=dact_s.at[slot], dst_ref=grad.at[m], send_sem=bsend_sem.at[slot], recv_sem=grad_sem.at[m],
            device_id=prev_id, device_id_type=MESH_ID)

    def store_dx(m, slot):
        return pltpu.make_async_copy(dact_s.at[slot], dx_hbm.at[m], bsend_sem.at[slot])

    def give_dx(m, slot):
        return pltpu.make_async_remote_copy(
            src_ref=dact_s.at[slot], dst_ref=dx_hbm.at[m], send_sem=bsend_sem.at[slot], recv_sem=dx_sem.at[m],
            device_id=here.across_id, device_id_type=MESH_ID)

    def token_range(m):
        return pl.ds(pl.multiple_of(m * tokens, tokens), tokens)

    def fout_copies(m, slot):
        rows = token_range(m)
        return (
            (0, pltpu.make_async_copy(n1_s.at[slot], n1_hbm.at[rows, :], fout_sem.at[slot, 0])),
            (0, pltpu.make_async_copy(qkv_s.at[slot], qkv_hbm.at[m], fout_sem.at[slot, 1])),
            (1, pltpu.make_async_copy(ctx_s.at[slot], ctx_hbm.at[:, rows], fout_sem.at[slot, 2])),
            (1, pltpu.make_async_copy(stat_s.at[slot], stat_hbm.at[m], fout_sem.at[slot, 3])),
            (1, pltpu.make_async_copy(hid_s.at[slot], hid_hbm.at[m], fout_sem.at[slot, 4])),
            (1, pltpu.make_async_copy(n2_s.at[slot], n2_hbm.at[rows, :], fout_sem.at[slot, 5])),
            (2, pltpu.make_async_copy(gp_s.at[slot], gp_hbm.at[m], fout_sem.at[slot, 6])),
            (2, pltpu.make_async_copy(up_s.at[slot], up_hbm.at[rows, :], fout_sem.at[slot, 7])),
        )

    def bin_copies(m):
        return (
            pltpu.make_async_copy(qkv_hbm.at[m], qkv_s.at[2], bin_sem.at[0]),
            pltpu.make_async_copy(stat_hbm.at[m], stat_s.at[2], bin_sem.at[1]),
            pltpu.make_async_copy(hid_hbm.at[m], hid_s.at[2], bin_sem.at[2]),
            pltpu.make_async_copy(gp_hbm.at[m], gp_s.at[2], bin_sem.at[3]),
        )

    def bout_copies(m, slot):
        rows = token_range(m)
        return (
            (0, pltpu.make_async_copy(grad.at[m], g_hbm.at[rows, :], bout_sem.at[slot, 0])),
            (0, pltpu.make_async_copy(dpre_s.at[slot], dpre_hbm.at[rows, :], bout_sem.at[slot, 1])),
            (1, pltpu.make_async_copy(dhid_s.at[slot], dhid_hbm.at[rows, :], bout_sem.at[slot, 2])),
            (2, pltpu.make_async_copy(dqkv_s.at[slot], dqkv_hbm.at[:, rows], bout_sem.at[slot, 3])),
        )

    def flusher(copies):
        def flush(group):
            for when, copy in copies:
                if when == group:
                    copy.start()
        return flush

    def in_range(m):
        return (m >= 0) & (m < n_seq)

    def tick(t, carry):
        fwd_m = t - stage
        bwd_m = t + stage - (2 * n_stages - 2)

        @pl.when(in_range(fwd_m))
        def _():
            m = fwd_m
            slot = lax.rem(m, 2)

            @pl.when(is_first & own_data)
            def _():
                load_embed(m).wait()

            @pl.when(jnp.logical_not(is_first & own_data))
            def _():
                send_act(m, slot).wait_recv()

            def run_forward(ready):
                forward_layer(
                    dims, act.at[m], wqkv, wout, wup, wdown, n1_s.at[slot], qkv_s.at[slot], stat_s.at[slot],
                    ctx_s.at[slot], hid_s.at[slot], n2_s.at[slot], gp_s.at[slot], up_s.at[slot], out_s.at[slot],
                    flusher(fout_copies(m, slot)), n1t_s, score_s, prob_s, acc_s, ready)

            @pl.when(m == 0)
            def _():
                run_forward(await_weight)

            @pl.when(m > 0)
            def _():
                run_forward(lambda idx: None)

            @pl.when(jnp.logical_not(is_last))
            def _():
                send_act(m, slot).start()

            @pl.when(is_last & own_data)
            def _():
                load_target(m).wait()

            @pl.when(is_last & jnp.logical_not(own_data))
            def _():
                send_grad(m, slot).wait_recv()

            @pl.when(is_last)
            def _():
                for start in range(0, tokens, 32):
                    rows = pl.ds(start, 32)
                    error = out_s[slot, rows, :].astype(jnp.float32) - grad[m, rows, :].astype(jnp.float32)
                    square = error * error
                    loss_acc[...] += (square[0:8] + square[8:16]) + (square[16:24] + square[24:32])
                    grad[m, rows, :] = (error * grad_scale).astype(jnp.bfloat16)

        @pl.when(in_range(bwd_m))
        def _():
            m = bwd_m
            slot = lax.rem(m, 2)

            @pl.when(jnp.logical_not(is_last))
            def _():
                for copy in bin_copies(m):
                    copy.wait()
                send_grad(m, slot).wait_recv()

            saved = jnp.where(is_last, slot, 2)
            backward_layer(
                dims, grad.at[m], act.at[m], wqkv, wout, wup, wdown, qkv_s.at[saved], stat_s.at[saved], hid_s.at[saved],
                gp_s.at[saved], dpre_s.at[slot], dhid_s.at[slot], dctx_s, dqkv_s.at[slot], dact_s.at[slot],
                flusher(bout_copies(m, slot)), acc_s, dhid_s32, n1t_s, score_s, dprob_s, prob_s, dscore_s)

            @pl.when(jnp.logical_not(is_first))
            def _():
                send_grad(m, slot).start()

            @pl.when(is_first & own_data)
            def _():
                store_dx(m, slot).start()

            @pl.when(is_first & jnp.logical_not(own_data))
            def _():
                give_dx(m, slot).start()

        fwd_old = fwd_m - 1
        bwd_old = bwd_m - 1

        @pl.when(in_range(fwd_old))
        def _():
            slot = lax.rem(fwd_old, 2)
            for _, copy in fout_copies(fwd_old, slot):
                copy.wait()

            @pl.when(jnp.logical_not(is_last))
            def _():
                send_act(fwd_old, slot).wait_send()

        @pl.when(in_range(bwd_old))
        def _():
            slot = lax.rem(bwd_old, 2)
            for _, copy in bout_copies(bwd_old, slot):
                copy.wait()

            @pl.when(jnp.logical_not(is_first))
            def _():
                send_grad(bwd_old, slot).wait_send()

            @pl.when(is_first & own_data)
            def _():
                store_dx(bwd_old, slot).wait()

            @pl.when(is_first & jnp.logical_not(own_data))
            def _():
                give_dx(bwd_old, slot).wait_send()

        @pl.when(in_range(bwd_m + 1) & jnp.logical_not(is_last))
        def _():
            for copy in bin_copies(bwd_m + 1):
                copy.start()

        return carry

    lax.fori_loop(0, n_seq + 2 * n_stages - 1, tick, 0)

    def send_loss():
        return pltpu.make_async_remote_copy(
            src_ref=loss_ref, dst_ref=loss_ref, send_sem=loss_sem.at[0], recv_sem=loss_sem.at[1],
            device_id=prev_id, device_id_type=MESH_ID)

    @pl.when(is_last)
    def _():
        lanes = loss_ref.shape[1]
        total = loss_acc[:, 0:lanes]
        for col in range(lanes, loss_acc.shape[1], lanes):
            total = total + loss_acc[:, col:col + lanes]
        loss_ref[...] = total

    @pl.when(jnp.logical_not(is_last))
    def _():
        send_loss().wait_recv()

    @pl.when(jnp.logical_not(is_first))
    def _():
        send_loss().start()
        send_loss().wait_send()

    @pl.when(own_weights)
    def _():
        for idx in range(4):
            give_weight(idx).wait_send()

    each_seq(feeds_first, lambda m: give_embed(m).wait_send())
    each_seq(feeds_last, lambda m: give_target(m).wait_send())
    each_seq(feeds_first, lambda m: give_dx(m, 0).wait_recv())


def run_pipeline(n_stages, grad_scale, embeds, targets, wqkv, wout, wup, wdown, heads, hdim):
    n_seq, tokens, width = embeds.shape
    ffn = wdown.shape[0]
    dims = (heads, hdim, 512 if ffn % 512 == 0 else ffn)
    bf16, f32 = jnp.bfloat16, jnp.float32
    total = n_seq * tokens
    out_shapes = [
        ((8, 128), f32),
        ((total, width), bf16),
        ((total, width), bf16),
        ((total, ffn), bf16),
        ((width, total), bf16),
        ((3 * width, total), bf16),
        ((total, ffn), bf16),
        ((total, width), bf16),
        ((total, width), bf16),
        ((n_seq, tokens, width), bf16),
        ((n_seq, 3 * width, tokens), bf16),
        ((n_seq, tokens, ffn), f32),
        ((n_seq, tokens, width), bf16),
        ((n_seq, heads, 8, tokens), f32),
    ]
    any_spec = pl.BlockSpec(memory_space=pl.ANY)
    scratch = [
        pltpu.VMEM(wqkv.shape, bf16), pltpu.VMEM(wout.shape, bf16), pltpu.VMEM(wup.shape, bf16), pltpu.VMEM(wdown.shape, bf16),
        pltpu.VMEM((n_seq, tokens, width), bf16), pltpu.VMEM((n_seq, tokens, width), bf16),
        pltpu.VMEM((2, tokens, width), bf16), pltpu.VMEM((2, tokens, width), bf16),
        pltpu.VMEM((2, tokens, width), bf16), pltpu.VMEM((2, tokens, width), bf16),
        pltpu.VMEM((2, tokens, ffn), bf16), pltpu.VMEM((2, width, tokens), bf16),
        pltpu.VMEM((3, 3 * width, tokens), bf16), pltpu.VMEM((3, tokens, ffn), f32),
        pltpu.VMEM((3, tokens, width), bf16), pltpu.VMEM((3, heads, 8, tokens), f32),
        pltpu.VMEM((2, tokens, ffn), bf16), pltpu.VMEM((2, tokens, width), bf16),
        pltpu.VMEM((width, tokens), bf16), pltpu.VMEM((2, 3 * width, tokens), bf16),
        pltpu.SemaphoreType.DMA((12,)), pltpu.SemaphoreType.DMA((n_seq,)),
        pltpu.SemaphoreType.DMA((n_seq,)), pltpu.SemaphoreType.DMA((n_seq,)),
        pltpu.SemaphoreType.DMA((2, 8)), pltpu.SemaphoreType.DMA((4,)), pltpu.SemaphoreType.DMA((2, 4)),
        pltpu.SemaphoreType.DMA((2,)), pltpu.SemaphoreType.DMA((2,)),
        pltpu.VMEM((8, width), f32), pltpu.SemaphoreType.DMA((2,)), pltpu.SemaphoreType.DMA((n_seq,)),
        pltpu.VMEM((width, tokens), bf16), pltpu.VMEM((3, tokens, tokens), f32), pltpu.VMEM((2, tokens, tokens), bf16),
        pltpu.VMEM((3, tokens, tokens), f32), pltpu.VMEM((2, tokens, tokens), bf16), pltpu.VMEM((tokens, width), f32), pltpu.VMEM((tokens, width), f32),
    ]
    linear = 2 * total * (wqkv.size + wout.size + wup.size + wdown.size)
    return pl.pallas_call(
        functools.partial(pipeline_kernel, (n_stages, n_seq, tokens, grad_scale, dims)),
        out_shape=[jax.ShapeDtypeStruct(s, d) for s, d in out_shapes],
        in_specs=[any_spec] * 6,
        out_specs=[pl.BlockSpec(memory_space=pltpu.VMEM)] + [any_spec] * (len(out_shapes) - 1),
        scratch_shapes=scratch,
        compiler_params=pltpu.CompilerParams(collective_id=0, has_side_effects=True, vmem_limit_bytes=67043328),
        cost_estimate=pl.CostEstimate(flops=3 * linear, bytes_accessed=200 * 2 ** 20, transcendentals=0),
        name='stage_pipeline',
    )(embeds, targets, wqkv, wout, wup, wdown)


def reduce_kernel(
    cfg,
    loss_hbm, ctx_hbm, dhid_hbm, dqkv_hbm, n1_hbm, up_hbm, g_hbm, n2_hbm, dpre_hbm, dx_hbm,
    loss_ref, dout_hbm, dqkvw_hbm, ddown_hbm, dup_hbm, demb_hbm,
    out_res, qkv_res, down_res, up_res, out_in, qkv_in, down_in, up_in,
    out_give, qkv_give, down_give, up_give, out_core, qkv_core, down_core, up_core, out_row, qkv_row, down_row, up_row, loss_sl,
    res_sem, in_sem, give_sem, core_sem, row_send, row_recv, put_send, put_recv, pass_send, store_sem, dx_sem,
    loss_send, loss_recv, loss_in,
):
    (n_stages,) = cfg
    here = placement(n_stages)
    row, core, stage = here.row, here.core, here.index
    pair = lax.rem(row, 2)
    pair_row = row + 1 - 2 * pair
    across = 3 - row
    is_home = here.home == stage
    home_id = {'data': row, 'stage': here.home}
    pair_id = {'data': pair_row, 'stage': stage}
    pair_home_id = {'data': pair_row, 'stage': here.home}
    across_home_id = {'data': across, 'stage': here.home}

    kinds = (
        ('rows', dhid_hbm, out_res, ctx_hbm, out_in, out_give, out_core, out_row, dout_hbm),
        ('rows', n1_hbm, qkv_res, dqkv_hbm, qkv_in, qkv_give, qkv_core, qkv_row, dqkvw_hbm),
        ('tall', g_hbm, down_res, up_hbm, down_in, down_give, down_core, down_row, ddown_hbm),
        ('wide', n2_hbm, up_res, dpre_hbm, up_in, up_give, up_core, up_row, dup_hbm),
    )
    n_kinds = len(kinds)
    turns = ((1, 1), (0, 1), (1, 0), (0, 0))

    def piece(kind, member, unit, num):
        size = kinds[kind][4].shape[1 if kinds[kind][0] == 'rows' else 2]
        return pl.ds(pl.multiple_of(((member * 2 + unit) * 2 + num) * size, size), size)

    def flip(val, by):
        return 1 - val if by else val

    def read_piece(kind, turn, num):
        form, _, _, src, buf = kinds[kind][:5]
        part = piece(kind, flip(pair, turns[turn][0]), flip(core, turns[turn][1]), num)
        view = src.at[part, :] if form == 'rows' else src.at[:, part]
        return pltpu.make_async_copy(view, buf.at[turn % 2], in_sem.at[kind, turn % 2])

    def out_view(kind, member, unit, num):
        part = piece(kind, member, unit, num)
        dst = kinds[kind][8]
        return dst.at[:, part] if kinds[kind][0] == 'wide' else dst.at[part, :]

    tile = min(256, out_res.shape[1])
    n_tiles = out_res.shape[1] // tile

    def tile_at(kind, n):
        span = pl.ds(pl.multiple_of(n * tile, tile), tile)
        return (span, slice(None)) if kinds[kind][0] == 'wide' else (slice(None), span)

    def each_tile(action):
        def body(n, carry):
            action(n)
            return carry
        lax.fori_loop(0, n_tiles, body, 0)

    def give(kind, other, num):
        return pltpu.make_async_remote_copy(
            src_ref=kinds[kind][5].at[other], dst_ref=kinds[kind][6].at[num, other], send_sem=give_sem.at[kind, other],
            recv_sem=core_sem.at[kind, num, other], device_id=here.mate_id, device_id_type=MESH_ID)

    def send_row(kind, num, n):
        at = tile_at(kind, n)
        return pltpu.make_async_remote_copy(
            src_ref=kinds[kind][6].at[(num, 1) + at], dst_ref=kinds[kind][7].at[(num,) + at], send_sem=row_send.at[kind, num, n],
            recv_sem=row_recv.at[kind, num, n], device_id=pair_id, device_id_type=MESH_ID)

    def put_view(kind, member, unit, num, n):
        part = piece(kind, member, unit, num)
        span = pl.ds(pl.multiple_of(n * tile, tile), tile)
        dst = kinds[kind][8]
        return dst.at[span, part] if kinds[kind][0] == 'wide' else dst.at[part, span]

    def put(kind, num, n, target, device_id):
        return pltpu.make_async_remote_copy(
            src_ref=kinds[kind][7].at[(num,) + tile_at(kind, n)], dst_ref=put_view(kind, pair, core, num, n),
            send_sem=put_send.at[target, kind, num, n], recv_sem=put_recv.at[pair, core, kind, num, n],
            device_id=device_id, device_id_type=MESH_ID)

    def keep(kind, num):
        return pltpu.make_async_copy(kinds[kind][7].at[num], out_view(kind, pair, core, num), store_sem.at[kind, num])

    def arrival(kind, num, n, member, unit):
        view = put_view(kind, member, unit, num, n)
        return pltpu.make_async_remote_copy(
            src_ref=view, dst_ref=view, send_sem=pass_send.at[unit, kind, num, n], recv_sem=put_recv.at[member, unit, kind, num, n],
            device_id=across_home_id, device_id_type=MESH_ID)

    def load_resident(kind):
        return pltpu.make_async_copy(kinds[kind][1], kinds[kind][2], res_sem.at[kind])

    def pipeline_id(row_idx, unit):
        return 2 * jnp.minimum(row_idx, 3 - row_idx) + unit

    my_loss = pltpu.make_async_copy(loss_hbm, loss_sl.at[pipeline_id(row, core)], loss_in)
    my_loss.start()
    for kind in range(n_kinds):
        load_resident(kind).start()
        read_piece(kind, 0, 0).start()

    source = here.upper
    rank = stage + source - 2 * source * core
    spans = []
    span = n_stages // 2
    while span >= 1:
        spans.append(span)
        span //= 2

    def swapped(span):
        return stage + span - 2 * span * lax.rem(lax.div(stage, span), 2)

    loss_ids = (
        ({'data': row, 'stage': here.mate}, row, 1 - core),
        ({'data': pair_row, 'stage': stage}, pair_row, core),
        ({'data': pair_row, 'stage': here.mate}, pair_row, 1 - core),
    )
    peers = [ident for ident, _, _ in loss_ids]
    peers += [{'data': across, 'stage': stage}, {'data': across, 'stage': here.mate}]
    peers += [{'data': row, 'stage': swapped(span)} for span in spans if span > 1]
    barrier = pltpu.get_barrier_semaphore()
    for ident in peers:
        pl.semaphore_signal(barrier, inc=1, device_id=ident, device_id_type=MESH_ID)
    pl.semaphore_wait(barrier, len(peers))

    def send_loss(idx):
        slot = loss_sl.at[pipeline_id(row, core)]
        return pltpu.make_async_remote_copy(
            src_ref=slot, dst_ref=slot, send_sem=loss_send.at[idx], recv_sem=loss_recv.at[idx],
            device_id=loss_ids[idx][0], device_id_type=MESH_ID)

    def loss_arrival(idx):
        slot = loss_sl.at[pipeline_id(loss_ids[idx][1], loss_ids[idx][2])]
        return pltpu.make_async_remote_copy(
            src_ref=slot, dst_ref=slot, send_sem=loss_send.at[idx], recv_sem=loss_recv.at[idx],
            device_id=loss_ids[idx][0], device_id_type=MESH_ID)

    my_loss.wait()
    for idx in range(3):
        send_loss(idx).start()

    def spread(idx):
        return pltpu.make_async_remote_copy(
            src_ref=demb_hbm, dst_ref=demb_hbm, send_sem=dx_sem.at[0, idx], recv_sem=dx_sem.at[1, idx],
            device_id={'data': row, 'stage': swapped(spans[idx])}, device_id_type=MESH_ID)

    def sends_at(idx):
        return lax.rem(rank, 2 * spans[idx]) == 0

    def receives_at(idx):
        return lax.rem(rank, 2 * spans[idx]) == spans[idx]

    def spread_round(idx):
        if idx > 0:
            @pl.when(receives_at(idx - 1))
            def _():
                spread(idx - 1).wait_recv()
        if idx < len(spans):
            @pl.when(sends_at(idx))
            def _():
                spread(idx).start()

    def product(kind, turn, num, sink, base, before=None, after=None):
        form, _, res, _, buf = kinds[kind][:5]
        read_piece(kind, turn, num).wait()
        if turn < 3:
            read_piece(kind, turn + 1, num).start()
        else:
            @pl.when(num == 0)
            def _():
                read_piece(kind, 0, 1).start()
        fed = buf.at[turn % 2]

        def body(n):
            at = tile_at(kind, n)
            span = pl.ds(pl.multiple_of(n * tile, tile), tile)
            if before is not None:
                before(n)
            if form == 'rows':
                part = dot_nn(fed[...], res[:, span])
            elif form == 'tall':
                part = dot_tn(fed[...], res[:, span])
            else:
                part = dot_tn(res[:, span], fed[...])
            for ref in base:
                part = part + ref[at]
            sink[at] = part
            if after is not None:
                after(n)

        each_tile(body)

    def first_half(kind, num):
        give_buf, core_buf = kinds[kind][5:7]

        @pl.when(num == 0)
        def _():
            load_resident(kind).wait()

        for turn, other in ((0, 1), (1, 0)):
            @pl.when(num > 0)
            def _():
                give(kind, other, num - 1).wait_send()

            product(kind, turn, num, give_buf.at[other], ())
            give(kind, other, num).start()
        give(kind, 1, num).wait_recv()
        product(kind, 2, num, core_buf.at[num, 1], (core_buf.at[num, 1],), after=lambda n: send_row(kind, num, n).start())

    def second_half(kind, num):
        core_buf, row_buf = kinds[kind][6:8]
        give(kind, 0, num).wait_recv()

        def after(n):
            put(kind, num, n, 1, pair_home_id).start()
            put(kind, num, n, 2, across_home_id).start()

            @pl.when(jnp.logical_not(is_home))
            def _():
                put(kind, num, n, 0, home_id).start()

        product(kind, 3, num, row_buf.at[num], (core_buf.at[num, 0], row_buf.at[num]),
                before=lambda n: send_row(kind, num, n).wait_recv(), after=after)

        @pl.when(is_home)
        def _():
            keep(kind, num).start()

    def pass_on(kind, num):
        @pl.when(is_home)
        def _():
            def go(n):
                for unit in range(2):
                    arrival(kind, num, n, 1 - pair, unit).wait_recv()
                    arrival(kind, num, n, 1 - pair, unit).start()
            each_tile(go)

    def kind_at(pos):
        late = jnp.where(pos == 4, 2, jnp.where(pos == 5, 3, jnp.where(pos == 6, 1, 0)))
        return jnp.where(pos < 4, pos, late)

    def num_at(pos):
        return jnp.where(pos < 4, 0, 1)

    n_steps = 2 * n_kinds

    def step_body(pos, carry):
        for kind in range(n_kinds):
            @pl.when((pos < n_steps) & (kind_at(pos) == kind))
            def _():
                first_half(kind, num_at(pos))

        for kind in range(n_kinds):
            @pl.when((pos >= 1) & (pos < n_steps + 1) & (kind_at(pos - 1) == kind))
            def _():
                second_half(kind, num_at(pos - 1))

        for kind in range(n_kinds):
            @pl.when((pos >= 2) & (kind_at(pos - 2) == kind))
            def _():
                pass_on(kind, num_at(pos - 2))

        for idx in range(len(spans) + 1):
            @pl.when(pos == 3 * idx)
            def _():
                spread_round(idx)
        return carry

    lax.fori_loop(0, n_steps + 2, step_body, 0)

    for idx in range(3):
        loss_arrival(idx).wait_recv()
    total = loss_sl[0]
    for idx in range(1, 4):
        total = total + loss_sl[idx]
    loss_ref[...] = total

    for kind in range(n_kinds):
        for num in range(2):
            def settle(n):
                @pl.when(is_home)
                def _():
                    arrival(kind, num, n, pair, 1 - core).wait_recv()
                    for unit in range(2):
                        arrival(kind, num, n, 1 - pair, unit).wait_send()

                @pl.when(jnp.logical_not(is_home))
                def _():
                    for member in range(2):
                        for unit in range(2):
                            arrival(kind, num, n, member, unit).wait_recv()
                    put(kind, num, n, 0, home_id).wait_send()

                send_row(kind, num, n).wait_send()
                put(kind, num, n, 1, pair_home_id).wait_send()
                put(kind, num, n, 2, across_home_id).wait_send()

            each_tile(settle)

            @pl.when(is_home)
            def _():
                keep(kind, num).wait()
        for other in range(2):
            give(kind, other, 1).wait_send()
    for idx in range(3):
        send_loss(idx).wait_send()
    for idx in range(len(spans)):
        @pl.when(sends_at(idx))
        def _():
            spread(idx).wait_send()


def sum_gradients(n_stages, loss_part, ctx_t, dhid, dqkv_t, n1, upper, grads, n2, dpre, dx):
    bf16, f32 = jnp.bfloat16, jnp.float32
    total, width = n1.shape
    ffn = upper.shape[1]
    small, mid, big = width // 8, 3 * width // 8, ffn // 8
    any_spec = pl.BlockSpec(memory_space=pl.ANY)
    vmem_spec = pl.BlockSpec(memory_space=pltpu.VMEM)
    out_shapes = [(loss_part.shape, f32), ((width, width), f32), ((3 * width, width), f32), ((ffn, width), f32), ((width, ffn), f32), (dx.shape, bf16)]
    n_spans = n_stages.bit_length() - 1
    n_tiles = max(1, width // 256)
    pieces = ((small, width), (mid, width), (big, width), (width, big))
    dma = pltpu.SemaphoreType.DMA
    scratch = [pltpu.VMEM((total, width), bf16)] * 4 + [
        pltpu.VMEM((2, small, total), bf16), pltpu.VMEM((2, mid, total), bf16),
        pltpu.VMEM((2, total, big), bf16), pltpu.VMEM((2, total, big), bf16),
    ]
    scratch += [pltpu.VMEM((2,) + p, f32) for p in pieces]
    scratch += [pltpu.VMEM((2, 2) + p, f32) for p in pieces]
    scratch += [pltpu.VMEM((2,) + p, f32) for p in pieces]
    scratch += [
        pltpu.VMEM((4,) + loss_part.shape, f32),
        dma((4,)), dma((4, 2)), dma((4, 2)), dma((4, 2, 2)), dma((4, 2, n_tiles)), dma((4, 2, n_tiles)),
        dma((3, 4, 2, n_tiles)), dma((2, 2, 4, 2, n_tiles)), dma((2, 4, 2, n_tiles)), dma((4, 2)), dma((2, n_spans)), dma((3,)), dma((3,)), dma(()),
    ]
    flops = 2 * total * width * (4 * width + 2 * ffn)
    return pl.pallas_call(
        functools.partial(reduce_kernel, (n_stages,)),
        out_shape=[jax.ShapeDtypeStruct(s, d) for s, d in out_shapes],
        in_specs=[any_spec] * 10,
        out_specs=[vmem_spec] + [any_spec] * 5,
        scratch_shapes=scratch,
        input_output_aliases={9: 5},
        compiler_params=pltpu.CompilerParams(collective_id=1, has_side_effects=True, vmem_limit_bytes=67043328),
        cost_estimate=pl.CostEstimate(flops=flops, bytes_accessed=150 * 2 ** 20, transcendentals=0),
        name='gradient_sums',
    )(loss_part, ctx_t, dhid, dqkv_t, n1, upper, grads, n2, dpre, dx)


def settle_kernel(plan, loss_factor, loss_in, *refs):
    count = len(plan)
    sources, loss_ref, results = refs[:count], refs[count], refs[count + 1:2 * count + 1]
    holds, sem = refs[2 * count + 1:-1], refs[-1]
    copies = []
    for src, hold, dst, parts in zip(sources, holds, results, plan):
        lead = src.shape[0] // parts
        for idx in range(parts):
            part = pl.ds(idx * lead, lead)
            num = len(copies)
            copies.append((
                pltpu.make_async_copy(src.at[part], hold.at[part], sem.at[0, num]),
                pltpu.make_async_copy(hold.at[part], dst.at[part], sem.at[1, num])))
    for read, _ in copies:
        read.start()
    loss_ref[0] = loss_factor * jnp.sum(loss_in[...])
    for read, write in copies:
        read.wait()
        write.start()
    for _, write in copies:
        write.wait()


def settle(loss_factor, loss_sum, arrays):
    plan = tuple(next(p for p in (4, 3, 2, 1) if arr.shape[0] % (16 * p) == 0 or p == 1 or (arr.ndim == 3 and arr.shape[0] % p == 0)) for arr in arrays)
    any_spec = pl.BlockSpec(memory_space=pl.ANY)
    outs = pl.pallas_call(
        functools.partial(settle_kernel, plan, loss_factor),
        out_shape=[jax.ShapeDtypeStruct((1,), jnp.float32)] + [jax.ShapeDtypeStruct(arr.shape, arr.dtype) for arr in arrays],
        in_specs=[pl.BlockSpec(memory_space=pltpu.VMEM)] + [any_spec] * len(arrays),
        out_specs=[pl.BlockSpec(memory_space=pltpu.SMEM)] + [any_spec] * len(arrays),
        scratch_shapes=[pltpu.VMEM(arr.shape, arr.dtype) for arr in arrays] + [pltpu.SemaphoreType.DMA((2, sum(plan)))],
        compiler_params=pltpu.CompilerParams(vmem_limit_bytes=60 * 2 ** 20),
        name='settle_results',
    )(loss_sum, *arrays)
    return outs[0], outs[1:]


def solution(mesh):
    n_stages = mesh.shape['stage']
    n_data = mesh.shape['data']
    act_spec = P(('rep', 'data'))
    weight_spec = P(('rep', 'stage'))

    def per_device(embeds, targets, w_qkv, w_out, w_up, w_down):
        n_micro, micro_b, seq_len, width = embeds.shape
        heads, hdim = w_qkv.shape[2], w_qkv.shape[3]
        grad_scale = 1.0 / (n_data * n_micro)
        loss_norm = 1.0 / (n_data * n_micro * micro_b * seq_len * width)
        flat = (n_micro * micro_b, seq_len, width)
        outs = run_pipeline(
            n_stages, grad_scale, embeds.reshape(flat), targets.reshape(flat), w_qkv.reshape(3 * width, width),
            w_out.reshape(width, width), w_up[0], w_down[0], heads, hdim)
        loss_part, n1, n2, upper, ctx_t, dqkv_t, dpre, dhid, grads, dx = outs[:10]
        loss_sum, *sums = sum_gradients(
            n_stages, loss_part, ctx_t, dhid, dqkv_t, n1, upper, grads, n2, dpre, dx)
        loss, (d_out, d_qkv, d_down, d_up, d_embeds) = settle(0.5 * loss_norm, loss_sum, sums)
        return (loss, d_qkv.reshape(w_qkv.shape), d_out.reshape(w_out.shape), d_up[None], d_down[None], d_embeds.reshape(embeds.shape))

    return jax.shard_map(per_device, mesh=mesh, in_specs=(act_spec, act_spec, weight_spec, weight_spec, weight_spec, weight_spec), out_specs=(P('rep'), weight_spec, weight_spec, weight_spec, weight_spec, act_spec), check_vma=False)
```

```python
import functools

import jax
import jax.numpy as jnp
from jax import lax
from jax.experimental import pallas as pl
from jax.experimental.pallas import tpu as pltpu
from jax.sharding import PartitionSpec as P

NORM_EPS = 1e-6
LOG2E = 1.4426950408889634
GELU_C = 0.7978845608028654
GELU_A = 0.044715
MESH_ID = pl.DeviceIdType.MESH
LAG_MLP = 1
GROUP = 4
ROW_BLOCK = 32


def dot_nn(lhs, rhs):
    return lax.dot_general(lhs, rhs, (((1,), (0,)), ((), ())), preferred_element_type=jnp.float32)


def dot_nt(lhs, rhs):
    return lax.dot_general(lhs, rhs, (((1,), (1,)), ((), ())), preferred_element_type=jnp.float32)


def dot_tn(lhs, rhs):
    return lax.dot_general(lhs, rhs, (((0,), (0,)), ((), ())), preferred_element_type=jnp.float32)


def rms_scale(vals):
    return lax.rsqrt(jnp.mean(vals * vals, axis=-1, keepdims=True) + NORM_EPS)


def rms_vjp(vals, cotangent):
    scale = rms_scale(vals)
    inner = jnp.mean(vals * cotangent, axis=-1, keepdims=True)
    return scale * (cotangent - vals * (scale * scale * inner))


def row_blocks(count):
    return [pl.ds(start, ROW_BLOCK) for start in range(0, count, ROW_BLOCK)]


def causal_weights(scores_t, col_max, col_inv, scale):
    half = scores_t.shape[0] // 2
    diag = lax.broadcasted_iota(jnp.int32, (half, half), 0) <= lax.broadcasted_iota(jnp.int32, (half, half), 1)
    upper_l = jnp.where(diag, scores_t[:half, :half], -1e30)
    upper_r = scores_t[:half, half:]
    lower_r = jnp.where(diag, scores_t[half:, half:], -1e30)
    fresh = col_max is None
    if fresh:
        max_l = jnp.max(upper_l, axis=0, keepdims=True)
        max_r = jnp.maximum(jnp.max(upper_r, axis=0, keepdims=True), jnp.max(lower_r, axis=0, keepdims=True))
    else:
        max_l, max_r = col_max[:, :half], col_max[:, half:]
    factor = scale * LOG2E
    exp_ul = jnp.exp2((upper_l - max_l) * factor)
    exp_ur = jnp.exp2((upper_r - max_r) * factor)
    exp_lr = jnp.exp2((lower_r - max_r) * factor)
    if fresh:
        inv_l = 1.0 / jnp.sum(exp_ul, axis=0, keepdims=True)
        inv_r = 1.0 / (jnp.sum(exp_ur, axis=0, keepdims=True) + jnp.sum(exp_lr, axis=0, keepdims=True))
        stats = (jnp.concatenate([max_l, max_r], axis=1), jnp.concatenate([inv_l, inv_r], axis=1))
    else:
        inv_l, inv_r = col_inv[:, :half], col_inv[:, half:]
        stats = None
    return (exp_ul * inv_l, exp_ur * inv_r, exp_lr * inv_r), stats


def assemble(blocks, dtype):
    upper_l, upper_r, lower_r = (b.astype(dtype) for b in blocks)
    upper = jnp.concatenate([upper_l, upper_r], axis=1)
    lower = jnp.concatenate([jnp.zeros_like(upper_l), lower_r], axis=1)
    return jnp.concatenate([upper, lower], axis=0)


def forward_layer(dims, act_ref, wqkv, wout, wup, wdown, n1_ref, qkv_ref, stat_ref, ctx_ref, hid_ref, n2_ref, gp_ref, up_ref, out_ref, flush, n1t_s, score_s, prob_s, acc_s, ready):
    heads, hdim, ffn_tile = dims
    width = heads * hdim
    ffn = wdown.shape[0]
    scale = hdim ** -0.5
    for rows in row_blocks(act_ref.shape[0]):
        act32 = act_ref[rows, :].astype(jnp.float32)
        n1_ref[rows, :] = (act32 * rms_scale(act32)).astype(jnp.bfloat16)
    n1t_s[...] = n1_ref[...].T
    ready(0)

    def rows_of(h):
        return tuple(pl.ds(part * width + h * hdim, hdim) for part in range(3))

    def project(h):
        rows = rows_of(h)
        stacked = jnp.concatenate([wqkv[r, :] for r in rows], axis=0)
        proj = dot_nn(stacked, n1t_s[...]).astype(jnp.bfloat16)
        for part, r in enumerate(rows):
            qkv_ref[r, :] = proj[part * hdim:(part + 1) * hdim]

    def score(h):
        rows = rows_of(h)
        score_s[h % 3] = dot_tn(qkv_ref[rows[1], :], qkv_ref[rows[0], :])

    def soften(h):
        blocks, stats = causal_weights(score_s.at[h % 3], None, None, scale)
        stat_ref[h, 0:1, :] = stats[0]
        stat_ref[h, 1:2, :] = stats[1]
        prob_s[h % 2] = assemble(blocks, jnp.bfloat16)

    def mix(h):
        rows = rows_of(h)
        ctx_ref[rows[0], :] = dot_nn(qkv_ref[rows[2], :], prob_s[h % 2]).astype(jnp.bfloat16)

    for step in range(heads + 5):
        for lag, action in ((0, project), (2, score), (4, soften), (5, mix)):
            h = step - lag
            if 0 <= h < heads:
                action(h)
    flush(0)
    ready(1)
    acc_s[...] = dot_tn(ctx_ref[...], wout[...])
    for rows in row_blocks(act_ref.shape[0]):
        hid16 = (act_ref[rows, :].astype(jnp.float32) + acc_s[rows, :]).astype(jnp.bfloat16)
        hid_ref[rows, :] = hid16
        hid32 = hid16.astype(jnp.float32)
        n2_ref[rows, :] = (hid32 * rms_scale(hid32)).astype(jnp.bfloat16)
    normed2 = n2_ref[...]
    flush(1)
    ready(2)
    for tile in range(ffn // ffn_tile):
        cols = pl.ds(tile * ffn_tile, ffn_tile)
        pre = dot_nn(normed2, wup[:, cols])
        gp_ref[:, cols] = pre
        tanh = jnp.tanh(pre * (GELU_C + (GELU_C * GELU_A) * (pre * pre)))
        up_ref[:, cols] = (pre * (0.5 + 0.5 * tanh)).astype(jnp.bfloat16)
    flush(2)
    ready(3)
    acc_s[...] = dot_nn(up_ref[...], wdown[...])
    for rows in row_blocks(act_ref.shape[0]):
        out_ref[rows, :] = (hid_ref[rows, :].astype(jnp.float32) + acc_s[rows, :]).astype(jnp.bfloat16)


def backward_layer(dims, grad_ref, act_ref, wqkv, wout, wup, wdown, qkv_ref, stat_ref, hid_ref, gp_ref, dpre_ref, dhid_ref, dctx_ref, dqkv_ref, dact_ref, flush, acc_s, dhid_s32, dhidt_s, score_s, dprob_s, prob_s, dscore_s):
    heads, hdim, ffn_tile = dims
    width = heads * hdim
    ffn = wdown.shape[0]
    scale = hdim ** -0.5
    grad16 = grad_ref[...]

    def slope(tile):
        cols = pl.ds(tile * ffn_tile, ffn_tile)
        dup = dot_nt(grad16, wdown[cols, :])
        pre = gp_ref[:, cols]
        pre_sq = pre * pre
        tanh = jnp.tanh(pre * (GELU_C + (GELU_C * GELU_A) * pre_sq))
        half = 0.5 + 0.5 * tanh
        bend = (half * (1.0 - half)) * (pre * (2.0 * GELU_C + (6.0 * GELU_C * GELU_A) * pre_sq))
        dpre_ref[:, cols] = (dup * (half + bend)).astype(jnp.bfloat16)

    def gather(tile):
        cols = pl.ds(tile * ffn_tile, ffn_tile)
        part = dot_nt(dpre_ref[:, cols], wup[:, cols])
        if tile == 0:
            acc_s[...] = part
        else:
            acc_s[...] += part

    tiles = ffn // ffn_tile
    for step in range(tiles + LAG_MLP):
        if step < tiles:
            slope(step)
        if step >= LAG_MLP:
            gather(step - LAG_MLP)
    flush(0)
    for rows in row_blocks(act_ref.shape[0]):
        dhid32 = grad_ref[rows, :].astype(jnp.float32) + rms_vjp(hid_ref[rows, :].astype(jnp.float32), acc_s[rows, :])
        dhid_s32[rows, :] = dhid32
        dhid_ref[rows, :] = dhid32.astype(jnp.bfloat16)
    dhidt_s[...] = dhid_ref[...].T
    flush(1)

    def rows_of(h):
        return tuple(pl.ds(part * width + h * hdim, hdim) for part in range(3))

    def project(h):
        rows = rows_of(h)[0]
        dctx_ref[rows, :] = dot_nn(wout[rows, :], dhidt_s[...]).astype(jnp.bfloat16)

    def score(h):
        rows = rows_of(h)
        score_s[h % 3] = dot_tn(qkv_ref[rows[1], :], qkv_ref[rows[0], :])
        dprob_s[h % 3] = dot_tn(qkv_ref[rows[2], :], dctx_ref[rows[0], :])

    def soften(h):
        probs, _ = causal_weights(score_s.at[h % 3], stat_ref[h, 0:1, :], stat_ref[h, 1:2, :], scale)
        dprobs = dprob_s.at[h % 3]
        half = dprobs.shape[0] // 2
        d_ul, d_ur, d_lr = dprobs[:half, :half], dprobs[:half, half:], dprobs[half:, half:]
        p_ul, p_ur, p_lr = probs
        delta_l = jnp.sum(d_ul * p_ul, axis=0, keepdims=True)
        delta_r = jnp.sum(d_ur * p_ur, axis=0, keepdims=True) + jnp.sum(d_lr * p_lr, axis=0, keepdims=True)
        prob_s[h % 2] = assemble(probs, jnp.bfloat16)
        dscore_s[h % 2] = assemble((p_ul * (d_ul - delta_l) * scale, p_ur * (d_ur - delta_r) * scale, p_lr * (d_lr - delta_r) * scale), jnp.bfloat16)

    def mix(h):
        rows = rows_of(h)
        dqkv_ref[rows[2], :] = dot_nt(dctx_ref[rows[0], :], prob_s[h % 2]).astype(jnp.bfloat16)
        dqkv_ref[rows[0], :] = dot_nn(qkv_ref[rows[1], :], dscore_s[h % 2]).astype(jnp.bfloat16)
        dqkv_ref[rows[1], :] = dot_nt(qkv_ref[rows[0], :], dscore_s[h % 2]).astype(jnp.bfloat16)

    def collect(first, count):
        spans = [pl.ds(part * width + first * hdim, count * hdim) for part in range(3)]
        part = dot_tn(jnp.concatenate([dqkv_ref[r, :] for r in spans], axis=0), jnp.concatenate([wqkv[r, :] for r in spans], axis=0))
        if first == 0:
            acc_s[...] = part
        else:
            acc_s[...] += part

    group = min(GROUP, heads)
    for step in range(heads + 5):
        for lag, action in ((0, project), (2, score), (4, soften), (5, mix)):
            h = step - lag
            if 0 <= h < heads:
                action(h)
        done = step - 6
        if done >= 0 and done % group == group - 1 and done < heads - group:
            collect(done - group + 1, group)
    flush(2)
    collect(heads - group, group)
    for rows in row_blocks(act_ref.shape[0]):
        dact = dhid_s32[rows, :] + rms_vjp(act_ref[rows, :].astype(jnp.float32), acc_s[rows, :])
        dact_ref[rows, :] = dact.astype(jnp.bfloat16)


class placement:
    def __init__(self, n_stages):
        row = lax.axis_index('data')
        self.row = row
        self.index = lax.axis_index('stage')
        self.column = lax.div(self.index, 2)
        self.core = lax.rem(self.index, 2)
        self.upper = lax.div(row, 2)
        self.half = lax.rem(self.upper + self.column, 2)
        self.layer = 2 * self.column + self.half
        self.home = self.layer
        self.mate = 2 * self.column + 1 - self.core
        across = 3 - row
        along = lax.rem(self.index + jnp.where(self.half == 1, 2, n_stages - 2), n_stages)
        self.mate_id = {'data': row, 'stage': self.mate}
        self.across_id = {'data': across, 'stage': self.index}
        self.along_id = {'data': row, 'stage': along}
        self.next_id = {'data': jnp.where(self.half == 1, row, across), 'stage': jnp.where(self.half == 1, along, self.index)}
        self.prev_id = {'data': jnp.where(self.half == 1, across, row), 'stage': jnp.where(self.half == 1, self.index, along)}


def pipeline_kernel(
    cfg,
    emb_hbm, tgt_hbm, wqkv_hbm, wout_hbm, wup_hbm, wdown_hbm,
    loss_ref, n1_hbm, n2_hbm, up_hbm, ctx_hbm, dqkv_hbm, dpre_hbm, dhid_hbm, g_hbm, dx_hbm, qkv_hbm, gp_hbm, hid_hbm, stat_hbm,
    wqkv, wout, wup, wdown, act, grad, out_s, dact_s,
    n1_s, n2_s, up_s, ctx_s, qkv_s, gp_s, hid_s, stat_s,
    dpre_s, dhid_s, dctx_s, dqkv_s,
    w_sem, in_sem, act_sem, grad_sem, fout_sem, bin_sem, bout_sem, fsend_sem, bsend_sem, loss_acc, loss_sem, dx_sem, n1t_s, score_s, prob_s, dprob_s, dscore_s, acc_s, dhid_s32,
):
    n_stages, n_seq, tokens, grad_scale, dims = cfg
    here = placement(n_stages)
    stage, core, next_id, prev_id = here.layer, here.core, here.next_id, here.prev_id
    is_first = stage == 0
    is_last = stage == n_stages - 1
    own_weights = here.layer == here.index
    own_data = here.upper == core
    feeds_first = (here.column == 0) & (here.half == 1) & (core == 1)
    feeds_last = (here.column == n_stages // 2 - 1) & (here.half == 0) & (core == 1)

    weight_pairs = ((wqkv_hbm, wqkv), (wout_hbm, wout), (wup_hbm, wup), (wdown_hbm, wdown))

    def load_weight(idx):
        return pltpu.make_async_copy(weight_pairs[idx][0], weight_pairs[idx][1], w_sem.at[idx])

    def give_weight(idx):
        return pltpu.make_async_remote_copy(
            src_ref=weight_pairs[idx][0], dst_ref=weight_pairs[idx][1], send_sem=w_sem.at[4 + idx], recv_sem=w_sem.at[8 + idx],
            device_id=here.mate_id, device_id_type=MESH_ID)

    def load_embed(m):
        return pltpu.make_async_copy(emb_hbm.at[m], act.at[m], in_sem.at[m])

    def load_target(m):
        return pltpu.make_async_copy(tgt_hbm.at[m], grad.at[m], in_sem.at[m])

    def give_embed(m):
        return pltpu.make_async_remote_copy(
            src_ref=emb_hbm.at[m], dst_ref=act.at[m], send_sem=in_sem.at[m], recv_sem=act_sem.at[m],
            device_id=here.across_id, device_id_type=MESH_ID)

    def give_target(m):
        return pltpu.make_async_remote_copy(
            src_ref=tgt_hbm.at[m], dst_ref=grad.at[m], send_sem=in_sem.at[m], recv_sem=grad_sem.at[m],
            device_id=here.across_id, device_id_type=MESH_ID)

    def each_seq(when, action):
        @pl.when(when)
        def _():
            def go(m, carry):
                action(m)
                return carry
            lax.fori_loop(0, n_seq, go, 0)

    @pl.when(own_weights)
    def _():
        for idx in range(4):
            load_weight(idx).start()

    each_seq(is_first & own_data, lambda m: load_embed(m).start())
    each_seq(is_last & own_data, lambda m: load_target(m).start())

    barrier = pltpu.get_barrier_semaphore()
    for peer in (here.mate_id, here.across_id, here.along_id):
        pl.semaphore_signal(barrier, inc=1, device_id=peer, device_id_type=MESH_ID)
    pl.semaphore_wait(barrier, 3)

    @pl.when(own_weights)
    def _():
        for idx in range(4):
            give_weight(idx).start()

    each_seq(feeds_first, lambda m: give_embed(m).start())
    each_seq(feeds_last, lambda m: give_target(m).start())
    loss_acc[...] = jnp.zeros_like(loss_acc)

    def await_weight(idx):
        @pl.when(own_weights)
        def _():
            load_weight(idx).wait()

        @pl.when(jnp.logical_not(own_weights))
        def _():
            give_weight(idx).wait_recv()

    def send_act(m, slot):
        return pltpu.make_async_remote_copy(
            src_ref=out_s.at[slot], dst_ref=act.at[m], send_sem=fsend_sem.at[slot], recv_sem=act_sem.at[m],
            device_id=next_id, device_id_type=MESH_ID)

    def send_grad(m, slot):
        return pltpu.make_async_remote_copy(
            src_ref=dact_s.at[slot], dst_ref=grad.at[m], send_sem=bsend_sem.at[slot], recv_sem=grad_sem.at[m],
            device_id=prev_id, device_id_type=MESH_ID)

    def store_dx(m, slot):
        return pltpu.make_async_copy(dact_s.at[slot], dx_hbm.at[m], bsend_sem.at[slot])

    def give_dx(m, slot):
        return pltpu.make_async_remote_copy(
            src_ref=dact_s.at[slot], dst_ref=dx_hbm.at[m], send_sem=bsend_sem.at[slot], recv_sem=dx_sem.at[m],
            device_id=here.across_id, device_id_type=MESH_ID)

    def token_range(m):
        return pl.ds(pl.multiple_of(m * tokens, tokens), tokens)

    def fout_copies(m, slot):
        rows = token_range(m)
        return (
            (0, pltpu.make_async_copy(n1_s.at[slot], n1_hbm.at[rows, :], fout_sem.at[slot, 0])),
            (0, pltpu.make_async_copy(qkv_s.at[slot], qkv_hbm.at[m], fout_sem.at[slot, 1])),
            (1, pltpu.make_async_copy(ctx_s.at[slot], ctx_hbm.at[:, rows], fout_sem.at[slot, 2])),
            (1, pltpu.make_async_copy(stat_s.at[slot], stat_hbm.at[m], fout_sem.at[slot, 3])),
            (1, pltpu.make_async_copy(hid_s.at[slot], hid_hbm.at[m], fout_sem.at[slot, 4])),
            (1, pltpu.make_async_copy(n2_s.at[slot], n2_hbm.at[rows, :], fout_sem.at[slot, 5])),
            (2, pltpu.make_async_copy(gp_s.at[slot], gp_hbm.at[m], fout_sem.at[slot, 6])),
            (2, pltpu.make_async_copy(up_s.at[slot], up_hbm.at[rows, :], fout_sem.at[slot, 7])),
        )

    def bin_copies(m):
        return (
            pltpu.make_async_copy(qkv_hbm.at[m], qkv_s.at[2], bin_sem.at[0]),
            pltpu.make_async_copy(stat_hbm.at[m], stat_s.at[2], bin_sem.at[1]),
            pltpu.make_async_copy(hid_hbm.at[m], hid_s.at[2], bin_sem.at[2]),
            pltpu.make_async_copy(gp_hbm.at[m], gp_s.at[2], bin_sem.at[3]),
        )

    def bout_copies(m, slot):
        rows = token_range(m)
        return (
            (0, pltpu.make_async_copy(grad.at[m], g_hbm.at[rows, :], bout_sem.at[slot, 0])),
            (0, pltpu.make_async_copy(dpre_s.at[slot], dpre_hbm.at[rows, :], bout_sem.at[slot, 1])),
            (1, pltpu.make_async_copy(dhid_s.at[slot], dhid_hbm.at[rows, :], bout_sem.at[slot, 2])),
            (2, pltpu.make_async_copy(dqkv_s.at[slot], dqkv_hbm.at[:, rows], bout_sem.at[slot, 3])),
        )

    def flusher(copies):
        def flush(group):
            for when, copy in copies:
                if when == group:
                    copy.start()
        return flush

    def in_range(m):
        return (m >= 0) & (m < n_seq)

    def tick(t, carry):
        fwd_m = t - stage
        bwd_m = t + 2 * stage - 3 * (n_stages - 1)

        @pl.when(in_range(fwd_m))
        def _():
            m = fwd_m
            slot = lax.rem(m, 2)

            @pl.when(is_first & own_data)
            def _():
                load_embed(m).wait()

            @pl.when(jnp.logical_not(is_first & own_data))
            def _():
                send_act(m, slot).wait_recv()

            def run_forward(ready):
                forward_layer(
                    dims, act.at[m], wqkv, wout, wup, wdown, n1_s.at[slot], qkv_s.at[slot], stat_s.at[slot],
                    ctx_s.at[slot], hid_s.at[slot], n2_s.at[slot], gp_s.at[slot], up_s.at[slot], out_s.at[slot],
                    flusher(fout_copies(m, slot)), n1t_s, score_s, prob_s, acc_s, ready)

            @pl.when(m == 0)
            def _():
                run_forward(await_weight)

            @pl.when(m > 0)
            def _():
                run_forward(lambda idx: None)

            @pl.when(jnp.logical_not(is_last))
            def _():
                send_act(m, slot).start()

            @pl.when(is_last & own_data)
            def _():
                load_target(m).wait()

            @pl.when(is_last & jnp.logical_not(own_data))
            def _():
                send_grad(m, slot).wait_recv()

            @pl.when(is_last)
            def _():
                for start in range(0, tokens, 32):
                    rows = pl.ds(start, 32)
                    error = out_s[slot, rows, :].astype(jnp.float32) - grad[m, rows, :].astype(jnp.float32)
                    square = error * error
                    loss_acc[...] += (square[0:8] + square[8:16]) + (square[16:24] + square[24:32])
                    grad[m, rows, :] = (error * grad_scale).astype(jnp.bfloat16)

        @pl.when(in_range(bwd_m))
        def _():
            m = bwd_m
            slot = lax.rem(m, 2)

            @pl.when(jnp.logical_not(is_last))
            def _():
                for copy in bin_copies(m):
                    copy.wait()
                send_grad(m, slot).wait_recv()

            saved = jnp.where(is_last, slot, 2)
            backward_layer(
                dims, grad.at[m], act.at[m], wqkv, wout, wup, wdown, qkv_s.at[saved], stat_s.at[saved], hid_s.at[saved],
                gp_s.at[saved], dpre_s.at[slot], dhid_s.at[slot], dctx_s, dqkv_s.at[slot], dact_s.at[slot],
                flusher(bout_copies(m, slot)), acc_s, dhid_s32, n1t_s, score_s, dprob_s, prob_s, dscore_s)

            @pl.when(jnp.logical_not(is_first))
            def _():
                send_grad(m, slot).start()

            @pl.when(is_first & own_data)
            def _():
                store_dx(m, slot).start()

            @pl.when(is_first & jnp.logical_not(own_data))
            def _():
                give_dx(m, slot).start()

        fwd_old = fwd_m - 1
        bwd_old = bwd_m - 1

        @pl.when(in_range(fwd_old))
        def _():
            slot = lax.rem(fwd_old, 2)
            for _, copy in fout_copies(fwd_old, slot):
                copy.wait()

            @pl.when(jnp.logical_not(is_last))
            def _():
                send_act(fwd_old, slot).wait_send()

        @pl.when(in_range(bwd_old))
        def _():
            slot = lax.rem(bwd_old, 2)
            for _, copy in bout_copies(bwd_old, slot):
                copy.wait()

            @pl.when(jnp.logical_not(is_first))
            def _():
                send_grad(bwd_old, slot).wait_send()

            @pl.when(is_first & own_data)
            def _():
                store_dx(bwd_old, slot).wait()

            @pl.when(is_first & jnp.logical_not(own_data))
            def _():
                give_dx(bwd_old, slot).wait_send()

        @pl.when(in_range(bwd_m + 1) & jnp.logical_not(is_last))
        def _():
            for copy in bin_copies(bwd_m + 1):
                copy.start()

        return carry

    lax.fori_loop(0, n_seq + 3 * (n_stages - 1) + 1, tick, 0)

    def send_loss():
        return pltpu.make_async_remote_copy(
            src_ref=loss_ref, dst_ref=loss_ref, send_sem=loss_sem.at[0], recv_sem=loss_sem.at[1],
            device_id=prev_id, device_id_type=MESH_ID)

    @pl.when(is_last)
    def _():
        lanes = loss_ref.shape[1]
        total = loss_acc[:, 0:lanes]
        for col in range(lanes, loss_acc.shape[1], lanes):
            total = total + loss_acc[:, col:col + lanes]
        loss_ref[...] = total

    @pl.when(jnp.logical_not(is_last))
    def _():
        send_loss().wait_recv()

    @pl.when(jnp.logical_not(is_first))
    def _():
        send_loss().start()
        send_loss().wait_send()

    @pl.when(own_weights)
    def _():
        for idx in range(4):
            give_weight(idx).wait_send()

    each_seq(feeds_first, lambda m: give_embed(m).wait_send())
    each_seq(feeds_last, lambda m: give_target(m).wait_send())
    each_seq(feeds_first, lambda m: give_dx(m, 0).wait_recv())


def run_pipeline(n_stages, grad_scale, embeds, targets, wqkv, wout, wup, wdown, heads, hdim):
    n_seq, tokens, width = embeds.shape
    ffn = wdown.shape[0]
    dims = (heads, hdim, 512 if ffn % 512 == 0 else ffn)
    bf16, f32 = jnp.bfloat16, jnp.float32
    total = n_seq * tokens
    out_shapes = [
        ((8, 128), f32),
        ((total, width), bf16),
        ((total, width), bf16),
        ((total, ffn), bf16),
        ((width, total), bf16),
        ((3 * width, total), bf16),
        ((total, ffn), bf16),
        ((total, width), bf16),
        ((total, width), bf16),
        ((n_seq, tokens, width), bf16),
        ((n_seq, 3 * width, tokens), bf16),
        ((n_seq, tokens, ffn), f32),
        ((n_seq, tokens, width), bf16),
        ((n_seq, heads, 8, tokens), f32),
    ]
    any_spec = pl.BlockSpec(memory_space=pl.ANY)
    scratch = [
        pltpu.VMEM(wqkv.shape, bf16), pltpu.VMEM(wout.shape, bf16), pltpu.VMEM(wup.shape, bf16), pltpu.VMEM(wdown.shape, bf16),
        pltpu.VMEM((n_seq, tokens, width), bf16), pltpu.VMEM((n_seq, tokens, width), bf16),
        pltpu.VMEM((2, tokens, width), bf16), pltpu.VMEM((2, tokens, width), bf16),
        pltpu.VMEM((2, tokens, width), bf16), pltpu.VMEM((2, tokens, width), bf16),
        pltpu.VMEM((2, tokens, ffn), bf16), pltpu.VMEM((2, width, tokens), bf16),
        pltpu.VMEM((3, 3 * width, tokens), bf16), pltpu.VMEM((3, tokens, ffn), f32),
        pltpu.VMEM((3, tokens, width), bf16), pltpu.VMEM((3, heads, 8, tokens), f32),
        pltpu.VMEM((2, tokens, ffn), bf16), pltpu.VMEM((2, tokens, width), bf16),
        pltpu.VMEM((width, tokens), bf16), pltpu.VMEM((2, 3 * width, tokens), bf16),
        pltpu.SemaphoreType.DMA((12,)), pltpu.SemaphoreType.DMA((n_seq,)),
        pltpu.SemaphoreType.DMA((n_seq,)), pltpu.SemaphoreType.DMA((n_seq,)),
        pltpu.SemaphoreType.DMA((2, 8)), pltpu.SemaphoreType.DMA((4,)), pltpu.SemaphoreType.DMA((2, 4)),
        pltpu.SemaphoreType.DMA((2,)), pltpu.SemaphoreType.DMA((2,)),
        pltpu.VMEM((8, width), f32), pltpu.SemaphoreType.DMA((2,)), pltpu.SemaphoreType.DMA((n_seq,)),
        pltpu.VMEM((width, tokens), bf16), pltpu.VMEM((3, tokens, tokens), f32), pltpu.VMEM((2, tokens, tokens), bf16),
        pltpu.VMEM((3, tokens, tokens), f32), pltpu.VMEM((2, tokens, tokens), bf16), pltpu.VMEM((tokens, width), f32), pltpu.VMEM((tokens, width), f32),
    ]
    linear = 2 * total * (wqkv.size + wout.size + wup.size + wdown.size)
    return pl.pallas_call(
        functools.partial(pipeline_kernel, (n_stages, n_seq, tokens, grad_scale, dims)),
        out_shape=[jax.ShapeDtypeStruct(s, d) for s, d in out_shapes],
        in_specs=[any_spec] * 6,
        out_specs=[pl.BlockSpec(memory_space=pltpu.VMEM)] + [any_spec] * (len(out_shapes) - 1),
        scratch_shapes=scratch,
        compiler_params=pltpu.CompilerParams(collective_id=0, has_side_effects=True, vmem_limit_bytes=67043328),
        cost_estimate=pl.CostEstimate(flops=3 * linear, bytes_accessed=200 * 2 ** 20, transcendentals=0),
        name='stage_pipeline',
    )(embeds, targets, wqkv, wout, wup, wdown)


def reduce_kernel(
    cfg,
    loss_hbm, ctx_hbm, dhid_hbm, dqkv_hbm, n1_hbm, up_hbm, g_hbm, n2_hbm, dpre_hbm, dx_hbm,
    loss_ref, dout_hbm, dqkvw_hbm, ddown_hbm, dup_hbm, demb_hbm,
    out_res, qkv_res, down_res, up_res, out_in, qkv_in, down_in, up_in,
    out_give, qkv_give, down_give, up_give, out_core, qkv_core, down_core, up_core, out_row, qkv_row, down_row, up_row, loss_sl,
    res_sem, in_sem, give_sem, core_sem, row_send, row_recv, put_send, put_recv, pass_send, store_sem, dx_sem,
    loss_send, loss_recv, loss_in,
):
    (n_stages,) = cfg
    here = placement(n_stages)
    row, core, stage = here.row, here.core, here.index
    pair = lax.rem(row, 2)
    pair_row = row + 1 - 2 * pair
    across = 3 - row
    is_home = here.home == stage
    home_id = {'data': row, 'stage': here.home}
    pair_id = {'data': pair_row, 'stage': stage}
    pair_home_id = {'data': pair_row, 'stage': here.home}
    across_home_id = {'data': across, 'stage': here.home}

    kinds = (
        ('rows', dhid_hbm, out_res, ctx_hbm, out_in, out_give, out_core, out_row, dout_hbm),
        ('rows', n1_hbm, qkv_res, dqkv_hbm, qkv_in, qkv_give, qkv_core, qkv_row, dqkvw_hbm),
        ('tall', g_hbm, down_res, up_hbm, down_in, down_give, down_core, down_row, ddown_hbm),
        ('wide', n2_hbm, up_res, dpre_hbm, up_in, up_give, up_core, up_row, dup_hbm),
    )
    n_kinds = len(kinds)
    turns = ((1, 1), (0, 1), (1, 0), (0, 0))

    def piece(kind, member, unit, num):
        size = kinds[kind][4].shape[1 if kinds[kind][0] == 'rows' else 2]
        return pl.ds(pl.multiple_of(((member * 2 + unit) * 2 + num) * size, size), size)

    def flip(val, by):
        return 1 - val if by else val

    def read_piece(kind, turn, num):
        form, _, _, src, buf = kinds[kind][:5]
        part = piece(kind, flip(pair, turns[turn][0]), flip(core, turns[turn][1]), num)
        view = src.at[part, :] if form == 'rows' else src.at[:, part]
        return pltpu.make_async_copy(view, buf.at[turn % 2], in_sem.at[kind, turn % 2])

    def out_view(kind, member, unit, num):
        part = piece(kind, member, unit, num)
        dst = kinds[kind][8]
        return dst.at[:, part] if kinds[kind][0] == 'wide' else dst.at[part, :]

    tile = min(256, out_res.shape[1])
    n_tiles = out_res.shape[1] // tile

    def tile_at(kind, n):
        span = pl.ds(pl.multiple_of(n * tile, tile), tile)
        return (span, slice(None)) if kinds[kind][0] == 'wide' else (slice(None), span)

    def each_tile(action):
        def body(n, carry):
            action(n)
            return carry
        lax.fori_loop(0, n_tiles, body, 0)

    def give(kind, other, num):
        return pltpu.make_async_remote_copy(
            src_ref=kinds[kind][5].at[other], dst_ref=kinds[kind][6].at[num, other], send_sem=give_sem.at[kind, other],
            recv_sem=core_sem.at[kind, num, other], device_id=here.mate_id, device_id_type=MESH_ID)

    def send_row(kind, num, n):
        at = tile_at(kind, n)
        return pltpu.make_async_remote_copy(
            src_ref=kinds[kind][6].at[(num, 1) + at], dst_ref=kinds[kind][7].at[(num,) + at], send_sem=row_send.at[kind, num, n],
            recv_sem=row_recv.at[kind, num, n], device_id=pair_id, device_id_type=MESH_ID)

    def put_view(kind, member, unit, num, n):
        part = piece(kind, member, unit, num)
        span = pl.ds(pl.multiple_of(n * tile, tile), tile)
        dst = kinds[kind][8]
        return dst.at[span, part] if kinds[kind][0] == 'wide' else dst.at[part, span]

    def put(kind, num, n, target, device_id):
        return pltpu.make_async_remote_copy(
            src_ref=kinds[kind][7].at[(num,) + tile_at(kind, n)], dst_ref=put_view(kind, pair, core, num, n),
            send_sem=put_send.at[target, kind, num, n], recv_sem=put_recv.at[pair, core, kind, num, n],
            device_id=device_id, device_id_type=MESH_ID)

    def keep(kind, num):
        return pltpu.make_async_copy(kinds[kind][7].at[num], out_view(kind, pair, core, num), store_sem.at[kind, num])

    def arrival(kind, num, n, member, unit):
        view = put_view(kind, member, unit, num, n)
        return pltpu.make_async_remote_copy(
            src_ref=view, dst_ref=view, send_sem=pass_send.at[unit, kind, num, n], recv_sem=put_recv.at[member, unit, kind, num, n],
            device_id=across_home_id, device_id_type=MESH_ID)

    def load_resident(kind):
        return pltpu.make_async_copy(kinds[kind][1], kinds[kind][2], res_sem.at[kind])

    def pipeline_id(row_idx, unit):
        return 2 * jnp.minimum(row_idx, 3 - row_idx) + unit

    my_loss = pltpu.make_async_copy(loss_hbm, loss_sl.at[pipeline_id(row, core)], loss_in)
    my_loss.start()
    load_resident(0).start()
    read_piece(0, 0, 0).start()

    source = here.upper
    rank = stage + source - 2 * source * core
    spans = []
    span = n_stages // 2
    while span >= 1:
        spans.append(span)
        span //= 2

    def swapped(span):
        return stage + span - 2 * span * lax.rem(lax.div(stage, span), 2)

    loss_ids = (
        ({'data': row, 'stage': here.mate}, row, 1 - core),
        ({'data': pair_row, 'stage': stage}, pair_row, core),
        ({'data': pair_row, 'stage': here.mate}, pair_row, 1 - core),
    )
    peers = [ident for ident, _, _ in loss_ids]
    peers += [{'data': across, 'stage': stage}, {'data': across, 'stage': here.mate}]
    peers += [{'data': row, 'stage': swapped(span)} for span in spans if span > 1]
    barrier = pltpu.get_barrier_semaphore()
    for ident in peers:
        pl.semaphore_signal(barrier, inc=1, device_id=ident, device_id_type=MESH_ID)
    pl.semaphore_wait(barrier, len(peers))

    def send_loss(idx):
        slot = loss_sl.at[pipeline_id(row, core)]
        return pltpu.make_async_remote_copy(
            src_ref=slot, dst_ref=slot, send_sem=loss_send.at[idx], recv_sem=loss_recv.at[idx],
            device_id=loss_ids[idx][0], device_id_type=MESH_ID)

    def loss_arrival(idx):
        slot = loss_sl.at[pipeline_id(loss_ids[idx][1], loss_ids[idx][2])]
        return pltpu.make_async_remote_copy(
            src_ref=slot, dst_ref=slot, send_sem=loss_send.at[idx], recv_sem=loss_recv.at[idx],
            device_id=loss_ids[idx][0], device_id_type=MESH_ID)

    for kind in range(1, n_kinds):
        load_resident(kind).start()
        read_piece(kind, 0, 0).start()
    my_loss.wait()
    for idx in range(3):
        send_loss(idx).start()

    def spread(idx):
        return pltpu.make_async_remote_copy(
            src_ref=demb_hbm, dst_ref=demb_hbm, send_sem=dx_sem.at[0, idx], recv_sem=dx_sem.at[1, idx],
            device_id={'data': row, 'stage': swapped(spans[idx])}, device_id_type=MESH_ID)

    def sends_at(idx):
        return lax.rem(rank, 2 * spans[idx]) == 0

    def receives_at(idx):
        return lax.rem(rank, 2 * spans[idx]) == spans[idx]

    def spread_round(idx):
        if idx > 0:
            @pl.when(receives_at(idx - 1))
            def _():
                spread(idx - 1).wait_recv()
        if idx < len(spans):
            @pl.when(sends_at(idx))
            def _():
                spread(idx).start()

    def product(kind, turn, num, sink, base, before=None, after=None):
        form, _, res, _, buf = kinds[kind][:5]
        read_piece(kind, turn, num).wait()
        if turn < 3:
            read_piece(kind, turn + 1, num).start()
        else:
            @pl.when(num == 0)
            def _():
                read_piece(kind, 0, 1).start()
        fed = buf.at[turn % 2]

        def body(n):
            at = tile_at(kind, n)
            span = pl.ds(pl.multiple_of(n * tile, tile), tile)
            if before is not None:
                before(n)
            if form == 'rows':
                part = dot_nn(fed[...], res[:, span])
            elif form == 'tall':
                part = dot_tn(fed[...], res[:, span])
            else:
                part = dot_tn(res[:, span], fed[...])
            for ref in base:
                part = part + ref[at]
            sink[at] = part
            if after is not None:
                after(n)

        each_tile(body)

    def first_half(kind, num):
        give_buf, core_buf = kinds[kind][5:7]

        @pl.when(num == 0)
        def _():
            load_resident(kind).wait()

        for turn, other in ((0, 1), (1, 0)):
            @pl.when(num > 0)
            def _():
                give(kind, other, num - 1).wait_send()

            product(kind, turn, num, give_buf.at[other], ())
            give(kind, other, num).start()
        give(kind, 1, num).wait_recv()
        product(kind, 2, num, core_buf.at[num, 1], (core_buf.at[num, 1],), after=lambda n: send_row(kind, num, n).start())

    def second_half(kind, num):
        core_buf, row_buf = kinds[kind][6:8]
        give(kind, 0, num).wait_recv()

        def after(n):
            put(kind, num, n, 1, pair_home_id).start()
            put(kind, num, n, 2, across_home_id).start()

            @pl.when(jnp.logical_not(is_home))
            def _():
                put(kind, num, n, 0, home_id).start()

        product(kind, 3, num, row_buf.at[num], (core_buf.at[num, 0], row_buf.at[num]),
                before=lambda n: send_row(kind, num, n).wait_recv(), after=after)

        @pl.when(is_home)
        def _():
            keep(kind, num).start()

    def pass_on(kind, num):
        @pl.when(is_home)
        def _():
            def go(n):
                for unit in range(2):
                    arrival(kind, num, n, 1 - pair, unit).wait_recv()
                    arrival(kind, num, n, 1 - pair, unit).start()
            each_tile(go)

    def kind_at(pos):
        late = jnp.where(pos == 4, 2, jnp.where(pos == 5, 3, jnp.where(pos == 6, 1, 0)))
        return jnp.where(pos < 4, pos, late)

    def num_at(pos):
        return jnp.where(pos < 4, 0, 1)

    n_steps = 2 * n_kinds

    def step_body(pos, carry):
        for kind in range(n_kinds):
            @pl.when((pos < n_steps) & (kind_at(pos) == kind))
            def _():
                first_half(kind, num_at(pos))

        for kind in range(n_kinds):
            @pl.when((pos >= 1) & (pos < n_steps + 1) & (kind_at(pos - 1) == kind))
            def _():
                second_half(kind, num_at(pos - 1))

        for kind in range(n_kinds):
            @pl.when((pos >= 2) & (kind_at(pos - 2) == kind))
            def _():
                pass_on(kind, num_at(pos - 2))

        for idx in range(len(spans) + 1):
            @pl.when(pos == 3 * idx)
            def _():
                spread_round(idx)
        return carry

    lax.fori_loop(0, n_steps + 2, step_body, 0)

    for idx in range(3):
        loss_arrival(idx).wait_recv()
    total = loss_sl[0]
    for idx in range(1, 4):
        total = total + loss_sl[idx]
    loss_ref[...] = total

    for kind in range(n_kinds):
        for num in range(2):
            def settle(n):
                @pl.when(is_home)
                def _():
                    arrival(kind, num, n, pair, 1 - core).wait_recv()
                    for unit in range(2):
                        arrival(kind, num, n, 1 - pair, unit).wait_send()

                @pl.when(jnp.logical_not(is_home))
                def _():
                    for member in range(2):
                        for unit in range(2):
                            arrival(kind, num, n, member, unit).wait_recv()
                    put(kind, num, n, 0, home_id).wait_send()

                send_row(kind, num, n).wait_send()
                put(kind, num, n, 1, pair_home_id).wait_send()
                put(kind, num, n, 2, across_home_id).wait_send()

            each_tile(settle)

            @pl.when(is_home)
            def _():
                keep(kind, num).wait()
        for other in range(2):
            give(kind, other, 1).wait_send()
    for idx in range(3):
        send_loss(idx).wait_send()
    for idx in range(len(spans)):
        @pl.when(sends_at(idx))
        def _():
            spread(idx).wait_send()


def sum_gradients(n_stages, loss_part, ctx_t, dhid, dqkv_t, n1, upper, grads, n2, dpre, dx):
    bf16, f32 = jnp.bfloat16, jnp.float32
    total, width = n1.shape
    ffn = upper.shape[1]
    small, mid, big = width // 8, 3 * width // 8, ffn // 8
    any_spec = pl.BlockSpec(memory_space=pl.ANY)
    vmem_spec = pl.BlockSpec(memory_space=pltpu.VMEM)
    out_shapes = [(loss_part.shape, f32), ((width, width), f32), ((3 * width, width), f32), ((ffn, width), f32), ((width, ffn), f32), (dx.shape, bf16)]
    n_spans = n_stages.bit_length() - 1
    n_tiles = max(1, width // 256)
    pieces = ((small, width), (mid, width), (big, width), (width, big))
    dma = pltpu.SemaphoreType.DMA
    scratch = [pltpu.VMEM((total, width), bf16)] * 4 + [
        pltpu.VMEM((2, small, total), bf16), pltpu.VMEM((2, mid, total), bf16),
        pltpu.VMEM((2, total, big), bf16), pltpu.VMEM((2, total, big), bf16),
    ]
    scratch += [pltpu.VMEM((2,) + p, f32) for p in pieces]
    scratch += [pltpu.VMEM((2, 2) + p, f32) for p in pieces]
    scratch += [pltpu.VMEM((2,) + p, f32) for p in pieces]
    scratch += [
        pltpu.VMEM((4,) + loss_part.shape, f32),
        dma((4,)), dma((4, 2)), dma((4, 2)), dma((4, 2, 2)), dma((4, 2, n_tiles)), dma((4, 2, n_tiles)),
        dma((3, 4, 2, n_tiles)), dma((2, 2, 4, 2, n_tiles)), dma((2, 4, 2, n_tiles)), dma((4, 2)), dma((2, n_spans)), dma((3,)), dma((3,)), dma(()),
    ]
    flops = 2 * total * width * (4 * width + 2 * ffn)
    return pl.pallas_call(
        functools.partial(reduce_kernel, (n_stages,)),
        out_shape=[jax.ShapeDtypeStruct(s, d) for s, d in out_shapes],
        in_specs=[any_spec] * 10,
        out_specs=[vmem_spec] + [any_spec] * 5,
        scratch_shapes=scratch,
        input_output_aliases={9: 5},
        compiler_params=pltpu.CompilerParams(collective_id=1, has_side_effects=True, vmem_limit_bytes=67043328),
        cost_estimate=pl.CostEstimate(flops=flops, bytes_accessed=150 * 2 ** 20, transcendentals=0),
        name='gradient_sums',
    )(loss_part, ctx_t, dhid, dqkv_t, n1, upper, grads, n2, dpre, dx)


def settle_kernel(plan, loss_factor, loss_in, *refs):
    count = len(plan)
    sources, loss_ref, results = refs[:count], refs[count], refs[count + 1:2 * count + 1]
    holds, sem = refs[2 * count + 1:-1], refs[-1]
    copies = []
    for src, hold, dst, parts in zip(sources, holds, results, plan):
        lead = src.shape[0] // parts
        for idx in range(parts):
            part = pl.ds(idx * lead, lead)
            num = len(copies)
            copies.append((
                pltpu.make_async_copy(src.at[part], hold.at[part], sem.at[0, num]),
                pltpu.make_async_copy(hold.at[part], dst.at[part], sem.at[1, num])))
    for read, _ in copies:
        read.start()
    loss_ref[0] = loss_factor * jnp.sum(loss_in[...])
    for read, write in copies:
        read.wait()
        write.start()
    for _, write in copies:
        write.wait()


def settle(loss_factor, loss_sum, arrays):
    plan = tuple(next(p for p in (4, 3, 2, 1) if arr.shape[0] % (16 * p) == 0 or p == 1 or (arr.ndim == 3 and arr.shape[0] % p == 0)) for arr in arrays)
    any_spec = pl.BlockSpec(memory_space=pl.ANY)
    outs = pl.pallas_call(
        functools.partial(settle_kernel, plan, loss_factor),
        out_shape=[jax.ShapeDtypeStruct((1,), jnp.float32)] + [jax.ShapeDtypeStruct(arr.shape, arr.dtype) for arr in arrays],
        in_specs=[pl.BlockSpec(memory_space=pltpu.VMEM)] + [any_spec] * len(arrays),
        out_specs=[pl.BlockSpec(memory_space=pltpu.SMEM)] + [any_spec] * len(arrays),
        scratch_shapes=[pltpu.VMEM(arr.shape, arr.dtype) for arr in arrays] + [pltpu.SemaphoreType.DMA((2, sum(plan)))],
        compiler_params=pltpu.CompilerParams(vmem_limit_bytes=60 * 2 ** 20),
        name='settle_results',
    )(loss_sum, *arrays)
    return outs[0], outs[1:]


def solution(mesh):
    n_stages = mesh.shape['stage']
    n_data = mesh.shape['data']
    act_spec = P(('rep', 'data'))
    weight_spec = P(('rep', 'stage'))

    def per_device(embeds, targets, w_qkv, w_out, w_up, w_down):
        n_micro, micro_b, seq_len, width = embeds.shape
        heads, hdim = w_qkv.shape[2], w_qkv.shape[3]
        grad_scale = 1.0 / (n_data * n_micro)
        loss_norm = 1.0 / (n_data * n_micro * micro_b * seq_len * width)
        flat = (n_micro * micro_b, seq_len, width)
        outs = run_pipeline(
            n_stages, grad_scale, embeds.reshape(flat), targets.reshape(flat), w_qkv.reshape(3 * width, width),
            w_out.reshape(width, width), w_up[0], w_down[0], heads, hdim)
        loss_part, n1, n2, upper, ctx_t, dqkv_t, dpre, dhid, grads, dx = outs[:10]
        loss_sum, *sums = sum_gradients(
            n_stages, loss_part, ctx_t, dhid, dqkv_t, n1, upper, grads, n2, dpre, dx)
        loss, (d_out, d_qkv, d_down, d_up, d_embeds) = settle(0.5 * loss_norm, loss_sum, sums)
        return (loss, d_qkv.reshape(w_qkv.shape), d_out.reshape(w_out.shape), d_up[None], d_down[None], d_embeds.reshape(embeds.shape))

    return jax.shard_map(per_device, mesh=mesh, in_specs=(act_spec, act_spec, weight_spec, weight_spec, weight_spec, weight_spec), out_specs=(P('rep'), weight_spec, weight_spec, weight_spec, weight_spec, act_spec), check_vma=False)
```

```python
import functools

import jax
import jax.numpy as jnp
from jax import lax
from jax.experimental import pallas as pl
from jax.experimental.pallas import tpu as pltpu
from jax.sharding import PartitionSpec as P

NORM_EPS = 1e-6
LOG2E = 1.4426950408889634
GELU_C = 0.7978845608028654
GELU_A = 0.044715
MESH_ID = pl.DeviceIdType.MESH
LAG_MLP = 1
GROUP = 4
ROW_BLOCK = 32


def dot_nn(lhs, rhs):
    return lax.dot_general(lhs, rhs, (((1,), (0,)), ((), ())), preferred_element_type=jnp.float32)


def dot_nt(lhs, rhs):
    return lax.dot_general(lhs, rhs, (((1,), (1,)), ((), ())), preferred_element_type=jnp.float32)


def dot_tn(lhs, rhs):
    return lax.dot_general(lhs, rhs, (((0,), (0,)), ((), ())), preferred_element_type=jnp.float32)


def rms_scale(vals):
    return lax.rsqrt(jnp.mean(vals * vals, axis=-1, keepdims=True) + NORM_EPS)


def rms_vjp(vals, cotangent):
    scale = rms_scale(vals)
    inner = jnp.mean(vals * cotangent, axis=-1, keepdims=True)
    return scale * (cotangent - vals * (scale * scale * inner))


def row_blocks(count):
    return [pl.ds(start, ROW_BLOCK) for start in range(0, count, ROW_BLOCK)]


def causal_weights(scores_t, col_max, col_inv, scale):
    half = scores_t.shape[0] // 2
    diag = lax.broadcasted_iota(jnp.int32, (half, half), 0) <= lax.broadcasted_iota(jnp.int32, (half, half), 1)
    upper_l = jnp.where(diag, scores_t[:half, :half], -1e30)
    upper_r = scores_t[:half, half:]
    lower_r = jnp.where(diag, scores_t[half:, half:], -1e30)
    fresh = col_max is None
    if fresh:
        max_l = jnp.max(upper_l, axis=0, keepdims=True)
        max_r = jnp.maximum(jnp.max(upper_r, axis=0, keepdims=True), jnp.max(lower_r, axis=0, keepdims=True))
    else:
        max_l, max_r = col_max[:, :half], col_max[:, half:]
    factor = scale * LOG2E
    exp_ul = jnp.exp2((upper_l - max_l) * factor)
    exp_ur = jnp.exp2((upper_r - max_r) * factor)
    exp_lr = jnp.exp2((lower_r - max_r) * factor)
    if fresh:
        inv_l = 1.0 / jnp.sum(exp_ul, axis=0, keepdims=True)
        inv_r = 1.0 / (jnp.sum(exp_ur, axis=0, keepdims=True) + jnp.sum(exp_lr, axis=0, keepdims=True))
        stats = (jnp.concatenate([max_l, max_r], axis=1), jnp.concatenate([inv_l, inv_r], axis=1))
    else:
        inv_l, inv_r = col_inv[:, :half], col_inv[:, half:]
        stats = None
    return (exp_ul * inv_l, exp_ur * inv_r, exp_lr * inv_r), stats


def assemble(blocks, dtype):
    upper_l, upper_r, lower_r = (b.astype(dtype) for b in blocks)
    upper = jnp.concatenate([upper_l, upper_r], axis=1)
    lower = jnp.concatenate([jnp.zeros_like(upper_l), lower_r], axis=1)
    return jnp.concatenate([upper, lower], axis=0)


def forward_layer(dims, act_ref, wqkv, wout, wup, wdown, n1_ref, qkv_ref, stat_ref, ctx_ref, hid_ref, n2_ref, gp_ref, up_ref, out_ref, flush, n1t_s, score_s, prob_s, acc_s, ready):
    heads, hdim, ffn_tile = dims
    width = heads * hdim
    ffn = wdown.shape[0]
    scale = hdim ** -0.5
    for rows in row_blocks(act_ref.shape[0]):
        act32 = act_ref[rows, :].astype(jnp.float32)
        n1_ref[rows, :] = (act32 * rms_scale(act32)).astype(jnp.bfloat16)
    n1t_s[...] = n1_ref[...].T
    ready(0)

    def rows_of(h):
        return tuple(pl.ds(part * width + h * hdim, hdim) for part in range(3))

    def project(h):
        rows = rows_of(h)
        stacked = jnp.concatenate([wqkv[r, :] for r in rows], axis=0)
        proj = dot_nn(stacked, n1t_s[...]).astype(jnp.bfloat16)
        for part, r in enumerate(rows):
            qkv_ref[r, :] = proj[part * hdim:(part + 1) * hdim]

    def score(h):
        rows = rows_of(h)
        score_s[h % 3] = dot_tn(qkv_ref[rows[1], :], qkv_ref[rows[0], :])

    def soften(h):
        blocks, stats = causal_weights(score_s.at[h % 3], None, None, scale)
        stat_ref[h, 0:1, :] = stats[0]
        stat_ref[h, 1:2, :] = stats[1]
        prob_s[h % 2] = assemble(blocks, jnp.bfloat16)

    def mix(h):
        rows = rows_of(h)
        ctx_ref[rows[0], :] = dot_nn(qkv_ref[rows[2], :], prob_s[h % 2]).astype(jnp.bfloat16)

    for step in range(heads + 5):
        for lag, action in ((0, project), (2, score), (4, soften), (5, mix)):
            h = step - lag
            if 0 <= h < heads:
                action(h)
    flush(0)
    ready(1)
    acc_s[...] = dot_tn(ctx_ref[...], wout[...])
    for rows in row_blocks(act_ref.shape[0]):
        hid16 = (act_ref[rows, :].astype(jnp.float32) + acc_s[rows, :]).astype(jnp.bfloat16)
        hid_ref[rows, :] = hid16
        hid32 = hid16.astype(jnp.float32)
        n2_ref[rows, :] = (hid32 * rms_scale(hid32)).astype(jnp.bfloat16)
    normed2 = n2_ref[...]
    flush(1)
    ready(2)
    for tile in range(ffn // ffn_tile):
        cols = pl.ds(tile * ffn_tile, ffn_tile)
        pre = dot_nn(normed2, wup[:, cols])
        gp_ref[:, cols] = pre
        tanh = jnp.tanh(pre * (GELU_C + (GELU_C * GELU_A) * (pre * pre)))
        up_ref[:, cols] = (pre * (0.5 + 0.5 * tanh)).astype(jnp.bfloat16)
    flush(2)
    ready(3)
    acc_s[...] = dot_nn(up_ref[...], wdown[...])
    for rows in row_blocks(act_ref.shape[0]):
        out_ref[rows, :] = (hid_ref[rows, :].astype(jnp.float32) + acc_s[rows, :]).astype(jnp.bfloat16)


def backward_layer(dims, grad_ref, act_ref, wqkv, wout, wup, wdown, qkv_ref, stat_ref, hid_ref, gp_ref, dpre_ref, dhid_ref, dctx_ref, dqkv_ref, dact_ref, flush, acc_s, dhid_s32, dhidt_s, score_s, dprob_s, prob_s, dscore_s):
    heads, hdim, ffn_tile = dims
    width = heads * hdim
    ffn = wdown.shape[0]
    scale = hdim ** -0.5
    grad16 = grad_ref[...]

    def slope(tile):
        cols = pl.ds(tile * ffn_tile, ffn_tile)
        dup = dot_nt(grad16, wdown[cols, :])
        pre = gp_ref[:, cols]
        pre_sq = pre * pre
        tanh = jnp.tanh(pre * (GELU_C + (GELU_C * GELU_A) * pre_sq))
        half = 0.5 + 0.5 * tanh
        bend = (half * (1.0 - half)) * (pre * (2.0 * GELU_C + (6.0 * GELU_C * GELU_A) * pre_sq))
        dpre_ref[:, cols] = (dup * (half + bend)).astype(jnp.bfloat16)

    def gather(tile):
        cols = pl.ds(tile * ffn_tile, ffn_tile)
        part = dot_nt(dpre_ref[:, cols], wup[:, cols])
        if tile == 0:
            acc_s[...] = part
        else:
            acc_s[...] += part

    tiles = ffn // ffn_tile
    for step in range(tiles + LAG_MLP):
        if step < tiles:
            slope(step)
        if step >= LAG_MLP:
            gather(step - LAG_MLP)
    flush(0)
    for rows in row_blocks(act_ref.shape[0]):
        dhid32 = grad_ref[rows, :].astype(jnp.float32) + rms_vjp(hid_ref[rows, :].astype(jnp.float32), acc_s[rows, :])
        dhid_s32[rows, :] = dhid32
        dhid_ref[rows, :] = dhid32.astype(jnp.bfloat16)
    dhidt_s[...] = dhid_ref[...].T
    flush(1)

    def rows_of(h):
        return tuple(pl.ds(part * width + h * hdim, hdim) for part in range(3))

    def project(h):
        rows = rows_of(h)[0]
        dctx_ref[rows, :] = dot_nn(wout[rows, :], dhidt_s[...]).astype(jnp.bfloat16)

    def score(h):
        rows = rows_of(h)
        score_s[h % 3] = dot_tn(qkv_ref[rows[1], :], qkv_ref[rows[0], :])
        dprob_s[h % 3] = dot_tn(qkv_ref[rows[2], :], dctx_ref[rows[0], :])

    def soften(h):
        probs, _ = causal_weights(score_s.at[h % 3], stat_ref[h, 0:1, :], stat_ref[h, 1:2, :], scale)
        dprobs = dprob_s.at[h % 3]
        half = dprobs.shape[0] // 2
        d_ul, d_ur, d_lr = dprobs[:half, :half], dprobs[:half, half:], dprobs[half:, half:]
        p_ul, p_ur, p_lr = probs
        delta_l = jnp.sum(d_ul * p_ul, axis=0, keepdims=True)
        delta_r = jnp.sum(d_ur * p_ur, axis=0, keepdims=True) + jnp.sum(d_lr * p_lr, axis=0, keepdims=True)
        prob_s[h % 2] = assemble(probs, jnp.bfloat16)
        dscore_s[h % 2] = assemble((p_ul * (d_ul - delta_l) * scale, p_ur * (d_ur - delta_r) * scale, p_lr * (d_lr - delta_r) * scale), jnp.bfloat16)

    def mix(h):
        rows = rows_of(h)
        dqkv_ref[rows[2], :] = dot_nt(dctx_ref[rows[0], :], prob_s[h % 2]).astype(jnp.bfloat16)
        dqkv_ref[rows[0], :] = dot_nn(qkv_ref[rows[1], :], dscore_s[h % 2]).astype(jnp.bfloat16)
        dqkv_ref[rows[1], :] = dot_nt(qkv_ref[rows[0], :], dscore_s[h % 2]).astype(jnp.bfloat16)

    def collect(first, count):
        spans = [pl.ds(part * width + first * hdim, count * hdim) for part in range(3)]
        part = dot_tn(jnp.concatenate([dqkv_ref[r, :] for r in spans], axis=0), jnp.concatenate([wqkv[r, :] for r in spans], axis=0))
        if first == 0:
            acc_s[...] = part
        else:
            acc_s[...] += part

    group = min(GROUP, heads)
    for step in range(heads + 5):
        for lag, action in ((0, project), (2, score), (4, soften), (5, mix)):
            h = step - lag
            if 0 <= h < heads:
                action(h)
        done = step - 6
        if done >= 0 and done % group == group - 1 and done < heads - group:
            collect(done - group + 1, group)
    flush(2)
    collect(heads - group, group)
    for rows in row_blocks(act_ref.shape[0]):
        dact = dhid_s32[rows, :] + rms_vjp(act_ref[rows, :].astype(jnp.float32), acc_s[rows, :])
        dact_ref[rows, :] = dact.astype(jnp.bfloat16)


class placement:
    def __init__(self, n_stages):
        row = lax.axis_index('data')
        self.row = row
        self.index = lax.axis_index('stage')
        self.column = lax.div(self.index, 2)
        self.core = lax.rem(self.index, 2)
        self.upper = lax.div(row, 2)
        self.half = lax.rem(self.upper + self.column, 2)
        self.layer = 2 * self.column + self.half
        self.home = self.layer
        self.mate = 2 * self.column + 1 - self.core
        across = 3 - row
        along = lax.rem(self.index + jnp.where(self.half == 1, 2, n_stages - 2), n_stages)
        self.mate_id = {'data': row, 'stage': self.mate}
        self.across_id = {'data': across, 'stage': self.index}
        self.along_id = {'data': row, 'stage': along}
        self.next_id = {'data': jnp.where(self.half == 1, row, across), 'stage': jnp.where(self.half == 1, along, self.index)}
        self.prev_id = {'data': jnp.where(self.half == 1, across, row), 'stage': jnp.where(self.half == 1, self.index, along)}


def pipeline_kernel(
    cfg,
    emb_hbm, tgt_hbm, wqkv_hbm, wout_hbm, wup_hbm, wdown_hbm,
    loss_ref, n1_hbm, n2_hbm, up_hbm, ctx_hbm, dqkv_hbm, dpre_hbm, dhid_hbm, g_hbm, dx_hbm, qkv_hbm, gp_hbm, hid_hbm, stat_hbm,
    wqkv, wout, wup, wdown, act, grad, out_s, dact_s,
    n1_s, n2_s, up_s, ctx_s, qkv_s, gp_s, hid_s, stat_s,
    dpre_s, dhid_s, dctx_s, dqkv_s,
    w_sem, in_sem, act_sem, grad_sem, fout_sem, bin_sem, bout_sem, fsend_sem, bsend_sem, loss_acc, loss_sem, dx_sem, n1t_s, score_s, prob_s, dprob_s, dscore_s, acc_s, dhid_s32,
):
    n_stages, n_seq, tokens, grad_scale, dims = cfg
    here = placement(n_stages)
    stage, core, next_id, prev_id = here.layer, here.core, here.next_id, here.prev_id
    is_first = stage == 0
    is_last = stage == n_stages - 1
    own_weights = here.layer == here.index
    own_data = here.upper == core
    feeds_first = (here.column == 0) & (here.half == 1) & (core == 1)
    feeds_last = (here.column == n_stages // 2 - 1) & (here.half == 0) & (core == 1)

    weight_pairs = ((wqkv_hbm, wqkv), (wout_hbm, wout), (wup_hbm, wup), (wdown_hbm, wdown))

    def load_weight(idx):
        return pltpu.make_async_copy(weight_pairs[idx][0], weight_pairs[idx][1], w_sem.at[idx])

    def give_weight(idx):
        return pltpu.make_async_remote_copy(
            src_ref=weight_pairs[idx][1], dst_ref=weight_pairs[idx][1], send_sem=w_sem.at[4 + idx], recv_sem=w_sem.at[8 + idx],
            device_id=here.mate_id, device_id_type=MESH_ID)

    def load_embed(m):
        return pltpu.make_async_copy(emb_hbm.at[m], act.at[m], in_sem.at[m])

    def load_target(m):
        return pltpu.make_async_copy(tgt_hbm.at[m], grad.at[m], in_sem.at[m])

    def give_embed(m):
        return pltpu.make_async_remote_copy(
            src_ref=emb_hbm.at[m], dst_ref=act.at[m], send_sem=in_sem.at[m], recv_sem=act_sem.at[m],
            device_id=here.across_id, device_id_type=MESH_ID)

    def give_target(m):
        return pltpu.make_async_remote_copy(
            src_ref=tgt_hbm.at[m], dst_ref=grad.at[m], send_sem=in_sem.at[m], recv_sem=grad_sem.at[m],
            device_id=here.across_id, device_id_type=MESH_ID)

    def each_seq(when, action):
        @pl.when(when)
        def _():
            def go(m, carry):
                action(m)
                return carry
            lax.fori_loop(0, n_seq, go, 0)

    @pl.when(own_weights)
    def _():
        for idx in range(4):
            load_weight(idx).start()

    each_seq(is_first & own_data, lambda m: load_embed(m).start())
    each_seq(is_last & own_data, lambda m: load_target(m).start())

    barrier = pltpu.get_barrier_semaphore()
    for peer in (here.mate_id, here.across_id, here.along_id):
        pl.semaphore_signal(barrier, inc=1, device_id=peer, device_id_type=MESH_ID)
    pl.semaphore_wait(barrier, 3)

    each_seq(feeds_first, lambda m: give_embed(m).start())
    each_seq(feeds_last, lambda m: give_target(m).start())
    loss_acc[...] = jnp.zeros_like(loss_acc)

    def await_weight(idx):
        @pl.when(own_weights)
        def _():
            load_weight(idx).wait()
            give_weight(idx).start()

        @pl.when(jnp.logical_not(own_weights))
        def _():
            give_weight(idx).wait_recv()

    def send_act(m, slot):
        return pltpu.make_async_remote_copy(
            src_ref=out_s.at[slot], dst_ref=act.at[m], send_sem=fsend_sem.at[slot], recv_sem=act_sem.at[m],
            device_id=next_id, device_id_type=MESH_ID)

    def send_grad(m, slot):
        return pltpu.make_async_remote_copy(
            src_ref=dact_s.at[slot], dst_ref=grad.at[m], send_sem=bsend_sem.at[slot], recv_sem=grad_sem.at[m],
            device_id=prev_id, device_id_type=MESH_ID)

    def store_dx(m, slot):
        return pltpu.make_async_copy(dact_s.at[slot], dx_hbm.at[m], bsend_sem.at[slot])

    def give_dx(m, slot):
        return pltpu.make_async_remote_copy(
            src_ref=dact_s.at[slot], dst_ref=dx_hbm.at[m], send_sem=bsend_sem.at[slot], recv_sem=dx_sem.at[m],
            device_id=here.across_id, device_id_type=MESH_ID)

    def token_range(m):
        return pl.ds(pl.multiple_of(m * tokens, tokens), tokens)

    def fout_copies(m, slot):
        rows = token_range(m)
        return (
            (0, pltpu.make_async_copy(n1_s.at[slot], n1_hbm.at[rows, :], fout_sem.at[slot, 0])),
            (0, pltpu.make_async_copy(qkv_s.at[slot], qkv_hbm.at[m], fout_sem.at[slot, 1])),
            (1, pltpu.make_async_copy(ctx_s.at[slot], ctx_hbm.at[:, rows], fout_sem.at[slot, 2])),
            (1, pltpu.make_async_copy(stat_s.at[slot], stat_hbm.at[m], fout_sem.at[slot, 3])),
            (1, pltpu.make_async_copy(hid_s.at[slot], hid_hbm.at[m], fout_sem.at[slot, 4])),
            (1, pltpu.make_async_copy(n2_s.at[slot], n2_hbm.at[rows, :], fout_sem.at[slot, 5])),
            (2, pltpu.make_async_copy(gp_s.at[slot], gp_hbm.at[m], fout_sem.at[slot, 6])),
            (2, pltpu.make_async_copy(up_s.at[slot], up_hbm.at[rows, :], fout_sem.at[slot, 7])),
        )

    def bin_copies(m):
        return (
            pltpu.make_async_copy(qkv_hbm.at[m], qkv_s.at[2], bin_sem.at[0]),
            pltpu.make_async_copy(stat_hbm.at[m], stat_s.at[2], bin_sem.at[1]),
            pltpu.make_async_copy(hid_hbm.at[m], hid_s.at[2], bin_sem.at[2]),
            pltpu.make_async_copy(gp_hbm.at[m], gp_s.at[2], bin_sem.at[3]),
        )

    def bout_copies(m, slot):
        rows = token_range(m)
        return (
            (0, pltpu.make_async_copy(grad.at[m], g_hbm.at[rows, :], bout_sem.at[slot, 0])),
            (0, pltpu.make_async_copy(dpre_s.at[slot], dpre_hbm.at[rows, :], bout_sem.at[slot, 1])),
            (1, pltpu.make_async_copy(dhid_s.at[slot], dhid_hbm.at[rows, :], bout_sem.at[slot, 2])),
            (2, pltpu.make_async_copy(dqkv_s.at[slot], dqkv_hbm.at[:, rows], bout_sem.at[slot, 3])),
        )

    def flusher(copies):
        def flush(group):
            for when, copy in copies:
                if when == group:
                    copy.start()
        return flush

    def in_range(m):
        return (m >= 0) & (m < n_seq)

    rehearses = (stage >= 2) | ((stage == 1) & own_weights)

    def tick(t, carry):
        fwd_m = t - stage
        rehearsal = rehearses & (fwd_m == -1)
        bwd_m = t + 2 * stage - 3 * (n_stages - 1)

        @pl.when(rehearsal)
        def _():
            tone = lax.broadcasted_iota(jnp.int32, act.shape[1:], 0) * 7 + lax.broadcasted_iota(jnp.int32, act.shape[1:], 1) * 5
            act[n_seq] = (lax.rem(tone, 31) - 15).astype(jnp.float32).astype(jnp.bfloat16)
            for idx in range(4):
                await_weight(idx)

        @pl.when(in_range(fwd_m) | rehearsal)
        def _():
            m = jnp.where(rehearsal, n_seq - 1, fwd_m)
            m_in = jnp.where(rehearsal, n_seq, fwd_m)
            slot = lax.rem(m, 2)

            @pl.when(is_first & own_data)
            def _():
                load_embed(m).wait()

            @pl.when(jnp.logical_not((is_first & own_data) | rehearsal))
            def _():
                send_act(m, slot).wait_recv()

            def run_forward(ready):
                forward_layer(
                    dims, act.at[m_in], wqkv, wout, wup, wdown, n1_s.at[slot], qkv_s.at[slot], stat_s.at[slot],
                    ctx_s.at[slot], hid_s.at[slot], n2_s.at[slot], gp_s.at[slot], up_s.at[slot], out_s.at[slot],
                    flusher(fout_copies(m, slot)), n1t_s, score_s, prob_s, acc_s, ready)

            first_use = (m == 0) & jnp.logical_not(rehearses)

            @pl.when(first_use)
            def _():
                run_forward(await_weight)

            @pl.when(jnp.logical_not(first_use))
            def _():
                run_forward(lambda idx: None)

            real = jnp.logical_not(rehearsal)

            @pl.when(jnp.logical_not(is_last) & real)
            def _():
                send_act(m, slot).start()

            @pl.when(is_last & own_data & real)
            def _():
                load_target(m).wait()

            @pl.when(is_last & jnp.logical_not(own_data) & real)
            def _():
                send_grad(m, slot).wait_recv()

            @pl.when(is_last & real)
            def _():
                for start in range(0, tokens, 32):
                    rows = pl.ds(start, 32)
                    error = out_s[slot, rows, :].astype(jnp.float32) - grad[m, rows, :].astype(jnp.float32)
                    square = error * error
                    loss_acc[...] += (square[0:8] + square[8:16]) + (square[16:24] + square[24:32])
                    grad[m, rows, :] = (error * grad_scale).astype(jnp.bfloat16)

        @pl.when(in_range(bwd_m))
        def _():
            m = bwd_m
            slot = lax.rem(m, 2)

            @pl.when(jnp.logical_not(is_last))
            def _():
                for copy in bin_copies(m):
                    copy.wait()
                send_grad(m, slot).wait_recv()

            saved = jnp.where(is_last, slot, 2)
            backward_layer(
                dims, grad.at[m], act.at[m], wqkv, wout, wup, wdown, qkv_s.at[saved], stat_s.at[saved], hid_s.at[saved],
                gp_s.at[saved], dpre_s.at[slot], dhid_s.at[slot], dctx_s, dqkv_s.at[slot], dact_s.at[slot],
                flusher(bout_copies(m, slot)), acc_s, dhid_s32, n1t_s, score_s, dprob_s, prob_s, dscore_s)

            @pl.when(jnp.logical_not(is_first))
            def _():
                send_grad(m, slot).start()

            @pl.when(is_first & own_data)
            def _():
                store_dx(m, slot).start()

            @pl.when(is_first & jnp.logical_not(own_data))
            def _():
                give_dx(m, slot).start()

        fwd_old = fwd_m - 1
        bwd_old = bwd_m - 1

        rehearsed = rehearses & (fwd_old == -1)

        @pl.when(in_range(fwd_old) | rehearsed)
        def _():
            m = jnp.where(rehearsed, n_seq - 1, fwd_old)
            slot = lax.rem(m, 2)
            for _, copy in fout_copies(m, slot):
                copy.wait()

            @pl.when(jnp.logical_not(is_last | rehearsed))
            def _():
                send_act(m, slot).wait_send()

        @pl.when(in_range(bwd_old))
        def _():
            slot = lax.rem(bwd_old, 2)
            for _, copy in bout_copies(bwd_old, slot):
                copy.wait()

            @pl.when(jnp.logical_not(is_first))
            def _():
                send_grad(bwd_old, slot).wait_send()

            @pl.when(is_first & own_data)
            def _():
                store_dx(bwd_old, slot).wait()

            @pl.when(is_first & jnp.logical_not(own_data))
            def _():
                give_dx(bwd_old, slot).wait_send()

        @pl.when(in_range(bwd_m + 1) & jnp.logical_not(is_last))
        def _():
            for copy in bin_copies(bwd_m + 1):
                copy.start()

        return carry

    lax.fori_loop(0, n_seq + 3 * (n_stages - 1) + 1, tick, 0)

    def send_loss():
        return pltpu.make_async_remote_copy(
            src_ref=loss_ref, dst_ref=loss_ref, send_sem=loss_sem.at[0], recv_sem=loss_sem.at[1],
            device_id=prev_id, device_id_type=MESH_ID)

    @pl.when(is_last)
    def _():
        lanes = loss_ref.shape[1]
        total = loss_acc[:, 0:lanes]
        for col in range(lanes, loss_acc.shape[1], lanes):
            total = total + loss_acc[:, col:col + lanes]
        loss_ref[...] = total

    @pl.when(jnp.logical_not(is_last))
    def _():
        send_loss().wait_recv()

    @pl.when(jnp.logical_not(is_first))
    def _():
        send_loss().start()
        send_loss().wait_send()

    @pl.when(own_weights)
    def _():
        for idx in range(4):
            give_weight(idx).wait_send()

    each_seq(feeds_first, lambda m: give_embed(m).wait_send())
    each_seq(feeds_last, lambda m: give_target(m).wait_send())
    each_seq(feeds_first, lambda m: give_dx(m, 0).wait_recv())


def run_pipeline(n_stages, grad_scale, embeds, targets, wqkv, wout, wup, wdown, heads, hdim):
    n_seq, tokens, width = embeds.shape
    ffn = wdown.shape[0]
    dims = (heads, hdim, 512 if ffn % 512 == 0 else ffn)
    bf16, f32 = jnp.bfloat16, jnp.float32
    total = n_seq * tokens
    out_shapes = [
        ((8, 128), f32),
        ((total, width), bf16),
        ((total, width), bf16),
        ((total, ffn), bf16),
        ((width, total), bf16),
        ((3 * width, total), bf16),
        ((total, ffn), bf16),
        ((total, width), bf16),
        ((total, width), bf16),
        ((n_seq, tokens, width), bf16),
        ((n_seq, 3 * width, tokens), bf16),
        ((n_seq, tokens, ffn), f32),
        ((n_seq, tokens, width), bf16),
        ((n_seq, heads, 8, tokens), f32),
    ]
    any_spec = pl.BlockSpec(memory_space=pl.ANY)
    scratch = [
        pltpu.VMEM(wqkv.shape, bf16), pltpu.VMEM(wout.shape, bf16), pltpu.VMEM(wup.shape, bf16), pltpu.VMEM(wdown.shape, bf16),
        pltpu.VMEM((n_seq + 1, tokens, width), bf16), pltpu.VMEM((n_seq, tokens, width), bf16),
        pltpu.VMEM((2, tokens, width), bf16), pltpu.VMEM((2, tokens, width), bf16),
        pltpu.VMEM((2, tokens, width), bf16), pltpu.VMEM((2, tokens, width), bf16),
        pltpu.VMEM((2, tokens, ffn), bf16), pltpu.VMEM((2, width, tokens), bf16),
        pltpu.VMEM((3, 3 * width, tokens), bf16), pltpu.VMEM((3, tokens, ffn), f32),
        pltpu.VMEM((3, tokens, width), bf16), pltpu.VMEM((3, heads, 8, tokens), f32),
        pltpu.VMEM((2, tokens, ffn), bf16), pltpu.VMEM((2, tokens, width), bf16),
        pltpu.VMEM((width, tokens), bf16), pltpu.VMEM((2, 3 * width, tokens), bf16),
        pltpu.SemaphoreType.DMA((12,)), pltpu.SemaphoreType.DMA((n_seq,)),
        pltpu.SemaphoreType.DMA((n_seq,)), pltpu.SemaphoreType.DMA((n_seq,)),
        pltpu.SemaphoreType.DMA((2, 8)), pltpu.SemaphoreType.DMA((4,)), pltpu.SemaphoreType.DMA((2, 4)),
        pltpu.SemaphoreType.DMA((2,)), pltpu.SemaphoreType.DMA((2,)),
        pltpu.VMEM((8, width), f32), pltpu.SemaphoreType.DMA((2,)), pltpu.SemaphoreType.DMA((n_seq,)),
        pltpu.VMEM((width, tokens), bf16), pltpu.VMEM((3, tokens, tokens), f32), pltpu.VMEM((2, tokens, tokens), bf16),
        pltpu.VMEM((3, tokens, tokens), f32), pltpu.VMEM((2, tokens, tokens), bf16), pltpu.VMEM((tokens, width), f32), pltpu.VMEM((tokens, width), f32),
    ]
    linear = 2 * total * (wqkv.size + wout.size + wup.size + wdown.size)
    return pl.pallas_call(
        functools.partial(pipeline_kernel, (n_stages, n_seq, tokens, grad_scale, dims)),
        out_shape=[jax.ShapeDtypeStruct(s, d) for s, d in out_shapes],
        in_specs=[any_spec] * 6,
        out_specs=[pl.BlockSpec(memory_space=pltpu.VMEM)] + [any_spec] * (len(out_shapes) - 1),
        scratch_shapes=scratch,
        compiler_params=pltpu.CompilerParams(
            collective_id=0, has_side_effects=True, vmem_limit_bytes=67043328),
        cost_estimate=pl.CostEstimate(flops=3 * linear, bytes_accessed=200 * 2 ** 20, transcendentals=0),
        name='stage_pipeline',
    )(embeds, targets, wqkv, wout, wup, wdown)


def reduce_kernel(
    cfg,
    loss_hbm, ctx_hbm, dhid_hbm, dqkv_hbm, n1_hbm, up_hbm, g_hbm, n2_hbm, dpre_hbm, dx_hbm,
    loss_ref, dout_hbm, dqkvw_hbm, ddown_hbm, dup_hbm, demb_hbm,
    out_res, qkv_res, down_res, up_res, out_in, qkv_in, down_in, up_in,
    out_give, qkv_give, down_give, up_give, out_core, qkv_core, down_core, up_core, out_row, qkv_row, down_row, up_row, loss_sl,
    res_sem, in_sem, give_sem, core_sem, row_send, row_recv, put_send, put_recv, pass_send, store_sem, dx_sem,
    loss_send, loss_recv, loss_in,
):
    (n_stages,) = cfg
    here = placement(n_stages)
    row, core, stage = here.row, here.core, here.index
    pair = lax.rem(row, 2)
    pair_row = row + 1 - 2 * pair
    across = 3 - row
    is_home = here.home == stage
    home_id = {'data': row, 'stage': here.home}
    pair_id = {'data': pair_row, 'stage': stage}
    pair_home_id = {'data': pair_row, 'stage': here.home}
    across_home_id = {'data': across, 'stage': here.home}

    kinds = (
        ('rows', dhid_hbm, out_res, ctx_hbm, out_in, out_give, out_core, out_row, dout_hbm),
        ('rows', n1_hbm, qkv_res, dqkv_hbm, qkv_in, qkv_give, qkv_core, qkv_row, dqkvw_hbm),
        ('tall', g_hbm, down_res, up_hbm, down_in, down_give, down_core, down_row, ddown_hbm),
        ('wide', n2_hbm, up_res, dpre_hbm, up_in, up_give, up_core, up_row, dup_hbm),
    )
    n_kinds = len(kinds)
    turns = ((1, 1), (0, 1), (1, 0), (0, 0))

    def piece(kind, member, unit, num):
        size = kinds[kind][4].shape[1 if kinds[kind][0] == 'rows' else 2]
        return pl.ds(pl.multiple_of(((member * 2 + unit) * 2 + num) * size, size), size)

    def flip(val, by):
        return 1 - val if by else val

    def read_piece(kind, turn, num):
        form, _, _, src, buf = kinds[kind][:5]
        part = piece(kind, flip(pair, turns[turn][0]), flip(core, turns[turn][1]), num)
        view = src.at[part, :] if form == 'rows' else src.at[:, part]
        return pltpu.make_async_copy(view, buf.at[turn % 2], in_sem.at[kind, turn % 2])

    def out_view(kind, member, unit, num):
        part = piece(kind, member, unit, num)
        dst = kinds[kind][8]
        return dst.at[:, part] if kinds[kind][0] == 'wide' else dst.at[part, :]

    tile = min(256, out_res.shape[1])
    n_tiles = out_res.shape[1] // tile

    def tile_at(kind, n):
        span = pl.ds(pl.multiple_of(n * tile, tile), tile)
        return (span, slice(None)) if kinds[kind][0] == 'wide' else (slice(None), span)

    def each_tile(action):
        def body(n, carry):
            action(n)
            return carry
        lax.fori_loop(0, n_tiles, body, 0)

    def give(kind, other, num):
        return pltpu.make_async_remote_copy(
            src_ref=kinds[kind][5].at[other], dst_ref=kinds[kind][6].at[num, other], send_sem=give_sem.at[kind, other],
            recv_sem=core_sem.at[kind, num, other], device_id=here.mate_id, device_id_type=MESH_ID)

    def send_row(kind, num, n):
        at = tile_at(kind, n)
        return pltpu.make_async_remote_copy(
            src_ref=kinds[kind][6].at[(num, 1) + at], dst_ref=kinds[kind][7].at[(num,) + at], send_sem=row_send.at[kind, num, n],
            recv_sem=row_recv.at[kind, num, n], device_id=pair_id, device_id_type=MESH_ID)

    def put_view(kind, member, unit, num, n):
        part = piece(kind, member, unit, num)
        span = pl.ds(pl.multiple_of(n * tile, tile), tile)
        dst = kinds[kind][8]
        return dst.at[span, part] if kinds[kind][0] == 'wide' else dst.at[part, span]

    def put(kind, num, n, target, device_id):
        return pltpu.make_async_remote_copy(
            src_ref=kinds[kind][7].at[(num,) + tile_at(kind, n)], dst_ref=put_view(kind, pair, core, num, n),
            send_sem=put_send.at[target, kind, num, n], recv_sem=put_recv.at[pair, core, kind, num, n],
            device_id=device_id, device_id_type=MESH_ID)

    def keep(kind, num):
        return pltpu.make_async_copy(kinds[kind][7].at[num], out_view(kind, pair, core, num), store_sem.at[kind, num])

    def arrival(kind, num, n, member, unit):
        view = put_view(kind, member, unit, num, n)
        return pltpu.make_async_remote_copy(
            src_ref=view, dst_ref=view, send_sem=pass_send.at[unit, kind, num, n], recv_sem=put_recv.at[member, unit, kind, num, n],
            device_id=across_home_id, device_id_type=MESH_ID)

    def load_resident(kind):
        return pltpu.make_async_copy(kinds[kind][1], kinds[kind][2], res_sem.at[kind])

    def pipeline_id(row_idx, unit):
        return 2 * jnp.minimum(row_idx, 3 - row_idx) + unit

    my_loss = pltpu.make_async_copy(loss_hbm, loss_sl.at[pipeline_id(row, core)], loss_in)
    my_loss.start()
    load_resident(0).start()
    read_piece(0, 0, 0).start()

    source = here.upper
    rank = stage + source - 2 * source * core
    spans = []
    span = n_stages // 2
    while span >= 1:
        spans.append(span)
        span //= 2

    def swapped(span):
        return stage + span - 2 * span * lax.rem(lax.div(stage, span), 2)

    loss_ids = (
        ({'data': row, 'stage': here.mate}, row, 1 - core),
        ({'data': pair_row, 'stage': stage}, pair_row, core),
        ({'data': pair_row, 'stage': here.mate}, pair_row, 1 - core),
    )
    peers = [ident for ident, _, _ in loss_ids]
    peers += [{'data': across, 'stage': stage}, {'data': across, 'stage': here.mate}]
    peers += [{'data': row, 'stage': swapped(span)} for span in spans if span > 1]
    barrier = pltpu.get_barrier_semaphore()
    for ident in peers:
        pl.semaphore_signal(barrier, inc=1, device_id=ident, device_id_type=MESH_ID)
    pl.semaphore_wait(barrier, len(peers))

    def send_loss(idx):
        slot = loss_sl.at[pipeline_id(row, core)]
        return pltpu.make_async_remote_copy(
            src_ref=slot, dst_ref=slot, send_sem=loss_send.at[idx], recv_sem=loss_recv.at[idx],
            device_id=loss_ids[idx][0], device_id_type=MESH_ID)

    def loss_arrival(idx):
        slot = loss_sl.at[pipeline_id(loss_ids[idx][1], loss_ids[idx][2])]
        return pltpu.make_async_remote_copy(
            src_ref=slot, dst_ref=slot, send_sem=loss_send.at[idx], recv_sem=loss_recv.at[idx],
            device_id=loss_ids[idx][0], device_id_type=MESH_ID)

    for kind in range(1, n_kinds):
        load_resident(kind).start()
        read_piece(kind, 0, 0).start()
    my_loss.wait()
    for idx in range(3):
        send_loss(idx).start()

    def spread(idx):
        return pltpu.make_async_remote_copy(
            src_ref=demb_hbm, dst_ref=demb_hbm, send_sem=dx_sem.at[0, idx], recv_sem=dx_sem.at[1, idx],
            device_id={'data': row, 'stage': swapped(spans[idx])}, device_id_type=MESH_ID)

    def sends_at(idx):
        return lax.rem(rank, 2 * spans[idx]) == 0

    def receives_at(idx):
        return lax.rem(rank, 2 * spans[idx]) == spans[idx]

    def spread_round(idx):
        if idx > 0:
            @pl.when(receives_at(idx - 1))
            def _():
                spread(idx - 1).wait_recv()
        if idx < len(spans):
            @pl.when(sends_at(idx))
            def _():
                spread(idx).start()

    def product(kind, turn, num, sink, base, before=None, after=None):
        form, _, res, _, buf = kinds[kind][:5]
        read_piece(kind, turn, num).wait()
        if turn < 3:
            read_piece(kind, turn + 1, num).start()
        else:
            @pl.when(num == 0)
            def _():
                read_piece(kind, 0, 1).start()
        fed = buf.at[turn % 2]

        def body(n):
            at = tile_at(kind, n)
            span = pl.ds(pl.multiple_of(n * tile, tile), tile)
            if before is not None:
                before(n)
            if form == 'rows':
                part = dot_nn(fed[...], res[:, span])
            elif form == 'tall':
                part = dot_tn(fed[...], res[:, span])
            else:
                part = dot_tn(res[:, span], fed[...])
            for ref in base:
                part = part + ref[at]
            sink[at] = part
            if after is not None:
                after(n)

        each_tile(body)

    def first_half(kind, num):
        give_buf, core_buf = kinds[kind][5:7]

        @pl.when(num == 0)
        def _():
            load_resident(kind).wait()

        for turn, other in ((0, 1), (1, 0)):
            @pl.when(num > 0)
            def _():
                give(kind, other, num - 1).wait_send()

            product(kind, turn, num, give_buf.at[other], ())
            give(kind, other, num).start()
        give(kind, 1, num).wait_recv()
        product(kind, 2, num, core_buf.at[num, 1], (core_buf.at[num, 1],), after=lambda n: send_row(kind, num, n).start())

    def second_half(kind, num):
        core_buf, row_buf = kinds[kind][6:8]
        give(kind, 0, num).wait_recv()

        def after(n):
            put(kind, num, n, 1, pair_home_id).start()
            put(kind, num, n, 2, across_home_id).start()

            @pl.when(jnp.logical_not(is_home))
            def _():
                put(kind, num, n, 0, home_id).start()

        product(kind, 3, num, row_buf.at[num], (core_buf.at[num, 0], row_buf.at[num]),
                before=lambda n: send_row(kind, num, n).wait_recv(), after=after)

        @pl.when(is_home)
        def _():
            keep(kind, num).start()

    def pass_on(kind, num):
        @pl.when(is_home)
        def _():
            def go(n):
                for unit in range(2):
                    arrival(kind, num, n, 1 - pair, unit).wait_recv()
                    arrival(kind, num, n, 1 - pair, unit).start()
            each_tile(go)

    def kind_at(pos):
        late = jnp.where(pos == 4, 2, jnp.where(pos == 5, 3, jnp.where(pos == 6, 1, 0)))
        return jnp.where(pos < 4, pos, late)

    def num_at(pos):
        return jnp.where(pos < 4, 0, 1)

    n_steps = 2 * n_kinds

    def step_body(pos, carry):
        for kind in range(n_kinds):
            @pl.when((pos < n_steps) & (kind_at(pos) == kind))
            def _():
                first_half(kind, num_at(pos))

        for kind in range(n_kinds):
            @pl.when((pos >= 1) & (pos < n_steps + 1) & (kind_at(pos - 1) == kind))
            def _():
                second_half(kind, num_at(pos - 1))

        for kind in range(n_kinds):
            @pl.when((pos >= 2) & (kind_at(pos - 2) == kind))
            def _():
                pass_on(kind, num_at(pos - 2))

        for idx in range(len(spans) + 1):
            @pl.when(pos == 3 * idx)
            def _():
                spread_round(idx)
        return carry

    lax.fori_loop(0, n_steps + 2, step_body, 0)

    for idx in range(3):
        loss_arrival(idx).wait_recv()
    total = loss_sl[0]
    for idx in range(1, 4):
        total = total + loss_sl[idx]
    loss_ref[...] = total

    for kind in range(n_kinds):
        for num in range(2):
            def settle(n):
                @pl.when(is_home)
                def _():
                    arrival(kind, num, n, pair, 1 - core).wait_recv()
                    for unit in range(2):
                        arrival(kind, num, n, 1 - pair, unit).wait_send()

                @pl.when(jnp.logical_not(is_home))
                def _():
                    for member in range(2):
                        for unit in range(2):
                            arrival(kind, num, n, member, unit).wait_recv()
                    put(kind, num, n, 0, home_id).wait_send()

                send_row(kind, num, n).wait_send()
                put(kind, num, n, 1, pair_home_id).wait_send()
                put(kind, num, n, 2, across_home_id).wait_send()

            each_tile(settle)

            @pl.when(is_home)
            def _():
                keep(kind, num).wait()
        for other in range(2):
            give(kind, other, 1).wait_send()
    for idx in range(3):
        send_loss(idx).wait_send()
    for idx in range(len(spans)):
        @pl.when(sends_at(idx))
        def _():
            spread(idx).wait_send()


def sum_gradients(n_stages, loss_part, ctx_t, dhid, dqkv_t, n1, upper, grads, n2, dpre, dx):
    bf16, f32 = jnp.bfloat16, jnp.float32
    total, width = n1.shape
    ffn = upper.shape[1]
    small, mid, big = width // 8, 3 * width // 8, ffn // 8
    any_spec = pl.BlockSpec(memory_space=pl.ANY)
    vmem_spec = pl.BlockSpec(memory_space=pltpu.VMEM)
    out_shapes = [(loss_part.shape, f32), ((width, width), f32), ((3 * width, width), f32), ((ffn, width), f32), ((width, ffn), f32), (dx.shape, bf16)]
    n_spans = n_stages.bit_length() - 1
    n_tiles = max(1, width // 256)
    pieces = ((small, width), (mid, width), (big, width), (width, big))
    dma = pltpu.SemaphoreType.DMA
    scratch = [pltpu.VMEM((total, width), bf16)] * 4 + [
        pltpu.VMEM((2, small, total), bf16), pltpu.VMEM((2, mid, total), bf16),
        pltpu.VMEM((2, total, big), bf16), pltpu.VMEM((2, total, big), bf16),
    ]
    scratch += [pltpu.VMEM((2,) + p, f32) for p in pieces]
    scratch += [pltpu.VMEM((2, 2) + p, f32) for p in pieces]
    scratch += [pltpu.VMEM((2,) + p, f32) for p in pieces]
    scratch += [
        pltpu.VMEM((4,) + loss_part.shape, f32),
        dma((4,)), dma((4, 2)), dma((4, 2)), dma((4, 2, 2)), dma((4, 2, n_tiles)), dma((4, 2, n_tiles)),
        dma((3, 4, 2, n_tiles)), dma((2, 2, 4, 2, n_tiles)), dma((2, 4, 2, n_tiles)), dma((4, 2)), dma((2, n_spans)), dma((3,)), dma((3,)), dma(()),
    ]
    flops = 2 * total * width * (4 * width + 2 * ffn)
    return pl.pallas_call(
        functools.partial(reduce_kernel, (n_stages,)),
        out_shape=[jax.ShapeDtypeStruct(s, d) for s, d in out_shapes],
        in_specs=[any_spec] * 10,
        out_specs=[vmem_spec] + [any_spec] * 5,
        scratch_shapes=scratch,
        input_output_aliases={9: 5},
        compiler_params=pltpu.CompilerParams(collective_id=1, has_side_effects=True, vmem_limit_bytes=67043328),
        cost_estimate=pl.CostEstimate(flops=flops, bytes_accessed=150 * 2 ** 20, transcendentals=0),
        name='gradient_sums',
    )(loss_part, ctx_t, dhid, dqkv_t, n1, upper, grads, n2, dpre, dx)


def settle_kernel(plan, loss_factor, loss_in, *refs):
    count = len(plan)
    sources, loss_ref, results = refs[:count], refs[count], refs[count + 1:2 * count + 1]
    holds, sem = refs[2 * count + 1:-1], refs[-1]
    copies = []
    for src, hold, dst, parts in zip(sources, holds, results, plan):
        lead = src.shape[0] // parts
        for idx in range(parts):
            part = pl.ds(idx * lead, lead)
            num = len(copies)
            copies.append((
                pltpu.make_async_copy(src.at[part], hold.at[part], sem.at[0, num]),
                pltpu.make_async_copy(hold.at[part], dst.at[part], sem.at[1, num])))
    for read, _ in copies:
        read.start()
    loss_ref[0] = loss_factor * jnp.sum(loss_in[...])
    for read, write in copies:
        read.wait()
        write.start()
    for _, write in copies:
        write.wait()


def settle(loss_factor, loss_sum, arrays):
    plan = tuple(next(p for p in (4, 3, 2, 1) if arr.shape[0] % (16 * p) == 0 or p == 1 or (arr.ndim == 3 and arr.shape[0] % p == 0)) for arr in arrays)
    any_spec = pl.BlockSpec(memory_space=pl.ANY)
    outs = pl.pallas_call(
        functools.partial(settle_kernel, plan, loss_factor),
        out_shape=[jax.ShapeDtypeStruct((1,), jnp.float32)] + [jax.ShapeDtypeStruct(arr.shape, arr.dtype) for arr in arrays],
        in_specs=[pl.BlockSpec(memory_space=pltpu.VMEM)] + [any_spec] * len(arrays),
        out_specs=[pl.BlockSpec(memory_space=pltpu.SMEM)] + [any_spec] * len(arrays),
        scratch_shapes=[pltpu.VMEM(arr.shape, arr.dtype) for arr in arrays] + [pltpu.SemaphoreType.DMA((2, sum(plan)))],
        compiler_params=pltpu.CompilerParams(vmem_limit_bytes=60 * 2 ** 20),
        name='settle_results',
    )(loss_sum, *arrays)
    return outs[0], outs[1:]


def solution(mesh):
    n_stages = mesh.shape['stage']
    n_data = mesh.shape['data']
    act_spec = P(('rep', 'data'))
    weight_spec = P(('rep', 'stage'))

    def per_device(embeds, targets, w_qkv, w_out, w_up, w_down):
        n_micro, micro_b, seq_len, width = embeds.shape
        heads, hdim = w_qkv.shape[2], w_qkv.shape[3]
        grad_scale = 1.0 / (n_data * n_micro)
        loss_norm = 1.0 / (n_data * n_micro * micro_b * seq_len * width)
        flat = (n_micro * micro_b, seq_len, width)
        outs = run_pipeline(
            n_stages, grad_scale, embeds.reshape(flat), targets.reshape(flat), w_qkv.reshape(3 * width, width),
            w_out.reshape(width, width), w_up[0], w_down[0], heads, hdim)
        loss_part, n1, n2, upper, ctx_t, dqkv_t, dpre, dhid, grads, dx = outs[:10]
        loss_sum, *sums = sum_gradients(
            n_stages, loss_part, ctx_t, dhid, dqkv_t, n1, upper, grads, n2, dpre, dx)
        loss, (d_out, d_qkv, d_down, d_up, d_embeds) = settle(0.5 * loss_norm, loss_sum, sums)
        return (loss, d_qkv.reshape(w_qkv.shape), d_out.reshape(w_out.shape), d_up[None], d_down[None], d_embeds.reshape(embeds.shape))

    return jax.shard_map(per_device, mesh=mesh, in_specs=(act_spec, act_spec, weight_spec, weight_spec, weight_spec, weight_spec), out_specs=(P('rep'), weight_spec, weight_spec, weight_spec, weight_spec, act_spec), check_vma=False)
```
